32 devices in a mesh: dp: 8 (over z, y), tensor: 4 (over x, core).
Axes of the slice: x: 2, y: 2, z: 4, core: 2. Of those that a mesh axis runs over, the one named last changes fastest.
Arguments:
- input_img: bfloat16 [24, 256, 1536], P('dp'), may hold values from -6 to 6
- input_txt: bfloat16 [24, 154, 1536], P('dp'), may hold values from -6 to 6
- conditioning: bfloat16 [24, 1536], replicated, may hold values from -6 to 6
- ada_weight: bfloat16 [2, 1536, 9216], P(None, None, ('dp', 'tensor')), may hold values from -0.15625 to 0.15625
- ada_bias: bfloat16 [2, 9216], P(None, ('dp', 'tensor')), may hold values from -3 to 3
- qkv_weight: bfloat16 [2, 1536, 3, 1536], P(None, None, None, 'tensor'), may hold values from -0.15625 to 0.15625
- qkv_bias: bfloat16 [2, 3, 1536], P(None, None, 'tensor'), may hold values from -3 to 3
- norm_gain: float32 [2, 2, 64], replicated, may hold values from 0.1 to 1.9
- proj_weight: bfloat16 [2, 1536, 1536], P(None, 'tensor'), may hold values from -0.4375 to 0.4375
- proj_bias: bfloat16 [2, 1536], replicated, may hold values from -3 to 3
- up_weight: bfloat16 [2, 1536, 6144], P(None, None, 'tensor'), may hold values from -0.15625 to 0.15625
- up_bias: bfloat16 [2, 6144], P(None, 'tensor'), may hold values from -3 to 3
- down_weight: bfloat16 [2, 6144, 1536], P(None, 'tensor'), may hold values from -0.078125 to 0.078125
- down_bias: bfloat16 [2, 1536], replicated, may hold values from -3 to 3
- cotangent_img: bfloat16 [24, 256, 1536], P('dp'), may hold values from -6 to 6
- cotangent_txt: bfloat16 [24, 154, 1536], P('dp'), may hold values from -6 to 6
Outputs:
- output_img: bfloat16 [24, 256, 1536], P('dp')
- output_txt: bfloat16 [24, 154, 1536], P('dp')
- grad_input_img: bfloat16 [24, 256, 1536], P('dp')
- grad_input_txt: bfloat16 [24, 154, 1536], P('dp')
- grad_conditioning: float32 [24, 1536], P('dp')
- grad_ada_weight: float32 [2, 1536, 9216], P(None, None, ('dp', 'tensor'))
- grad_ada_bias: float32 [2, 9216], P(None, ('dp', 'tensor'))
- grad_qkv_weight: float32 [2, 1536, 3, 1536], P(None, 'dp', None, 'tensor')
- grad_qkv_bias: float32 [2, 3, 1536], P(None, None, 'tensor')
- grad_norm_gain: float32 [2, 2, 64], replicated
- grad_proj_weight: float32 [2, 1536, 1536], P(None, 'tensor', 'dp')
- grad_proj_bias: float32 [2, 1536], replicated
- grad_up_weight: float32 [2, 1536, 6144], P(None, 'dp', 'tensor')
- grad_up_bias: float32 [2, 6144], P(None, 'tensor')
- grad_down_weight: float32 [2, 6144, 1536], P(None, 'tensor', 'dp')
- grad_down_bias: float32 [2, 1536], replicated
The draws below stay inside these ranges and needn't reach their ends.
All inputs are finite; a program needn't handle non-finite values.
Results may differ from the reference program's by a relative error of at most 0.012.
Values sent between devices are 32-bit elements; how exact they have to be, the bound alone decides.
A program may use at most 384 MiB of HBM per device.

```python
import jax
import jax.numpy as jnp
from jax import lax

D = 1536
HEAD_DIM = 64
FF = 6144
COND = 1536
IMG = 256
TXT = 154
SEQS = 24


def block_scale(key, dims, pieces, low, top_value):
    loudness = 1.0
    for position, parts in pieces:
        heights = jax.random.uniform(jax.random.fold_in(jax.random.fold_in(key, 6), position), (parts,), jnp.float32, low / len(pieces), top_value / len(pieces))
        loudness = loudness * jnp.repeat(jnp.exp(heights), dims[position] // parts).reshape((-1,) + (1,) * (len(dims) - 1 - position))
    return loudness


def bell_draw(own_key, shape, scale, bound, cuts=(), kind=jnp.bfloat16):
    array = jax.random.normal(own_key, shape, jnp.float32) * scale
    if len(cuts) > 0:
        array = block_scale(own_key, shape, cuts, -0.22, 0.18) * array
    return jnp.clip(array, min=-bound, max=bound).astype(kind)


def setup_inputs(seed: int = 0) -> dict:
    splits = jax.random.split(jax.random.key(seed), 17)
    return {
        "input_img": bell_draw(splits[0], (SEQS, IMG, D), 1.0, 6.0, ((0, 8),)),
        "input_txt": bell_draw(splits[1], (SEQS, TXT, D), 1.0, 6.0, ((0, 8),)),
        "conditioning": bell_draw(splits[2], (SEQS, COND), 1.0, 6.0),
        "ada_weight": bell_draw(splits[3], (2, COND, 6 * D), COND ** -0.5, 0.15625, ((2, 32),)),
        "ada_bias": bell_draw(splits[4], (2, 6 * D), 0.5, 3.0, ((1, 32),)),
        "qkv_weight": bell_draw(splits[5], (2, D, 3, D), D ** -0.5, 0.15625, ((3, 4),)),
        "qkv_bias": bell_draw(splits[6], (2, 3, D), 0.5, 3.0, ((2, 4),)),
        "norm_gain": jnp.clip(1.0 + 0.18 * jax.random.normal(splits[7], (2, 2, HEAD_DIM), jnp.float32), 0.1, 1.9),
        "proj_weight": bell_draw(splits[8], (2, D, D), (D // 8) ** -0.5, 0.4375, ((1, 4),)),
        "proj_bias": bell_draw(splits[9], (2, D), 0.5, 3.0),
        "up_weight": bell_draw(splits[10], (2, D, FF), D ** -0.5, 0.15625, ((2, 4),)),
        "up_bias": bell_draw(splits[11], (2, FF), 0.5, 3.0, ((1, 4),)),
        "down_weight": bell_draw(splits[12], (2, FF, D), FF ** -0.5, 0.078125, ((1, 4),)),
        "down_bias": bell_draw(splits[13], (2, D), 0.5, 3.0),
        "cotangent_img": bell_draw(splits[14], (SEQS, IMG, D), 1.0, 6.0, ((0, 8),)),
        "cotangent_txt": bell_draw(splits[15], (SEQS, TXT, D), 1.0, 6.0, ((0, 8),)),
    }


epsilon = 1e-06
GELU_C = 0.7978845608028654
GELU_A = 0.044715

def mixed(pattern, first_op, second_op):
    return jnp.einsum(pattern, first_op.astype(jnp.float32), second_op.astype(jnp.float32))

def dot_plain(first_op, second_op):
    return jnp.dot(first_op, second_op, preferred_element_type=jnp.float32)

def dot_right_t(first_op, second_op):
    return lax.dot_general(first_op, second_op, (((1,), (1,)), ((), ())), preferred_element_type=jnp.float32)

def dot_left_t(first_op, second_op):
    return lax.dot_general(first_op, second_op, (((0,), (0,)), ((), ())), preferred_element_type=jnp.float32)

def layer_norm(values):
    center = values - lax.optimization_barrier(jnp.mean(values, axis=-1, keepdims=True))
    inverse = lax.rsqrt(lax.optimization_barrier(jnp.mean(center * center, axis=-1, keepdims=True)) + epsilon)
    return (center * inverse, inverse)

def norm_back(grad_normed, normed, inverse):
    return inverse * (grad_normed - lax.optimization_barrier(jnp.mean(grad_normed, axis=-1, keepdims=True)) - normed * lax.optimization_barrier(jnp.mean(grad_normed * normed, axis=-1, keepdims=True)))

def gelu_tanh(values):
    return 0.5 * values * (1.0 + jnp.tanh(GELU_C * (values + GELU_A * values * values * values)))

def gelu_slope(values):
    inner = jnp.tanh(GELU_C * (values + GELU_A * values * values * values))
    return 0.5 * (1.0 + inner) + 0.5 * values * (1.0 - inner * inner) * GELU_C * (1.0 + 3.0 * GELU_A * values * values)

def piece_of(modulate, piece_index):
    feat_width = modulate.shape[1] // 6
    return modulate[:, None, piece_index * feat_width:(piece_index + 1) * feat_width]

def token_span(array_in, stream):
    if stream == 0:
        return array_in[:, :IMG]
    return array_in[:, IMG:]

def paired(records, field_name):
    return jnp.stack([records[0][field_name], records[1][field_name]])

def front_part(values, modulate, qkv_w, qkv_b, gain_pair):
    batch_size, length, feat_width = values.shape
    normed, inverse = layer_norm(values.astype(jnp.float32))
    hidden = (normed * (1.0 + piece_of(modulate, 1)) + piece_of(modulate, 0)).astype(jnp.bfloat16)
    packed = dot_plain(hidden.reshape(batch_size * length, feat_width), qkv_w.reshape(feat_width, -1))
    head_dim = gain_pair.shape[1]
    packed = (packed.reshape(batch_size, length, 3, -1) + qkv_b).reshape(batch_size, length, 3, -1, head_dim)
    q_raw = packed[:, :, 0]
    k_raw = packed[:, :, 1]
    q_factor = lax.rsqrt(lax.optimization_barrier(jnp.mean(q_raw * q_raw, axis=-1, keepdims=True)) + epsilon)
    k_factor = lax.rsqrt(lax.optimization_barrier(jnp.mean(k_raw * k_raw, axis=-1, keepdims=True)) + epsilon)
    return {'normed': normed, 'inverse': inverse, 'hidden': hidden, 'q_raw': q_raw, 'k_raw': k_raw, 'q_factor': q_factor, 'k_factor': k_factor, 'q_low': (q_raw * q_factor * gain_pair[0]).astype(jnp.bfloat16), 'k_low': (k_raw * k_factor * gain_pair[1]).astype(jnp.bfloat16), 'v_low': packed[:, :, 2].astype(jnp.bfloat16)}

def attn_scores(q_all, k_all):
    return mixed('bqhd,bkhd->bhqk', q_all, k_all) * q_all.shape[3] ** (-0.5)

def attn_forward(q_all, k_all, v_all):
    scores = attn_scores(q_all, k_all)
    row_top = lax.optimization_barrier(jnp.max(scores, axis=-1, keepdims=True))
    log_total = row_top + jnp.log(lax.optimization_barrier(jnp.sum(jnp.exp(scores - row_top), axis=-1, keepdims=True)))
    prob_low = jnp.exp(scores - log_total).astype(jnp.bfloat16)
    attn_all = mixed('bhqk,bkhd->bqhd', prob_low, v_all).astype(jnp.bfloat16)
    return (attn_all, log_total)

def attn_backward(q_all, k_all, v_all, log_total, grad_attn):
    scores = attn_scores(q_all, k_all)
    prob_full = jnp.exp(scores - log_total)
    prob_low = prob_full.astype(jnp.bfloat16)
    grad_vals = mixed('bhqk,bqhd->bkhd', prob_low, grad_attn)
    grad_prob = mixed('bqhd,bkhd->bhqk', grad_attn, v_all)
    grad_scores = (prob_full * (grad_prob - lax.optimization_barrier(jnp.sum(prob_full * grad_prob, axis=-1, keepdims=True)))).astype(jnp.bfloat16)
    score_scale = q_all.shape[3] ** (-0.5)
    grad_query = mixed('bhqk,bkhd->bqhd', grad_scores, k_all) * score_scale
    grad_keys = mixed('bhqk,bqhd->bkhd', grad_scores, q_all) * score_scale
    return (grad_query, grad_keys, grad_vals)

def middle_part(values, modulate, branch_sum, proj_b, up_w, up_b):
    batch_size, length, feat_width = values.shape
    branch = branch_sum.reshape(batch_size, length, feat_width) + proj_b
    residual = values.astype(jnp.float32) + piece_of(modulate, 2) * branch
    normed, inverse = layer_norm(residual)
    hidden = (normed * (1.0 + piece_of(modulate, 4)) + piece_of(modulate, 3)).astype(jnp.bfloat16)
    upward = dot_plain(hidden.reshape(-1, feat_width), up_w) + up_b
    return {'branch': branch, 'residual': residual, 'normed': normed, 'inverse': inverse, 'hidden': hidden, 'upward': upward, 'active': gelu_tanh(upward).astype(jnp.bfloat16)}

def finish_part(state, mlp_sum, modulate, down_b):
    mlp_out = mlp_sum.reshape(state['residual'].shape) + down_b
    state['mlp_out'] = mlp_out
    return (state['residual'] + piece_of(modulate, 5) * mlp_out).astype(jnp.bfloat16)

def mlp_back_part(state, cotangent, modulate, down_w):
    feat_width = cotangent.shape[2]
    grad_out = cotangent.astype(jnp.float32)
    grad_mlp = grad_out * piece_of(modulate, 5)
    grad_mlp_low = grad_mlp.astype(jnp.bfloat16).reshape(-1, feat_width)
    grad_upward = dot_right_t(grad_mlp_low, down_w) * gelu_slope(state['upward'])
    grad_up_low = grad_upward.astype(jnp.bfloat16)
    return {'grad_out': grad_out, 'gate_two': lax.optimization_barrier(jnp.sum(grad_out * state['mlp_out'], axis=1)), 'down_b': lax.optimization_barrier(jnp.sum(grad_mlp, axis=(0, 1))), 'down_w': dot_left_t(state['active'], grad_mlp_low), 'up_b': lax.optimization_barrier(jnp.sum(grad_upward, axis=0)), 'up_w': dot_left_t(state['hidden'].reshape(-1, feat_width), grad_up_low), 'up_low': grad_up_low}

def resid_back_part(state, mlp_back, hidden_sum, modulate, proj_w, attn_part):
    grad_hidden = hidden_sum.reshape(state['residual'].shape)
    grad_resid = mlp_back['grad_out'] + norm_back(grad_hidden * (1.0 + piece_of(modulate, 4)), state['normed'], state['inverse'])
    grad_branch = grad_resid * piece_of(modulate, 2)
    local_width = attn_part.shape[2] * attn_part.shape[3]
    grad_branch_low = grad_branch.astype(jnp.bfloat16).reshape(-1, grad_branch.shape[2])
    return {'shift_two': lax.optimization_barrier(jnp.sum(grad_hidden, axis=1)), 'scale_two': lax.optimization_barrier(jnp.sum(grad_hidden * state['normed'], axis=1)), 'gate_one': lax.optimization_barrier(jnp.sum(grad_resid * state['branch'], axis=1)), 'grad_resid': grad_resid, 'proj_b': lax.optimization_barrier(jnp.sum(grad_branch, axis=(0, 1))), 'proj_w': dot_left_t(attn_part.reshape(-1, local_width), grad_branch_low), 'grad_attn': dot_right_t(grad_branch_low, proj_w).astype(jnp.bfloat16).reshape(attn_part.shape)}

def qkv_back_part(front, grad_query, grad_keys, grad_vals, gain_pair, qkv_w):
    grad_q_gain = grad_query * gain_pair[0]
    grad_q_raw = front['q_factor'] * grad_q_gain - front['q_raw'] * front['q_factor'] ** 3 * lax.optimization_barrier(jnp.mean(grad_q_gain * front['q_raw'], axis=-1, keepdims=True))
    grad_k_gain = grad_keys * gain_pair[1]
    grad_k_raw = front['k_factor'] * grad_k_gain - front['k_raw'] * front['k_factor'] ** 3 * lax.optimization_barrier(jnp.mean(grad_k_gain * front['k_raw'], axis=-1, keepdims=True))
    gain_term = jnp.stack([lax.optimization_barrier(jnp.sum(grad_query * front['q_raw'] * front['q_factor'], axis=(0, 1, 2))), lax.optimization_barrier(jnp.sum(grad_keys * front['k_raw'] * front['k_factor'], axis=(0, 1, 2)))])
    batch_size, length, feat_width = front['hidden'].shape
    grad_packed = jnp.stack([grad_q_raw, grad_k_raw, grad_vals], axis=2).reshape(batch_size * length, -1)
    grad_packed_low = grad_packed.astype(jnp.bfloat16)
    return {'gain': gain_term, 'qkv_b': lax.optimization_barrier(jnp.sum(grad_packed, axis=0)).reshape(3, -1), 'qkv_w': dot_left_t(front['hidden'].reshape(batch_size * length, feat_width), grad_packed_low).reshape(feat_width, 3, -1), 'grad_hidden': dot_right_t(grad_packed_low, qkv_w.reshape(feat_width, -1))}

def input_back_part(front, grad_resid, hidden_sum, modulate):
    grad_hidden = hidden_sum.reshape(grad_resid.shape)
    grad_input = grad_resid + norm_back(grad_hidden * (1.0 + piece_of(modulate, 1)), front['normed'], front['inverse'])
    return {'shift_one': lax.optimization_barrier(jnp.sum(grad_hidden, axis=1)), 'scale_one': lax.optimization_barrier(jnp.sum(grad_hidden * front['normed'], axis=1)), 'grad_input': grad_input.astype(jnp.bfloat16)}

def block_pass(input_img, input_txt, cotangent_img, cotangent_txt, modulate, qkv_weight, qkv_bias, norm_gain, proj_weight, proj_bias, up_weight, up_bias, down_weight, down_bias):
    inputs = (input_img, input_txt)
    cotangents = (cotangent_img, cotangent_txt)
    fronts = [front_part(inputs[stream], modulate[:, stream], qkv_weight[stream], qkv_bias[stream], norm_gain[stream]) for stream in range(2)]
    q_all = jnp.concatenate([fronts[0]['q_low'], fronts[1]['q_low']], axis=1)
    k_all = jnp.concatenate([fronts[0]['k_low'], fronts[1]['k_low']], axis=1)
    v_all = jnp.concatenate([fronts[0]['v_low'], fronts[1]['v_low']], axis=1)
    attn_all, log_total = attn_forward(q_all, k_all, v_all)
    attn_parts = [token_span(attn_all, stream) for stream in range(2)]
    local_width = attn_all.shape[2] * attn_all.shape[3]
    branch_sums = [dot_plain(attn_parts[stream].reshape(-1, local_width), proj_weight[stream]) for stream in range(2)]
    states = [middle_part(inputs[stream], modulate[:, stream], branch_sums[stream], proj_bias[stream], up_weight[stream], up_bias[stream]) for stream in range(2)]
    mlp_sums = [dot_plain(states[stream]['active'], down_weight[stream]) for stream in range(2)]
    outputs = [finish_part(states[stream], mlp_sums[stream], modulate[:, stream], down_bias[stream]) for stream in range(2)]
    mlp_backs = [mlp_back_part(states[stream], cotangents[stream], modulate[:, stream], down_weight[stream]) for stream in range(2)]
    hidden_sums = [dot_right_t(mlp_backs[stream]['up_low'], up_weight[stream]) for stream in range(2)]
    resid_backs = [resid_back_part(states[stream], mlp_backs[stream], hidden_sums[stream], modulate[:, stream], proj_weight[stream], attn_parts[stream]) for stream in range(2)]
    grad_attn = jnp.concatenate([resid_backs[0]['grad_attn'], resid_backs[1]['grad_attn']], axis=1)
    grad_query, grad_keys, grad_vals = attn_backward(q_all, k_all, v_all, log_total, grad_attn)
    qkv_backs = [qkv_back_part(fronts[stream], token_span(grad_query, stream), token_span(grad_keys, stream), token_span(grad_vals, stream), norm_gain[stream], qkv_weight[stream]) for stream in range(2)]
    input_backs = [input_back_part(fronts[stream], resid_backs[stream]['grad_resid'], qkv_backs[stream]['grad_hidden'], modulate[:, stream]) for stream in range(2)]
    grad_modulate = jnp.stack([jnp.concatenate([input_backs[stream]['shift_one'], input_backs[stream]['scale_one'], resid_backs[stream]['gate_one'], resid_backs[stream]['shift_two'], resid_backs[stream]['scale_two'], mlp_backs[stream]['gate_two']], axis=-1) for stream in range(2)], axis=1)
    grads = (paired(qkv_backs, 'qkv_w'), paired(qkv_backs, 'qkv_b'), paired(qkv_backs, 'gain'), paired(resid_backs, 'proj_w'), paired(resid_backs, 'proj_b'), paired(mlp_backs, 'up_w'), paired(mlp_backs, 'up_b'), paired(mlp_backs, 'down_w'), paired(mlp_backs, 'down_b'))
    return ((outputs[0], outputs[1], input_backs[0]['grad_input'], input_backs[1]['grad_input'], grad_modulate), grads)

def reference(input_img, input_txt, conditioning, ada_weight, ada_bias, qkv_weight, qkv_bias, norm_gain, proj_weight, proj_bias, up_weight, up_bias, down_weight, down_bias, cotangent_img, cotangent_txt):
    cond_wide = conditioning.astype(jnp.float32)
    cond_sig = jax.nn.sigmoid(cond_wide)
    silu_cond = (cond_wide * cond_sig).astype(jnp.bfloat16)
    modulate = jnp.stack([dot_plain(silu_cond, ada_weight[stream]) + ada_bias[stream] for stream in range(2)], axis=1)
    weights = (qkv_weight, qkv_bias, norm_gain, proj_weight, proj_bias, up_weight, up_bias, down_weight, down_bias)

    def one_sequence(totals, sliced):
        results, grads = block_pass(sliced[0][None], sliced[1][None], sliced[2][None], sliced[3][None], sliced[4][None], weights[0], weights[1], weights[2], weights[3], weights[4], weights[5], weights[6], weights[7], weights[8])
        return (tuple((running + grad_one for running, grad_one in zip(totals, grads))), results)
    initial = tuple((jnp.zeros(weight_one.shape, jnp.float32) for weight_one in weights))
    totals, results = lax.scan(one_sequence, initial, (input_img, input_txt, cotangent_img, cotangent_txt, modulate))
    grad_modulate = results[4][:, 0]
    grad_ada_bias = lax.optimization_barrier(jnp.sum(grad_modulate, axis=0))
    grad_mod_low = grad_modulate.astype(jnp.bfloat16)
    grad_ada_weight = jnp.stack([dot_left_t(silu_cond, grad_mod_low[:, stream]) for stream in range(2)])
    grad_silu = dot_right_t(grad_mod_low[:, 0], ada_weight[0]) + dot_right_t(grad_mod_low[:, 1], ada_weight[1])
    grad_conditioning = grad_silu * cond_sig * (1.0 + cond_wide * (1.0 - cond_sig))
    return (results[0][:, 0], results[1][:, 0], results[2][:, 0], results[3][:, 0], grad_conditioning, grad_ada_weight, grad_ada_bias, totals[0], totals[1], totals[2], totals[3], totals[4], totals[5], totals[6], totals[7], totals[8])
```

```python
import functools

import jax
import jax.numpy as jnp
from jax import lax
from jax.experimental import pallas as pl
from jax.experimental.pallas import tpu as pltpu
from jax.sharding import PartitionSpec as P

epsilon = 1e-06
GELU_C = 0.7978845608028654
GELU_A = 0.044715
ROW_TILE = 16
NEG = -1e30


def dot_plain(first_op, second_op):
    return jnp.dot(first_op, second_op, preferred_element_type=jnp.float32)


def dot_right_t(first_op, second_op):
    return lax.dot_general(
        first_op, second_op, (((1,), (1,)), ((), ())), preferred_element_type=jnp.float32
    )


def dot_left_t(first_op, second_op):
    return lax.dot_general(
        first_op, second_op, (((0,), (0,)), ((), ())), preferred_element_type=jnp.float32
    )


def layer_norm(values):
    center = values - jnp.mean(values, axis=-1, keepdims=True)
    inverse = lax.rsqrt(jnp.mean(center * center, axis=-1, keepdims=True) + epsilon)
    return (center * inverse, inverse)


def norm_back(grad_normed, normed, inverse):
    return inverse * (
        grad_normed
        - jnp.mean(grad_normed, axis=-1, keepdims=True)
        - normed * jnp.mean(grad_normed * normed, axis=-1, keepdims=True)
    )


def gelu_both(values):
    inner = jnp.tanh(GELU_C * (values + GELU_A * values * values * values))
    active = 0.5 * values * (1.0 + inner)
    slope = 0.5 * (1.0 + inner) + 0.5 * values * (1.0 - inner * inner) * GELU_C * (
        1.0 + 3.0 * GELU_A * values * values
    )
    return active, slope


def head_norm(values, gain):
    head_dim = values.shape[1] // 2
    lower = lax.broadcasted_iota(jnp.int32, values.shape, 1) < head_dim
    square = values * values
    first = jnp.sum(jnp.where(lower, square, 0.0), axis=-1, keepdims=True) / head_dim
    second = jnp.sum(jnp.where(lower, 0.0, square), axis=-1, keepdims=True) / head_dim
    factor = jnp.where(lower, lax.rsqrt(first + epsilon), lax.rsqrt(second + epsilon))
    return values * factor * gain, factor


def rows_of(img_ref, txt_ref, cols):
    return jnp.concatenate(
        [img_ref[0, 0, :, cols], img_ref[1, 0, :, cols], txt_ref[0, 0, :, cols], txt_ref[1, 0, :, cols]],
        axis=0,
    )


def put_rows(img_ref, txt_ref, cols, values):
    img, txt = img_ref.shape[2], txt_ref.shape[2]
    img_ref[0, 0, :, cols] = values[:img]
    img_ref[1, 0, :, cols] = values[img : 2 * img]
    txt_ref[0, 0, :, cols] = values[2 * img : 2 * img + txt]
    txt_ref[1, 0, :, cols] = values[2 * img + txt :]


def gain_rows(gain_ref, which, img, txt):
    width = gain_ref.shape[2]
    return jnp.concatenate(
        [
            jnp.broadcast_to(gain_ref[0, which : which + 1, :], (2 * img, width)),
            jnp.broadcast_to(gain_ref[1, which : which + 1, :], (2 * txt, width)),
        ],
        axis=0,
    )


def key_bias(img, txt, real):
    where = lax.broadcasted_iota(jnp.int32, (1, 2 * (img + txt)), 1)
    first = where - 2 * img
    gone = ((first >= real) & (first < txt)) | (first >= txt + real)
    return jnp.where(gone, NEG, 0.0).astype(jnp.float32)


def probs(q_head, k_low, bias):
    scores = dot_right_t(q_head, k_low) + bias
    top = jnp.max(scores, axis=-1, keepdims=True)
    weights = jnp.exp(scores - top)
    return weights * (1.0 / jnp.sum(weights, axis=-1, keepdims=True))


def attn_forward_kernel(real, gain_ref, img_ref, txt_ref, out_img_ref, out_txt_ref):
    img, txt = img_ref.shape[2], txt_ref.shape[2]
    local = img_ref.shape[3] // 3
    pair = gain_ref.shape[2]
    q_gain, k_gain = gain_rows(gain_ref, 0, img, txt), gain_rows(gain_ref, 1, img, txt)
    bias = key_bias(img, txt, real)
    scale = (pair // 2) ** (-0.5)
    for start in range(0, local, pair):
        q_raw, k_raw, v_raw = (
            rows_of(img_ref, txt_ref, slice(part * local + start, part * local + start + pair))
            for part in range(3)
        )
        q_low = head_norm(q_raw, q_gain)[0].astype(jnp.bfloat16) * jnp.bfloat16(scale)
        k_low = head_norm(k_raw, k_gain)[0].astype(jnp.bfloat16)
        v_low = v_raw.astype(jnp.bfloat16)
        lower = lax.broadcasted_iota(jnp.int32, q_raw.shape, 1) < pair // 2
        results = []
        for head in range(2):
            mine = lower if head == 0 else jnp.logical_not(lower)
            q_head = jnp.where(mine, q_low, jnp.bfloat16(0))
            results.append(dot_plain(probs(q_head, k_low, bias).astype(jnp.bfloat16), v_low))
        out = jnp.where(lower, results[0], results[1]).astype(jnp.bfloat16)
        put_rows(out_img_ref, out_txt_ref, slice(start, start + pair), out)


def attn_backward_kernel(
    real, gain_ref, img_ref, txt_ref, d_img_ref, d_txt_ref, o_img_ref, o_txt_ref, bias_ref, dgain_ref
):
    img, txt = img_ref.shape[2], txt_ref.shape[2]
    local = img_ref.shape[3] // 3
    pair = gain_ref.shape[2]
    head_dim = pair // 2
    q_gain, k_gain = gain_rows(gain_ref, 0, img, txt), gain_rows(gain_ref, 1, img, txt)
    bias = key_bias(img, txt, real)
    scale = head_dim ** (-0.5)
    gain_sums = [[None, None], [None, None]]
    for start in range(0, local, pair):
        q_raw, k_raw, v_raw = (
            rows_of(img_ref, txt_ref, slice(part * local + start, part * local + start + pair))
            for part in range(3)
        )
        q_wide, q_factor = head_norm(q_raw, q_gain)
        k_wide, k_factor = head_norm(k_raw, k_gain)
        q_low = q_wide.astype(jnp.bfloat16) * jnp.bfloat16(scale)
        k_low = k_wide.astype(jnp.bfloat16)
        v_low = v_raw.astype(jnp.bfloat16)
        grad_out = rows_of(d_img_ref, d_txt_ref, slice(start, start + pair))
        lower = lax.broadcasted_iota(jnp.int32, q_raw.shape, 1) < head_dim
        parts = []
        for head in range(2):
            mine = lower if head == 0 else jnp.logical_not(lower)
            prob = probs(jnp.where(mine, q_low, jnp.bfloat16(0)), k_low, bias)
            grad_v = dot_left_t(prob.astype(jnp.bfloat16), grad_out)
            grad_prob = dot_right_t(jnp.where(mine, grad_out, jnp.bfloat16(0)), v_low)
            delta = jnp.sum(prob * grad_prob, axis=-1, keepdims=True)
            grad_scores = (prob * (grad_prob - delta)).astype(jnp.bfloat16)
            parts.append((dot_plain(grad_scores, k_low), dot_left_t(grad_scores, q_low), grad_v))
        grad_qn = jnp.where(lower, parts[0][0], parts[1][0]) * scale
        grad_kn = jnp.where(lower, parts[0][1], parts[1][1])
        grad_vn = jnp.where(lower, parts[0][2], parts[1][2])

        def raw_grad(grad_normed, raw, factor, gain, which):
            gained = grad_normed * gain
            product = gained * raw
            first = jnp.sum(jnp.where(lower, product, 0.0), axis=-1, keepdims=True) / head_dim
            second = jnp.sum(jnp.where(lower, 0.0, product), axis=-1, keepdims=True) / head_dim
            inner = jnp.where(lower, first, second)
            terms = grad_normed * raw * factor
            for stream, rows in enumerate((slice(0, 2 * img), slice(2 * img, 2 * (img + txt)))):
                total = jnp.sum(terms[rows], axis=0, keepdims=True)
                old = gain_sums[stream][which]
                gain_sums[stream][which] = total if old is None else old + total
            return factor * gained - raw * (factor * factor * factor) * inner

        grads = (
            raw_grad(grad_qn, q_raw, q_factor, q_gain, 0),
            raw_grad(grad_kn, k_raw, k_factor, k_gain, 1),
            grad_vn,
        )
        for part, grad in enumerate(grads):
            cols = slice(part * local + start, part * local + start + pair)
            bias_ref[0, 0:1, cols] = jnp.sum(grad[: 2 * img], axis=0, keepdims=True)
            bias_ref[0, 1:2, cols] = jnp.sum(grad[2 * img :], axis=0, keepdims=True)
            put_rows(o_img_ref, o_txt_ref, cols, grad.astype(jnp.bfloat16))
    for stream in range(2):
        for which in range(2):
            row = stream * 2 + which
            dgain_ref[0, row : row + 1, :] = gain_sums[stream][which]


def block_of(array):
    shape = array.shape
    return pl.BlockSpec((shape[0], 1) + shape[2:], lambda seq: (0, seq, 0, 0))


def whole_of(array):
    return pl.BlockSpec(array.shape, lambda seq: (0,) * array.ndim)


def attn_forward(gain_pair, packed_img, packed_txt, real):
    seqs = packed_img.shape[1]
    local = packed_img.shape[3] // 3
    outs = [
        jax.ShapeDtypeStruct(packed.shape[:3] + (local,), jnp.bfloat16)
        for packed in (packed_img, packed_txt)
    ]
    rows = 2 * (packed_img.shape[2] + packed_txt.shape[2])
    return pl.pallas_call(
        functools.partial(attn_forward_kernel, real),
        grid=(seqs,),
        out_shape=outs,
        in_specs=[whole_of(gain_pair), block_of(packed_img), block_of(packed_txt)],
        out_specs=[block_of(out) for out in outs],
        compiler_params=pltpu.CompilerParams(vmem_limit_bytes=48 << 20),
        cost_estimate=pl.CostEstimate(
            flops=seqs * rows * rows * local * 4,
            bytes_accessed=seqs * rows * local * 14,
            transcendentals=seqs * rows * rows * (local // 64),
        ),
        name="attn_forward",
    )(gain_pair, packed_img, packed_txt)


def attn_backward(gain_pair, packed_img, packed_txt, grad_img, grad_txt, real):
    seqs = packed_img.shape[1]
    local = packed_img.shape[3] // 3
    outs = [
        jax.ShapeDtypeStruct(packed_img.shape, jnp.bfloat16),
        jax.ShapeDtypeStruct(packed_txt.shape, jnp.bfloat16),
        jax.ShapeDtypeStruct((seqs, 2, 3 * local), jnp.float32),
        jax.ShapeDtypeStruct((seqs, 4, gain_pair.shape[2]), jnp.float32),
    ]
    rows = 2 * (packed_img.shape[2] + packed_txt.shape[2])
    return pl.pallas_call(
        functools.partial(attn_backward_kernel, real),
        grid=(seqs,),
        out_shape=outs,
        in_specs=[whole_of(gain_pair)]
        + [block_of(each) for each in (packed_img, packed_txt, grad_img, grad_txt)],
        out_specs=[
            block_of(outs[0]),
            block_of(outs[1]),
            pl.BlockSpec((1, 2, 3 * local), lambda seq: (seq, 0, 0)),
            pl.BlockSpec((1, 4, gain_pair.shape[2]), lambda seq: (seq, 0, 0)),
        ],
        compiler_params=pltpu.CompilerParams(vmem_limit_bytes=56 << 20),
        cost_estimate=pl.CostEstimate(
            flops=seqs * rows * rows * local * 10,
            bytes_accessed=seqs * rows * local * 20,
            transcendentals=seqs * rows * rows * (local // 64),
        ),
        name="attn_backward",
    )(gain_pair, packed_img, packed_txt, grad_img, grad_txt)


def xor_index(index, distance):
    return index + distance - 2 * distance * ((index // distance) % 2)


def peers_of(data_size, tensor_size):
    row, col = lax.axis_index("dp"), lax.axis_index("tensor")
    around = [(lax.rem(row + step, data_size), col) for step in range(1, data_size)]
    across = []
    distance = 1
    while distance < tensor_size:
        across.append((row, xor_index(col, distance)))
        distance *= 2
    return row, col, around, across


def greet(partners):
    barrier = pltpu.get_barrier_semaphore()
    for partner in partners:
        pl.semaphore_signal(barrier, inc=1, device_id=partner, device_id_type=pl.DeviceIdType.MESH)
    pl.semaphore_wait(barrier, len(partners))


def remote(source, target, sems, index, partner):
    copy = pltpu.make_async_remote_copy(
        src_ref=source,
        dst_ref=target,
        send_sem=sems.at[0, index],
        recv_sem=sems.at[1, index],
        device_id=partner,
        device_id_type=pl.DeviceIdType.MESH,
    )
    copy.start()
    return copy


def silu_of(cond_ref):
    wide = cond_ref[...].astype(jnp.float32)
    return (wide * (1.0 / (1.0 + jnp.exp(-wide)))).astype(jnp.bfloat16)


def mod_forward_kernel(
    data_size, tensor_size, cond_ref, weight_ref, bias_ref, out_ref, outgoing, blocks, sems
):
    row, col, around, across = peers_of(data_size, tensor_size)
    seqs, feat = out_ref.shape[1], out_ref.shape[2]
    silu_cond = silu_of(cond_ref)
    for stream in range(2):
        values = dot_plain(silu_cond, weight_ref[stream]) + bias_ref[stream : stream + 1].astype(
            jnp.float32
        )
        for index in range(data_size):
            outgoing[index, stream * seqs : (stream + 1) * seqs] = values[
                index * seqs : (index + 1) * seqs
            ]
    blocks[col, row] = outgoing[row]
    greet(around + across)
    copies = [
        remote(outgoing.at[partner[0]], blocks.at[col, row], sems, index, partner)
        for index, partner in enumerate(around)
    ]
    for copy in copies:
        copy.wait()
    held, used = [0], len(around)
    for level in reversed(range(len(across))):
        distance = 1 << level
        copies = []
        for offset in held:
            index = col
            for bit in range(len(across)):
                if offset >> bit & 1:
                    index = xor_index(index, 1 << bit)
            copies.append(remote(blocks.at[index], blocks.at[index], sems, used, across[level]))
            used += 1
        for copy in copies:
            copy.wait()
        held = held + [offset | distance for offset in held]
    for stream in range(2):
        full = jnp.concatenate(
            [
                blocks[second, first, stream * seqs : (stream + 1) * seqs]
                for first in range(data_size)
                for second in range(tensor_size)
            ],
            axis=1,
        )
        for index in range(6):
            out_ref[stream * 6 + index] = full[:, index * feat : (index + 1) * feat]


def mod_forward(conditioning, ada_weight, ada_bias, seqs, feat, data_size, tensor_size):
    cols = ada_weight.shape[2]
    vmem = pl.BlockSpec(memory_space=pltpu.VMEM)
    return pl.pallas_call(
        functools.partial(mod_forward_kernel, data_size, tensor_size),
        out_shape=jax.ShapeDtypeStruct((12, seqs, feat), jnp.float32),
        in_specs=[vmem] * 3,
        out_specs=vmem,
        scratch_shapes=[
            pltpu.VMEM((data_size, 2 * seqs, cols), jnp.float32),
            pltpu.VMEM((tensor_size, data_size, 2 * seqs, cols), jnp.float32),
            pltpu.SemaphoreType.DMA((2, data_size + tensor_size)),
        ],
        compiler_params=pltpu.CompilerParams(
            collective_id=0, has_side_effects=True, vmem_limit_bytes=32 << 20
        ),
        name="mod_forward",
    )(conditioning, ada_weight, ada_bias)


def mod_backward_kernel(
    data_size,
    tensor_size,
    mod_ref,
    cond_ref,
    weight_ref,
    group_ref,
    all_ref,
    weight_out,
    bias_out,
    silu_out,
    group_out,
    all_out,
    blocks,
    core_in,
    outgoing,
    cols_in,
    group_in,
    all_in,
    group_own,
    all_own,
    silu_blocks,
    silu_in,
    silu_send,
    silu_recv,
    all_send,
    all_recv,
    sems,
):
    row, col, around, across = peers_of(data_size, tensor_size)
    seqs, feat = silu_out.shape
    cols = bias_out.shape[1]
    for stream in range(2):
        full = jnp.concatenate([mod_ref[stream * 6 + index] for index in range(6)], axis=1)
        for first in range(data_size):
            for second in range(tensor_size):
                start = (first * tensor_size + second) * cols
                blocks[second, first, stream * seqs : (stream + 1) * seqs] = full[
                    :, start : start + cols
                ]
    silu_cond = silu_of(cond_ref)
    greet(around + across)

    used = 0
    copy = remote(blocks.at[xor_index(col, 1)], core_in, sems, used, across[0])
    used += 1
    copy.wait()
    for first in range(data_size):
        outgoing[first] = blocks[col, first] + core_in[first]

    cols_in[row] = outgoing[row]
    group_in[row] = group_ref[row]
    all_in[row] = all_ref[row]
    copies = []
    for partner in around:
        for source, target in ((group_ref, group_in), (all_ref, all_in), (outgoing, cols_in)):
            copies.append(
                remote(source.at[partner[0]], target.at[row], sems, used, partner)
            )
            used += 1
    for copy in copies:
        copy.wait()
    group_own[...] = functools.reduce(jnp.add, [group_in[index] for index in range(data_size)])
    all_own[...] = functools.reduce(jnp.add, [all_in[index] for index in range(data_size)])
    low = []
    for stream in range(2):
        wide = jnp.concatenate(
            [cols_in[index, stream * seqs : (stream + 1) * seqs] for index in range(data_size)],
            axis=0,
        )
        bias_out[stream : stream + 1] = jnp.sum(wide, axis=0, keepdims=True)
        low.append(wide.astype(jnp.bfloat16))
    silu_grad = dot_right_t(low[0], weight_ref[0]) + dot_right_t(low[1], weight_ref[1])
    for index in range(data_size):
        silu_blocks[index] = silu_grad[index * seqs : (index + 1) * seqs]
    for stream in range(2):
        weight_out[stream] = dot_left_t(silu_cond, low[stream])

    silu_in[row] = silu_blocks[row]
    group_out[row] = group_own[...]
    all_send[0, row] = all_own[...]
    copies = []
    for partner in around:
        for source, target in (
            (silu_blocks.at[partner[0]], silu_in.at[row]),
            (group_own, group_out.at[row]),
            (all_own, all_send.at[0, row]),
        ):
            copies.append(remote(source, target, sems, used, partner))
            used += 1
    for copy in copies:
        copy.wait()
    silu_send[0] = functools.reduce(jnp.add, [silu_in[index] for index in range(data_size)])

    for level, partner in enumerate(across):
        copies = [
            remote(silu_send.at[level], silu_recv.at[level], sems, used, partner),
            remote(all_send.at[level], all_recv.at[level], sems, used + 1, partner),
        ]
        used += 2
        for copy in copies:
            copy.wait()
        silu_send[level + 1] = silu_send[level] + silu_recv[level]
        all_send[level + 1] = all_send[level] + all_recv[level]
    silu_out[...] = silu_send[len(across)]
    all_out[...] = all_send[len(across)]


def mod_backward(mod_grads, conditioning, ada_weight, group, every, data_size, tensor_size):
    _, seqs, feat = mod_grads.shape
    cols = ada_weight.shape[2]
    levels = tensor_size.bit_length() - 1
    group_size, every_size = group.shape[-1], every.shape[-1]
    vmem = pl.BlockSpec(memory_space=pltpu.VMEM)

    def wide(*shape):
        return pltpu.VMEM(shape, jnp.float32)

    return pl.pallas_call(
        functools.partial(mod_backward_kernel, data_size, tensor_size),
        out_shape=[
            jax.ShapeDtypeStruct(ada_weight.shape, jnp.float32),
            jax.ShapeDtypeStruct((2, cols), jnp.float32),
            jax.ShapeDtypeStruct((seqs, feat), jnp.float32),
            jax.ShapeDtypeStruct(group.shape, jnp.float32),
            jax.ShapeDtypeStruct(every.shape, jnp.float32),
        ],
        in_specs=[vmem] * 5,
        out_specs=[vmem] * 5,
        scratch_shapes=[
            wide(tensor_size, data_size, 2 * seqs, cols),
            wide(data_size, 2 * seqs, cols),
            wide(data_size, 2 * seqs, cols),
            wide(data_size, 2 * seqs, cols),
            wide(*group.shape),
            wide(*every.shape),
            wide(1, group_size),
            wide(1, every_size),
            wide(data_size, seqs, feat),
            wide(data_size, seqs, feat),
            wide(levels + 1, seqs, feat),
            wide(levels, seqs, feat),
            wide(levels + 1, *every.shape),
            wide(levels, *every.shape),
            pltpu.SemaphoreType.DMA((2, 1 + 6 * (data_size - 1) + 2 * levels)),
        ],
        compiler_params=pltpu.CompilerParams(
            collective_id=1, has_side_effects=True, vmem_limit_bytes=48 << 20
        ),
        name="mod_backward",
    )(mod_grads, conditioning, ada_weight, group, every)


def swap_pairs(size, distance):
    return [(index, index ^ distance) for index in range(size)]


def tensor_sum(own_part, other_part, tensor_size):
    total = own_part + lax.ppermute(other_part, "tensor", swap_pairs(tensor_size, 1))
    distance = 2
    while distance < tensor_size:
        total = total + lax.ppermute(total, "tensor", swap_pairs(tensor_size, distance))
        distance *= 2
    return total


def share(own_rows, tensor_size):
    other = lax.ppermute(own_rows, "tensor", swap_pairs(tensor_size, 1))
    return jnp.stack([own_rows, other])


def ring_order(mesh):
    size = mesh.shape["dp"]
    fallback = list(range(0, size, 2)) + list(range(1, size, 2))[::-1]
    axis = list(mesh.axis_names).index("dp")
    devices = mesh.devices
    line = [devices[(slice(None),) * axis + (index,)].flatten()[0] for index in range(size)]
    coords = [getattr(device, "coords", None) for device in line]
    if any(place is None for place in coords):
        return fallback
    near = [
        [
            other
            for other in range(size)
            if sum(abs(a - b) for a, b in zip(coords[index], coords[other])) == 1
        ]
        for index in range(size)
    ]
    path, seen, budget = [0], {0}, [200000]

    def extend():
        budget[0] -= 1
        if budget[0] < 0:
            return False
        if len(path) == size:
            return path[0] in near[path[-1]]
        choices = [index for index in near[path[-1]] if index not in seen]
        choices.sort(key=lambda index: (sum(o not in seen for o in near[index]), index))
        for index in choices:
            path.append(index)
            seen.add(index)
            if extend():
                return True
            path.pop()
            seen.remove(index)
        return False

    return path if extend() else fallback


def ring_scatter(grad, order):
    size = len(order)
    ahead = [(order[index], order[(index + 1) % size]) for index in range(size)]
    back = [(second, first) for first, second in ahead]
    place = jnp.array([order.index(index) for index in range(size)], jnp.int32)[lax.axis_index("dp")]
    blocks = jnp.array(order, jnp.int32)
    halves = grad.reshape(size, 2, grad.shape[0] // (2 * size), grad.shape[1])

    def block(offset, way):
        index = blocks[(place + offset) % size]
        return lax.dynamic_slice(
            halves, (index, way, 0, 0), (1, 1) + halves.shape[2:]
        ).reshape(halves.shape[2:])

    first, second = block(size - 1, 0), block(1, 1)
    for step in range(size - 1):
        first = lax.ppermute(first, "dp", ahead) + block(2 * size - 2 - step, 0)
        second = lax.ppermute(second, "dp", back) + block(2 + step, 1)
    return jnp.concatenate([first, second], axis=0)


def on_device(
    order,
    tensor_size,
    input_img,
    input_txt,
    conditioning,
    ada_weight,
    ada_bias,
    qkv_weight,
    qkv_bias,
    norm_gain,
    proj_weight,
    proj_bias,
    up_weight,
    up_bias,
    down_weight,
    down_bias,
    cotangent_img,
    cotangent_txt,
):
    data_size = len(order)
    seqs, _, feat = input_img.shape
    core = lax.axis_index("tensor") % 2
    reals = (input_img.shape[1] // 2, input_txt.shape[1] // 2)

    def split_rows(array):
        half = array.shape[1] // 2
        pad = -half % ROW_TILE
        lower, upper = (
            jnp.pad(part, ((0, 0), (0, pad), (0, 0))) for part in (array[:, :half], array[:, half:])
        )
        first = core == 0
        return jnp.stack([jnp.where(first, lower, upper), jnp.where(first, upper, lower)])

    def join_rows(halves, real):
        own, other = halves.astype(jnp.bfloat16)
        first = core == 0
        lower, upper = jnp.where(first, own, other), jnp.where(first, other, own)
        return jnp.concatenate([lower[:, :real], upper[:, :real]], axis=1)

    modulate = mod_forward(
        conditioning, ada_weight, ada_bias, seqs, feat, data_size, tensor_size
    )
    piece = [
        [modulate[stream * 6 + index][:, None, :] for index in range(6)] for stream in range(2)
    ]

    inputs = [split_rows(input_img), split_rows(input_txt)]
    cotangents = [split_rows(cotangent_img), split_rows(cotangent_txt)]
    shapes = [array.shape for array in inputs]
    gain_pair = jnp.concatenate([norm_gain, norm_gain], axis=2)

    hidden1, packed, stats1 = [], [], []
    weights_in = [qkv_weight[stream].reshape(feat, -1) for stream in range(2)]
    for stream in range(2):
        normed, inverse = layer_norm(inputs[stream].astype(jnp.float32))
        hidden = (normed * (1.0 + piece[stream][1]) + piece[stream][0]).astype(jnp.bfloat16)
        hidden = hidden.reshape(-1, feat)
        flat = dot_plain(hidden, weights_in[stream]) + qkv_bias[stream].reshape(-1).astype(
            jnp.float32
        )
        hidden1.append(hidden)
        packed.append(flat.reshape(shapes[stream][:3] + (-1,)))
        stats1.append((normed[0], inverse[0]))
    attn = attn_forward(gain_pair, packed[0], packed[1], reals[1])
    local = attn[0].shape[3]

    down_rings, up_rings = [None, None], [None, None]
    state = [None, None]
    hidden_sums, mlp_sums = [None, None], [None, None]
    up_bias_sums = [None, None]
    for stream in (1, 0):
        rows = attn[stream].reshape(2, -1, local)
        other_part = dot_plain(rows[1], proj_weight[stream])
        own_part = dot_plain(rows[0], proj_weight[stream])
        total = tensor_sum(own_part, other_part, tensor_size).reshape(shapes[stream][1:])
        branch = total + proj_bias[stream]
        residual = inputs[stream][0].astype(jnp.float32) + piece[stream][2] * branch
        normed, inverse = layer_norm(residual)
        hidden = share(normed, tensor_size) * (1.0 + piece[stream][4]) + piece[stream][3]
        hidden = hidden.astype(jnp.bfloat16).reshape(-1, feat)
        upward = dot_plain(hidden, up_weight[stream]) + up_bias[stream].astype(jnp.float32)
        active, slope = gelu_both(upward)
        active = active.astype(jnp.bfloat16)
        grad_mlp = cotangents[stream].astype(jnp.float32) * piece[stream][5]
        grad_mlp_low = grad_mlp.astype(jnp.bfloat16).reshape(-1, feat)
        grad_up = dot_right_t(grad_mlp_low, down_weight[stream]) * slope
        grad_up_low = grad_up.astype(jnp.bfloat16)
        up_bias_sums[stream] = jnp.sum(grad_up, axis=0)
        half = grad_up_low.shape[0] // 2
        down_rings[stream] = ring_scatter(dot_left_t(grad_mlp_low, active), order)
        up_rings[stream] = ring_scatter(dot_left_t(hidden, grad_up_low), order)
        other_part = dot_right_t(grad_up_low[half:], up_weight[stream])
        own_part = dot_right_t(grad_up_low[:half], up_weight[stream])
        hidden_sums[stream] = tensor_sum(own_part, other_part, tensor_size)
        other_part = dot_plain(active[half:], down_weight[stream])
        own_part = dot_plain(active[:half], down_weight[stream])
        mlp_sums[stream] = tensor_sum(own_part, other_part, tensor_size)
        state[stream] = (branch, normed, inverse, jnp.sum(grad_mlp[0], axis=(0, 1)))

    grad_attn, proj_rings, proj_sums, resid_grads, mod_grads = (
        [None, None],
        [None, None],
        [None, None],
        [None, None],
        [None, None],
    )
    outputs = [None, None]
    for stream in (1, 0):
        branch, normed, inverse, _ = state[stream]
        grad_out = cotangents[stream][0].astype(jnp.float32)
        grad_hidden = hidden_sums[stream].reshape(normed.shape)
        through = norm_back(grad_hidden * (1.0 + piece[stream][4]), normed, inverse)
        grad_resid = grad_out + through
        grad_branch = share(grad_resid, tensor_size) * piece[stream][2]
        branch_low = grad_branch.astype(jnp.bfloat16).reshape(-1, feat)
        grad_attn[stream] = (
            dot_right_t(branch_low, proj_weight[stream])
            .astype(jnp.bfloat16)
            .reshape(attn[stream].shape)
        )
        proj_rings[stream] = ring_scatter(
            dot_left_t(branch_low, attn[stream].reshape(-1, local)), order
        )
        proj_sums[stream] = jnp.sum(grad_resid * piece[stream][2], axis=(0, 1))
        resid_grads[stream] = through
        mod_grads[stream] = [
            None,
            None,
            jnp.sum(grad_resid * branch, axis=1),
            jnp.sum(grad_hidden, axis=1),
            jnp.sum(grad_hidden * normed, axis=1),
            None,
        ]
    grad_packed = attn_backward(gain_pair, packed[0], packed[1], grad_attn[0], grad_attn[1], reals[1])
    qkv_bias_sums = jnp.sum(grad_packed[2], axis=0)
    gain_sums = jnp.sum(grad_packed[3], axis=0)
    head_dim = norm_gain.shape[2]
    gain_sums = gain_sums[:, :head_dim] + gain_sums[:, head_dim:]
    qkv_rings, first_sums = [None, None], [None, None]
    for stream in (1, 0):
        packed_low = grad_packed[stream].reshape(-1, 3 * local)
        half = packed_low.shape[0] // 2
        other_part = dot_right_t(packed_low[half:], weights_in[stream])
        own_part = dot_right_t(packed_low[:half], weights_in[stream])
        first_sums[stream] = tensor_sum(own_part, other_part, tensor_size)
        qkv_rings[stream] = ring_scatter(dot_left_t(hidden1[stream], packed_low), order)

    grad_inputs = [None, None]
    for stream in (1, 0):
        branch = state[stream][0]
        grad_out = cotangents[stream][0].astype(jnp.float32)
        mlp_out = mlp_sums[stream].reshape(branch.shape) + down_bias[stream]
        added = piece[stream][2] * branch + piece[stream][5] * mlp_out
        outputs[stream] = join_rows(
            inputs[stream].astype(jnp.float32) + share(added, tensor_size), reals[stream]
        )
        mod_grads[stream][5] = jnp.sum(grad_out * mlp_out, axis=1)
        normed, inverse = stats1[stream]
        grad_hidden = first_sums[stream].reshape(normed.shape)
        added = resid_grads[stream] + norm_back(
            grad_hidden * (1.0 + piece[stream][1]), normed, inverse
        )
        grad_inputs[stream] = join_rows(
            cotangents[stream].astype(jnp.float32) + share(added, tensor_size), reals[stream]
        )
        mod_grads[stream][0] = jnp.sum(grad_hidden, axis=1)
        mod_grads[stream][1] = jnp.sum(grad_hidden * normed, axis=1)

    row_share = 2.0 / tensor_size
    parts = (
        (qkv_bias_sums, jnp.stack(up_bias_sums)),
        (
            gain_sums,
            jnp.stack(proj_sums) * row_share,
            jnp.stack([state[0][3], state[1][3]]) * row_share,
        ),
    )
    vectors = [
        jnp.concatenate([each.reshape(-1) for each in group]).reshape(data_size, 1, -1)
        for group in parts
    ]
    grad_ada_weight, grad_ada_bias, silu_rows, *vectors = mod_backward(
        jnp.stack(mod_grads[0] + mod_grads[1]),
        conditioning,
        ada_weight,
        vectors[0],
        vectors[1],
        data_size,
        tensor_size,
    )
    sums = []
    for group, vector in zip(parts, vectors):
        flat, start = vector.reshape(-1), 0
        for each in group:
            sums.append(flat[start : start + each.size].reshape(each.shape))
            start += each.size
    qkv_bias_sums, up_bias_sums, gain_sums, proj_sums, down_sums = sums
    own_cond = lax.dynamic_slice_in_dim(
        conditioning, lax.axis_index("dp") * seqs, seqs, axis=0
    ).astype(jnp.float32)
    own_sig = jax.nn.sigmoid(own_cond)
    grad_conditioning = silu_rows * own_sig * (1.0 + own_cond * (1.0 - own_sig))
    return (
        outputs[0],
        outputs[1],
        grad_inputs[0],
        grad_inputs[1],
        grad_conditioning,
        grad_ada_weight,
        grad_ada_bias,
        jnp.stack([ring.reshape(ring.shape[0], 3, -1) for ring in qkv_rings]),
        qkv_bias_sums.reshape(2, 3, -1),
        gain_sums.reshape(norm_gain.shape),
        jnp.stack([ring.T for ring in proj_rings]),
        proj_sums,
        jnp.stack(up_rings),
        up_bias_sums,
        jnp.stack([ring.T for ring in down_rings]),
        down_sums,
    )


def solution(mesh):
    in_specs = (
        P("dp", None, None),
        P("dp", None, None),
        P(),
        P(None, None, ("dp", "tensor")),
        P(None, ("dp", "tensor")),
        P(None, None, None, "tensor"),
        P(None, None, "tensor"),
        P(),
        P(None, "tensor", None),
        P(),
        P(None, None, "tensor"),
        P(None, "tensor"),
        P(None, "tensor", None),
        P(),
        P("dp", None, None),
        P("dp", None, None),
    )
    out_specs = (
        P("dp", None, None),
        P("dp", None, None),
        P("dp", None, None),
        P("dp", None, None),
        P("dp", None),
        P(None, None, ("dp", "tensor")),
        P(None, ("dp", "tensor")),
        P(None, "dp", None, "tensor"),
        P(None, None, "tensor"),
        P(),
        P(None, "tensor", "dp"),
        P(),
        P(None, "dp", "tensor"),
        P(None, "tensor"),
        P(None, "tensor", "dp"),
        P(),
    )
    return jax.shard_map(
        functools.partial(on_device, ring_order(mesh), mesh.shape["tensor"]),
        mesh=mesh,
        in_specs=in_specs,
        out_specs=out_specs,
        check_vma=False,
    )
```

```python
import functools

import jax
import jax.numpy as jnp
from jax import lax
from jax.experimental import pallas as pl
from jax.experimental.pallas import tpu as pltpu
from jax.sharding import PartitionSpec as P

epsilon = 1e-06
GELU_C = 0.7978845608028654
GELU_A = 0.044715
ROW_TILE = 16
NEG = -1e30


def dot_plain(first_op, second_op):
    return jnp.dot(first_op, second_op, preferred_element_type=jnp.float32)


def dot_right_t(first_op, second_op):
    return lax.dot_general(
        first_op, second_op, (((1,), (1,)), ((), ())), preferred_element_type=jnp.float32
    )


def dot_left_t(first_op, second_op):
    return lax.dot_general(
        first_op, second_op, (((0,), (0,)), ((), ())), preferred_element_type=jnp.float32
    )


def layer_norm(values):
    center = values - jnp.mean(values, axis=-1, keepdims=True)
    inverse = lax.rsqrt(jnp.mean(center * center, axis=-1, keepdims=True) + epsilon)
    return (center * inverse, inverse)


def norm_back(grad_normed, normed, inverse):
    return inverse * (
        grad_normed
        - jnp.mean(grad_normed, axis=-1, keepdims=True)
        - normed * jnp.mean(grad_normed * normed, axis=-1, keepdims=True)
    )


def gelu_both(values):
    inner = jnp.tanh(GELU_C * (values + GELU_A * values * values * values))
    active = 0.5 * values * (1.0 + inner)
    slope = 0.5 * (1.0 + inner) + 0.5 * values * (1.0 - inner * inner) * GELU_C * (
        1.0 + 3.0 * GELU_A * values * values
    )
    return active, slope


def head_norm(values, gain):
    head_dim = values.shape[1] // 2
    lower = lax.broadcasted_iota(jnp.int32, values.shape, 1) < head_dim
    square = values * values
    first = jnp.sum(jnp.where(lower, square, 0.0), axis=-1, keepdims=True) / head_dim
    second = jnp.sum(jnp.where(lower, 0.0, square), axis=-1, keepdims=True) / head_dim
    factor = jnp.where(lower, lax.rsqrt(first + epsilon), lax.rsqrt(second + epsilon))
    return values * factor * gain, factor


def rows_of(img_ref, txt_ref, cols):
    return jnp.concatenate(
        [img_ref[0, 0, :, cols], img_ref[1, 0, :, cols], txt_ref[0, 0, :, cols], txt_ref[1, 0, :, cols]],
        axis=0,
    )


def put_rows(img_ref, txt_ref, cols, values):
    img, txt = img_ref.shape[2], txt_ref.shape[2]
    img_ref[0, 0, :, cols] = values[:img]
    img_ref[1, 0, :, cols] = values[img : 2 * img]
    txt_ref[0, 0, :, cols] = values[2 * img : 2 * img + txt]
    txt_ref[1, 0, :, cols] = values[2 * img + txt :]


def gain_rows(gain_ref, which, img, txt):
    width = gain_ref.shape[2]
    return jnp.concatenate(
        [
            jnp.broadcast_to(gain_ref[0, which : which + 1, :], (2 * img, width)),
            jnp.broadcast_to(gain_ref[1, which : which + 1, :], (2 * txt, width)),
        ],
        axis=0,
    )


def key_bias(img, txt, real):
    where = lax.broadcasted_iota(jnp.int32, (1, 2 * (img + txt)), 1)
    first = where - 2 * img
    gone = ((first >= real) & (first < txt)) | (first >= txt + real)
    return jnp.where(gone, NEG, 0.0).astype(jnp.float32)


def probs(q_head, k_low, bias):
    scores = dot_right_t(q_head, k_low) + bias
    top = jnp.max(scores, axis=-1, keepdims=True)
    weights = jnp.exp(scores - top)
    return weights * (1.0 / jnp.sum(weights, axis=-1, keepdims=True))


def attn_forward_kernel(real, gain_ref, *refs):
    raw_refs, (out_img_ref, out_txt_ref) = (refs[:3], refs[3:6]), refs[6:]
    img, txt = out_img_ref.shape[2], out_txt_ref.shape[2]
    local = out_img_ref.shape[3]
    pair = gain_ref.shape[2]
    q_gain, k_gain = gain_rows(gain_ref, 0, img, txt), gain_rows(gain_ref, 1, img, txt)
    bias = key_bias(img, txt, real)
    scale = (pair // 2) ** (-0.5)
    for start in range(0, local, pair):
        q_raw, k_raw, v_raw = (
            rows_of(raw_refs[0][part], raw_refs[1][part], slice(start, start + pair))
            for part in range(3)
        )
        q_low = head_norm(q_raw, q_gain)[0].astype(jnp.bfloat16) * jnp.bfloat16(scale)
        k_low = head_norm(k_raw, k_gain)[0].astype(jnp.bfloat16)
        v_low = v_raw.astype(jnp.bfloat16)
        lower = lax.broadcasted_iota(jnp.int32, q_raw.shape, 1) < pair // 2
        results = []
        for head in range(2):
            mine = lower if head == 0 else jnp.logical_not(lower)
            q_head = jnp.where(mine, q_low, jnp.bfloat16(0))
            results.append(dot_plain(probs(q_head, k_low, bias).astype(jnp.bfloat16), v_low))
        out = jnp.where(lower, results[0], results[1]).astype(jnp.bfloat16)
        put_rows(out_img_ref, out_txt_ref, slice(start, start + pair), out)


def attn_backward_kernel(real, gain_ref, *refs):
    raw_refs = (refs[:3], refs[3:6])
    d_img_ref, d_txt_ref, o_img_ref, o_txt_ref, bias_ref, dgain_ref = refs[6:]
    img, txt = d_img_ref.shape[2], d_txt_ref.shape[2]
    local = d_img_ref.shape[3]
    pair = gain_ref.shape[2]
    head_dim = pair // 2
    q_gain, k_gain = gain_rows(gain_ref, 0, img, txt), gain_rows(gain_ref, 1, img, txt)
    bias = key_bias(img, txt, real)
    scale = head_dim ** (-0.5)
    gain_sums = [[None, None], [None, None]]
    for start in range(0, local, pair):
        q_raw, k_raw, v_raw = (
            rows_of(raw_refs[0][part], raw_refs[1][part], slice(start, start + pair))
            for part in range(3)
        )
        q_wide, q_factor = head_norm(q_raw, q_gain)
        k_wide, k_factor = head_norm(k_raw, k_gain)
        q_low = q_wide.astype(jnp.bfloat16) * jnp.bfloat16(scale)
        k_low = k_wide.astype(jnp.bfloat16)
        v_low = v_raw.astype(jnp.bfloat16)
        grad_out = rows_of(d_img_ref, d_txt_ref, slice(start, start + pair))
        lower = lax.broadcasted_iota(jnp.int32, q_raw.shape, 1) < head_dim
        parts = []
        for head in range(2):
            mine = lower if head == 0 else jnp.logical_not(lower)
            prob = probs(jnp.where(mine, q_low, jnp.bfloat16(0)), k_low, bias)
            grad_v = dot_left_t(prob.astype(jnp.bfloat16), grad_out)
            grad_prob = dot_right_t(jnp.where(mine, grad_out, jnp.bfloat16(0)), v_low)
            delta = jnp.sum(prob * grad_prob, axis=-1, keepdims=True)
            grad_scores = (prob * (grad_prob - delta)).astype(jnp.bfloat16)
            parts.append((dot_plain(grad_scores, k_low), dot_left_t(grad_scores, q_low), grad_v))
        grad_qn = jnp.where(lower, parts[0][0], parts[1][0]) * scale
        grad_kn = jnp.where(lower, parts[0][1], parts[1][1])
        grad_vn = jnp.where(lower, parts[0][2], parts[1][2])

        def raw_grad(grad_normed, raw, factor, gain, which):
            gained = grad_normed * gain
            product = gained * raw
            first = jnp.sum(jnp.where(lower, product, 0.0), axis=-1, keepdims=True) / head_dim
            second = jnp.sum(jnp.where(lower, 0.0, product), axis=-1, keepdims=True) / head_dim
            inner = jnp.where(lower, first, second)
            terms = grad_normed * raw * factor
            for stream, rows in enumerate((slice(0, 2 * img), slice(2 * img, 2 * (img + txt)))):
                total = jnp.sum(terms[rows], axis=0, keepdims=True)
                old = gain_sums[stream][which]
                gain_sums[stream][which] = total if old is None else old + total
            return factor * gained - raw * (factor * factor * factor) * inner

        grads = (
            raw_grad(grad_qn, q_raw, q_factor, q_gain, 0),
            raw_grad(grad_kn, k_raw, k_factor, k_gain, 1),
            grad_vn,
        )
        for part, grad in enumerate(grads):
            cols = slice(part * local + start, part * local + start + pair)
            bias_ref[0, 0:1, cols] = jnp.sum(grad[: 2 * img], axis=0, keepdims=True)
            bias_ref[0, 1:2, cols] = jnp.sum(grad[2 * img :], axis=0, keepdims=True)
            put_rows(o_img_ref, o_txt_ref, cols, grad.astype(jnp.bfloat16))
    for stream in range(2):
        for which in range(2):
            row = stream * 2 + which
            dgain_ref[0, row : row + 1, :] = gain_sums[stream][which]


def block_of(array):
    shape = array.shape
    return pl.BlockSpec((shape[0], 1) + shape[2:], lambda seq: (0, seq, 0, 0))


def whole_of(array):
    return pl.BlockSpec(array.shape, lambda seq: (0,) * array.ndim)


def attn_forward(gain_pair, raw_img, raw_txt, real):
    seqs, local = raw_img[0].shape[1], raw_img[0].shape[3]
    outs = [jax.ShapeDtypeStruct(raw[0].shape, jnp.bfloat16) for raw in (raw_img, raw_txt)]
    rows = 2 * (raw_img[0].shape[2] + raw_txt[0].shape[2])
    return pl.pallas_call(
        functools.partial(attn_forward_kernel, real),
        grid=(seqs,),
        out_shape=outs,
        in_specs=[whole_of(gain_pair)] + [block_of(raw) for raw in raw_img + raw_txt],
        out_specs=[block_of(out) for out in outs],
        compiler_params=pltpu.CompilerParams(vmem_limit_bytes=48 << 20),
        cost_estimate=pl.CostEstimate(
            flops=seqs * rows * rows * local * 4,
            bytes_accessed=seqs * rows * local * 14,
            transcendentals=seqs * rows * rows * (local // 64),
        ),
        name="attn_forward",
    )(gain_pair, *raw_img, *raw_txt)


def attn_backward(gain_pair, raw_img, raw_txt, grad_img, grad_txt, real):
    seqs, local = raw_img[0].shape[1], raw_img[0].shape[3]
    outs = [
        jax.ShapeDtypeStruct(raw_img[0].shape[:3] + (3 * local,), jnp.bfloat16),
        jax.ShapeDtypeStruct(raw_txt[0].shape[:3] + (3 * local,), jnp.bfloat16),
        jax.ShapeDtypeStruct((seqs, 2, 3 * local), jnp.float32),
        jax.ShapeDtypeStruct((seqs, 4, gain_pair.shape[2]), jnp.float32),
    ]
    rows = 2 * (raw_img[0].shape[2] + raw_txt[0].shape[2])
    return pl.pallas_call(
        functools.partial(attn_backward_kernel, real),
        grid=(seqs,),
        out_shape=outs,
        in_specs=[whole_of(gain_pair)]
        + [block_of(each) for each in raw_img + raw_txt + [grad_img, grad_txt]],
        out_specs=[
            block_of(outs[0]),
            block_of(outs[1]),
            pl.BlockSpec((1, 2, 3 * local), lambda seq: (seq, 0, 0)),
            pl.BlockSpec((1, 4, gain_pair.shape[2]), lambda seq: (seq, 0, 0)),
        ],
        compiler_params=pltpu.CompilerParams(vmem_limit_bytes=56 << 20),
        cost_estimate=pl.CostEstimate(
            flops=seqs * rows * rows * local * 10,
            bytes_accessed=seqs * rows * local * 20,
            transcendentals=seqs * rows * rows * (local // 64),
        ),
        name="attn_backward",
    )(gain_pair, *raw_img, *raw_txt, grad_img, grad_txt)


def xor_index(index, distance):
    return index + distance - 2 * distance * ((index // distance) % 2)


def peers_of(data_size, tensor_size):
    row, col = lax.axis_index("dp"), lax.axis_index("tensor")
    around = [(lax.rem(row + step, data_size), col) for step in range(1, data_size)]
    across = []
    distance = 1
    while distance < tensor_size:
        across.append((row, xor_index(col, distance)))
        distance *= 2
    return row, col, around, across


def greet(partners):
    barrier = pltpu.get_barrier_semaphore()
    for partner in partners:
        pl.semaphore_signal(barrier, inc=1, device_id=partner, device_id_type=pl.DeviceIdType.MESH)
    pl.semaphore_wait(barrier, len(partners))


def remote(source, target, sems, index, partner):
    copy = pltpu.make_async_remote_copy(
        src_ref=source,
        dst_ref=target,
        send_sem=sems.at[0, index],
        recv_sem=sems.at[1, index],
        device_id=partner,
        device_id_type=pl.DeviceIdType.MESH,
    )
    copy.start()
    return copy


def silu_of(cond_ref):
    wide = cond_ref[...].astype(jnp.float32)
    return (wide * (1.0 / (1.0 + jnp.exp(-wide)))).astype(jnp.bfloat16)


def mod_forward_kernel(
    data_size, tensor_size, cond_ref, weight_ref, bias_ref, out_ref, outgoing, blocks, sems
):
    row, col, around, across = peers_of(data_size, tensor_size)
    seqs, feat = out_ref.shape[1], out_ref.shape[2]
    silu_cond = silu_of(cond_ref)
    for stream in range(2):
        values = dot_right_t(silu_cond, weight_ref[stream]) + bias_ref[stream : stream + 1].astype(
            jnp.float32
        )
        for index in range(data_size):
            outgoing[index, stream * seqs : (stream + 1) * seqs] = values[
                index * seqs : (index + 1) * seqs
            ]
    blocks[col, row] = outgoing[row]
    greet(around + across)
    copies = [
        remote(outgoing.at[partner[0]], blocks.at[col, row], sems, index, partner)
        for index, partner in enumerate(around)
    ]
    for copy in copies:
        copy.wait()
    held, used = [0], len(around)
    for level in reversed(range(len(across))):
        distance = 1 << level
        copies = []
        for offset in held:
            index = col
            for bit in range(len(across)):
                if offset >> bit & 1:
                    index = xor_index(index, 1 << bit)
            copies.append(remote(blocks.at[index], blocks.at[index], sems, used, across[level]))
            used += 1
        for copy in copies:
            copy.wait()
        held = held + [offset | distance for offset in held]
    for stream in range(2):
        full = jnp.concatenate(
            [
                blocks[second, first, stream * seqs : (stream + 1) * seqs]
                for first in range(data_size)
                for second in range(tensor_size)
            ],
            axis=1,
        )
        for index in range(6):
            out_ref[stream * 6 + index] = full[:, index * feat : (index + 1) * feat]


def mod_forward(conditioning, ada_weight, ada_bias, seqs, feat, data_size, tensor_size):
    cols = ada_weight.shape[1]
    vmem = pl.BlockSpec(memory_space=pltpu.VMEM)
    return pl.pallas_call(
        functools.partial(mod_forward_kernel, data_size, tensor_size),
        out_shape=jax.ShapeDtypeStruct((12, seqs, feat), jnp.float32),
        in_specs=[vmem] * 3,
        out_specs=vmem,
        scratch_shapes=[
            pltpu.VMEM((data_size, 2 * seqs, cols), jnp.float32),
            pltpu.VMEM((tensor_size, data_size, 2 * seqs, cols), jnp.float32),
            pltpu.SemaphoreType.DMA((2, data_size + tensor_size)),
        ],
        compiler_params=pltpu.CompilerParams(
            collective_id=0, has_side_effects=True, vmem_limit_bytes=32 << 20
        ),
        name="mod_forward",
    )(conditioning, ada_weight, ada_bias)


def mod_backward_kernel(
    data_size,
    tensor_size,
    mod_ref,
    cond_ref,
    weight_ref,
    *refs,
):
    refs = list(refs)

    def take(number):
        taken = refs[:number]
        del refs[:number]
        return taken

    group_refs, all_refs = take(2), take(3)
    weight_out, bias_out, silu_out = take(3)
    group_outs, all_outs = take(2), take(3)
    blocks, core_in, outgoing, cols_in, lines, lines_in, lines_own, lines_all = take(8)
    silu_blocks, silu_in, silu_send, silu_recv, all_send, all_recv, sems = take(7)
    row, col, around, across = peers_of(data_size, tensor_size)
    seqs, feat = silu_out.shape
    cols = bias_out.shape[1]
    for stream in range(2):
        full = jnp.concatenate([mod_ref[stream * 6 + index] for index in range(6)], axis=1)
        for first in range(data_size):
            for second in range(tensor_size):
                start = (first * tensor_size + second) * cols
                blocks[second, first, stream * seqs : (stream + 1) * seqs] = full[
                    :, start : start + cols
                ]
    silu_cond = silu_of(cond_ref)
    half = lines.shape[1] // 2
    width = lines.shape[2]

    def line_up(sources):
        padded = [
            jnp.pad(ref[...], ((0, 0), (0, feat - ref.shape[1]))) for ref in sources
        ]
        short = half - sum(ref.shape[0] for ref in sources)
        if short:
            padded.append(jnp.zeros((short, feat), jnp.float32))
        return jnp.concatenate(padded, axis=0)

    every_line = jnp.concatenate([line_up(group_refs), line_up(all_refs)], axis=0)
    for index in range(data_size):
        lines[index] = every_line[:, index * width : (index + 1) * width]
    greet(around + across)

    used = 0
    copy = remote(blocks.at[xor_index(col, 1)], core_in, sems, used, across[0])
    used += 1
    copy.wait()
    for first in range(data_size):
        outgoing[first] = blocks[col, first] + core_in[first]

    cols_in[row] = outgoing[row]
    lines_in[row] = lines[row]
    copies = []
    for partner in around:
        for source, target in ((lines, lines_in), (outgoing, cols_in)):
            copies.append(
                remote(source.at[partner[0]], target.at[row], sems, used, partner)
            )
            used += 1
    for copy in copies:
        copy.wait()
    lines_own[...] = functools.reduce(jnp.add, [lines_in[index] for index in range(data_size)])
    low = []
    for stream in range(2):
        wide = jnp.concatenate(
            [cols_in[index, stream * seqs : (stream + 1) * seqs] for index in range(data_size)],
            axis=0,
        )
        bias_out[stream : stream + 1] = jnp.sum(wide, axis=0, keepdims=True)
        low.append(wide.astype(jnp.bfloat16))
    silu_grad = dot_plain(low[0], weight_ref[0]) + dot_plain(low[1], weight_ref[1])
    for index in range(data_size):
        silu_blocks[index] = silu_grad[index * seqs : (index + 1) * seqs]
    for stream in range(2):
        weight_out[stream] = dot_left_t(low[stream], silu_cond)

    silu_in[row] = silu_blocks[row]
    lines_all[row] = lines_own[...]
    copies = []
    for partner in around:
        for source, target in (
            (silu_blocks.at[partner[0]], silu_in.at[row]),
            (lines_own, lines_all.at[row]),
        ):
            copies.append(remote(source, target, sems, used, partner))
            used += 1
    for copy in copies:
        copy.wait()
    silu_send[0] = functools.reduce(jnp.add, [silu_in[index] for index in range(data_size)])
    every_line = jnp.concatenate([lines_all[index] for index in range(data_size)], axis=1)
    all_send[0] = every_line[half:]

    def hand_out(values, targets):
        start = 0
        for target in targets:
            count, size = target.shape
            target[...] = values[start : start + count, :size]
            start += count

    hand_out(every_line[:half], group_outs)

    for level, partner in enumerate(across):
        copies = [
            remote(silu_send.at[level], silu_recv.at[level], sems, used, partner),
            remote(all_send.at[level], all_recv.at[level], sems, used + 1, partner),
        ]
        used += 2
        for copy in copies:
            copy.wait()
        silu_send[level + 1] = silu_send[level] + silu_recv[level]
        all_send[level + 1] = all_send[level] + all_recv[level]
    silu_out[...] = silu_send[len(across)]
    hand_out(all_send[len(across)], all_outs)


def mod_backward(mod_grads, conditioning, ada_weight, group, every, data_size, tensor_size):
    _, seqs, feat = mod_grads.shape
    cols = ada_weight.shape[1]
    levels = tensor_size.bit_length() - 1
    vmem = pl.BlockSpec(memory_space=pltpu.VMEM)
    lines, width = 16, feat // data_size

    def wide(*shape):
        return pltpu.VMEM(shape, jnp.float32)

    return pl.pallas_call(
        functools.partial(mod_backward_kernel, data_size, tensor_size),
        out_shape=[
            jax.ShapeDtypeStruct(ada_weight.shape, jnp.float32),
            jax.ShapeDtypeStruct((2, cols), jnp.float32),
            jax.ShapeDtypeStruct((seqs, feat), jnp.float32),
        ]
        + [jax.ShapeDtypeStruct(each.shape, jnp.float32) for each in group + every],
        in_specs=[vmem] * (3 + len(group) + len(every)),
        out_specs=[vmem] * (3 + len(group) + len(every)),
        scratch_shapes=[
            wide(tensor_size, data_size, 2 * seqs, cols),
            wide(data_size, 2 * seqs, cols),
            wide(data_size, 2 * seqs, cols),
            wide(data_size, 2 * seqs, cols),
            wide(data_size, lines, width),
            wide(data_size, lines, width),
            wide(lines, width),
            wide(data_size, lines, width),
            wide(data_size, seqs, feat),
            wide(data_size, seqs, feat),
            wide(levels + 1, seqs, feat),
            wide(levels, seqs, feat),
            wide(levels + 1, lines // 2, feat),
            wide(levels, lines // 2, feat),
            pltpu.SemaphoreType.DMA((2, 1 + 4 * (data_size - 1) + 2 * levels)),
        ],
        compiler_params=pltpu.CompilerParams(
            collective_id=1, has_side_effects=True, vmem_limit_bytes=48 << 20
        ),
        name="mod_backward",
    )(mod_grads, conditioning, ada_weight, *group, *every)


def swap_pairs(size, distance):
    return [(index, index ^ distance) for index in range(size)]


def core_sum(own_part, other_part, tensor_size):
    return own_part + lax.ppermute(other_part, "tensor", swap_pairs(tensor_size, 1))


def chip_sum(total, swapped, tensor_size):
    distance = 2
    while distance < tensor_size:
        if swapped is None or distance > 2:
            swapped = lax.ppermute(total, "tensor", swap_pairs(tensor_size, distance))
        total = total + swapped
        distance *= 2
    return total


def share(own_rows, tensor_size):
    other = lax.ppermute(own_rows, "tensor", swap_pairs(tensor_size, 1))
    return jnp.stack([own_rows, other])


def ring_order(mesh):
    size = mesh.shape["dp"]
    fallback = list(range(0, size, 2)) + list(range(1, size, 2))[::-1]
    axis = list(mesh.axis_names).index("dp")
    devices = mesh.devices
    line = [devices[(slice(None),) * axis + (index,)].flatten()[0] for index in range(size)]
    coords = [getattr(device, "coords", None) for device in line]
    if any(place is None for place in coords):
        return fallback
    near = [
        [
            other
            for other in range(size)
            if sum(abs(a - b) for a, b in zip(coords[index], coords[other])) == 1
        ]
        for index in range(size)
    ]
    path, seen, budget = [0], {0}, [200000]

    def extend():
        budget[0] -= 1
        if budget[0] < 0:
            return False
        if len(path) == size:
            return path[0] in near[path[-1]]
        choices = [index for index in near[path[-1]] if index not in seen]
        choices.sort(key=lambda index: (sum(o not in seen for o in near[index]), index))
        for index in choices:
            path.append(index)
            seen.add(index)
            if extend():
                return True
            path.pop()
            seen.remove(index)
        return False

    return path if extend() else fallback


def entry_of(table, index):
    value = jnp.int32(table[0])
    for place in range(1, len(table)):
        value = jnp.where(index == place, jnp.int32(table[place]), value)
    return value


def grad_ring_kernel(order, count, swaps, *refs):
    refs = list(refs)

    def take(number):
        taken = refs[:number]
        del refs[:number]
        return taken

    lefts, rights, gives = take(count), take(count), take(swaps)
    outs, gets = take(count), take(swaps)
    slots, terms, turned = take(count), take(count), take(count)
    (sems,) = take(1)
    swap_sems = refs[0] if swaps else None
    size = len(order)
    row, col = lax.axis_index("dp"), lax.axis_index("tensor")
    place = entry_of([order.index(index) for index in range(size)], row)
    after = entry_of(order, lax.rem(place + 1, size))
    before = entry_of(order, lax.rem(place + size - 1, size))
    targets = ((after, col), (before, col))
    half = slots[0].shape[2]
    facing = (row, xor_index(col, 2))

    greet(targets + ((facing,) if swaps else ()))
    swapped = [
        remote(gives[index], gets[index], swap_sems, index, facing) for index in range(swaps)
    ]
    for left, flipped in zip(lefts, turned):
        flipped[...] = left[...].T

    def work_out(which, way, index):
        start = pl.multiple_of((2 * index + way) * half, 8)
        terms[which][way] = dot_plain(turned[which][pl.ds(start, half), :], rights[which][...])

    def copy_of(which, way, step, source, target):
        return pltpu.make_async_remote_copy(
            src_ref=source,
            dst_ref=slots[which].at[way, target],
            send_sem=sems.at[0, which, way, step],
            recv_sem=sems.at[1, which, way, step],
            device_id=targets[way],
            device_id_type=pl.DeviceIdType.MESH,
        )

    chains = [(which, way) for which in range(count) for way in range(2)]
    for which, way in chains:
        work_out(which, way, (before, after)[way])
        slots[which][way, size - 1] = terms[which][way]
        copy_of(which, way, 0, slots[which].at[way, size - 1], 0).start()

    def arrive(which, way, step):
        copy_of(which, way, step, slots[which].at[way, step], step).wait_recv()

    def round_of(step, carry):
        ahead = entry_of(order, lax.rem(place + 2 * size - 2 - step, size))
        back = entry_of(order, lax.rem(place + 2 + step, size))
        for which, way in chains:
            work_out(which, way, (ahead, back)[way])
        for which, way in chains:
            arrive(which, way, step)
            slots[which][way, step] = slots[which][way, step] + terms[which][way]
            copy_of(which, way, step + 1, slots[which].at[way, step], step + 1).start()
        return carry

    lax.fori_loop(0, size - 2, round_of, 0)
    for which, way in chains:
        work_out(which, way, row)
    for which, way in chains:
        arrive(which, way, size - 2)
        total = slots[which][way, size - 2] + terms[which][way]
        parts, _, width = outs[which].shape
        for part in range(parts):
            outs[which][part, way * half : (way + 1) * half] = total[
                :, part * width : (part + 1) * width
            ]

    def sent(step, carry):
        for which, way in chains:
            copy_of(which, way, step, slots[which].at[way, size - 1], step).wait_send()
        return carry

    lax.fori_loop(0, size - 1, sent, 0)
    for copy in swapped:
        copy.wait()


def grad_ring(pairs, gives, order, collective_id, name):
    size, count, swaps = len(order), len(pairs), len(gives)
    vmem = pl.BlockSpec(memory_space=pltpu.VMEM)
    anywhere = pl.BlockSpec(memory_space=pl.ANY)
    halves = [(left.shape[1] // (2 * size), right.shape[1]) for left, right, _ in pairs]
    moved = sum(4 * 2 * (size - 1) * rows * cols for rows, cols in halves)
    results = pl.pallas_call(
        functools.partial(grad_ring_kernel, order, count, swaps),
        out_shape=[
            jax.ShapeDtypeStruct((parts, 2 * rows, cols // parts), jnp.float32)
            for (rows, cols), (_, _, parts) in zip(halves, pairs)
        ]
        + [jax.ShapeDtypeStruct(give.shape, give.dtype) for give in gives],
        in_specs=[vmem] * (2 * count) + [anywhere] * swaps,
        out_specs=[vmem] * count + [anywhere] * swaps,
        scratch_shapes=[pltpu.VMEM((2, size) + half, jnp.float32) for half in halves]
        + [pltpu.VMEM((2,) + half, jnp.float32) for half in halves]
        + [pltpu.VMEM(left.shape[::-1], left.dtype) for left, _, _ in pairs]
        + [pltpu.SemaphoreType.DMA((2, count, 2, size - 1))]
        + [pltpu.SemaphoreType.DMA((2, swaps))] * bool(swaps),
        compiler_params=pltpu.CompilerParams(
            collective_id=collective_id, has_side_effects=True, vmem_limit_bytes=58 << 20
        ),
        cost_estimate=pl.CostEstimate(flops=moved * 10000, bytes_accessed=moved, transcendentals=0),
        name=name,
    )(*[left for left, _, _ in pairs], *[right for _, right, _ in pairs], *gives)
    return results[:count], results[count:]


def on_device(
    order,
    tensor_size,
    input_img,
    input_txt,
    conditioning,
    ada_weight,
    ada_bias,
    qkv_weight,
    qkv_bias,
    norm_gain,
    proj_weight,
    proj_bias,
    up_weight,
    up_bias,
    down_weight,
    down_bias,
    cotangent_img,
    cotangent_txt,
):
    data_size = len(order)
    seqs, _, feat = input_img.shape
    core = lax.axis_index("tensor") % 2
    reals = (input_img.shape[1] // 2, input_txt.shape[1] // 2)

    def split_rows(array):
        half = array.shape[1] // 2
        pad = -half % ROW_TILE
        lower, upper = (
            jnp.pad(part, ((0, 0), (0, pad), (0, 0))) for part in (array[:, :half], array[:, half:])
        )
        first = core == 0
        return jnp.stack([jnp.where(first, lower, upper), jnp.where(first, upper, lower)])

    def join_rows(halves, real):
        own, other = halves.astype(jnp.bfloat16)
        first = core == 0
        lower, upper = jnp.where(first, own, other), jnp.where(first, other, own)
        return jnp.concatenate([lower[:, :real], upper[:, :real]], axis=1)

    ada_weight = ada_weight.transpose(0, 2, 1)
    modulate = mod_forward(
        conditioning, ada_weight, ada_bias, seqs, feat, data_size, tensor_size
    )
    piece = [
        [modulate[stream * 6 + index][:, None, :] for index in range(6)] for stream in range(2)
    ]

    inputs = [split_rows(input_img), split_rows(input_txt)]
    cotangents = [split_rows(cotangent_img), split_rows(cotangent_txt)]
    shapes = [array.shape for array in inputs]
    gain_pair = jnp.concatenate([norm_gain, norm_gain], axis=2)

    hidden1, raw, stats1 = [], [], []
    for stream in range(2):
        normed, inverse = layer_norm(inputs[stream].astype(jnp.float32))
        hidden = (normed * (1.0 + piece[stream][1]) + piece[stream][0]).astype(jnp.bfloat16)
        hidden = hidden.reshape(-1, feat)
        flat = [
            dot_plain(hidden, qkv_weight[stream, :, part]) + qkv_bias[stream, part].astype(jnp.float32)
            for part in range(3)
        ]
        hidden1.append(hidden)
        raw.append([each.reshape(shapes[stream][:3] + (-1,)) for each in flat])
        stats1.append((normed[0], inverse[0]))
    attn = attn_forward(gain_pair, raw[0], raw[1], reals[1])
    local = attn[0].shape[3]

    def mlp_stage(stream, total):
        branch = total.reshape(shapes[stream][1:]) + proj_bias[stream]
        residual = inputs[stream][0].astype(jnp.float32) + piece[stream][2] * branch
        normed, inverse = layer_norm(residual)
        hidden = share(normed, tensor_size) * (1.0 + piece[stream][4]) + piece[stream][3]
        hidden = hidden.astype(jnp.bfloat16).reshape(-1, feat)
        upward = dot_plain(hidden, up_weight[stream]) + up_bias[stream].astype(jnp.float32)
        active, slope = gelu_both(upward)
        active = active.astype(jnp.bfloat16)
        grad_mlp = cotangents[stream].astype(jnp.float32) * piece[stream][5]
        grad_mlp_low = grad_mlp.astype(jnp.bfloat16).reshape(-1, feat)
        grad_up = dot_right_t(grad_mlp_low, down_weight[stream]) * slope
        grad_up_low = grad_up.astype(jnp.bfloat16)
        half = grad_up_low.shape[0] // 2
        hidden_sum = core_sum(
            dot_right_t(grad_up_low[:half], up_weight[stream]),
            dot_right_t(grad_up_low[half:], up_weight[stream]),
            tensor_size,
        )
        mlp_sum = core_sum(
            dot_plain(active[:half], down_weight[stream]),
            dot_plain(active[half:], down_weight[stream]),
            tensor_size,
        )
        return {
            "branch": branch,
            "normed": normed,
            "inverse": inverse,
            "pairs": [(grad_mlp_low, active, 1), (hidden, grad_up_low, 1)],
            "hidden_sum": hidden_sum,
            "mlp_sum": mlp_sum,
            "up_bias": jnp.sum(grad_up, axis=0),
            "down_bias": jnp.sum(grad_mlp[0], axis=(0, 1)),
        }

    branch_sums = [None, None]
    for stream in (1, 0):
        rows = attn[stream].reshape(2, -1, local)
        branch_sums[stream] = core_sum(
            dot_plain(rows[0], proj_weight[stream]),
            dot_plain(rows[1], proj_weight[stream]),
            tensor_size,
        )
    state, mlp_rings = [None, None], [None, None]
    state[1] = mlp_stage(1, chip_sum(branch_sums[1], None, tensor_size))
    mlp_rings[1], (swapped,) = grad_ring(
        state[1]["pairs"], [branch_sums[0]], order, 2, "ring_mlp_txt"
    )
    state[0] = mlp_stage(0, chip_sum(branch_sums[0], swapped, tensor_size))
    gives = [state[stream][key] for key in ("hidden_sum", "mlp_sum") for stream in (1, 0)]
    mlp_rings[0], swapped = grad_ring(state[0]["pairs"], gives, order, 3, "ring_mlp_img")
    gives = [chip_sum(give, get, tensor_size) for give, get in zip(gives, swapped)]
    hidden_sums, mlp_sums = gives[1::-1], gives[:1:-1]

    grad_attn, proj_pairs, proj_sums, resid_grads, mod_grads = ([None, None] for _ in range(5))
    outputs = [None, None]
    for stream in (1, 0):
        branch, normed, inverse = (state[stream][key] for key in ("branch", "normed", "inverse"))
        grad_out = cotangents[stream][0].astype(jnp.float32)
        grad_hidden = hidden_sums[stream].reshape(normed.shape)
        through = norm_back(grad_hidden * (1.0 + piece[stream][4]), normed, inverse)
        grad_resid = grad_out + through
        grad_branch = share(grad_resid, tensor_size) * piece[stream][2]
        branch_low = grad_branch.astype(jnp.bfloat16).reshape(-1, feat)
        grad_attn[stream] = (
            dot_right_t(branch_low, proj_weight[stream])
            .astype(jnp.bfloat16)
            .reshape(attn[stream].shape)
        )
        proj_pairs[stream] = (branch_low, attn[stream].reshape(-1, local), 1)
        proj_sums[stream] = jnp.sum(grad_resid * piece[stream][2], axis=(0, 1))
        resid_grads[stream] = through
        mod_grads[stream] = [
            None,
            None,
            jnp.sum(grad_resid * branch, axis=1),
            jnp.sum(grad_hidden, axis=1),
            jnp.sum(grad_hidden * normed, axis=1),
            None,
        ]
    grad_packed = attn_backward(gain_pair, raw[0], raw[1], grad_attn[0], grad_attn[1], reals[1])
    qkv_bias_sums = jnp.sum(grad_packed[2], axis=0)
    gain_sums = jnp.sum(grad_packed[3], axis=0)
    head_dim = norm_gain.shape[2]
    gain_sums = gain_sums[:, :head_dim] + gain_sums[:, head_dim:]
    qkv_pairs, first_sums = [None, None], [None, None]
    for stream in (1, 0):
        packed_low = grad_packed[stream].reshape(-1, 3 * local)
        half = packed_low.shape[0] // 2

        def through_weights(rows):
            return sum(
                dot_right_t(
                    packed_low[rows, part * local : (part + 1) * local], qkv_weight[stream, :, part]
                )
                for part in range(3)
            )

        first_sums[stream] = core_sum(
            through_weights(slice(None, half)), through_weights(slice(half, None)), tensor_size
        )
        qkv_pairs[stream] = (hidden1[stream], packed_low, 3)
    rings, swapped = grad_ring(qkv_pairs + proj_pairs, first_sums, order, 4, "ring_attn")
    qkv_rings, proj_rings = rings[:2], rings[2:]
    first_sums = [chip_sum(give, get, tensor_size) for give, get in zip(first_sums, swapped)]

    grad_inputs = [None, None]
    for stream in (1, 0):
        branch = state[stream]["branch"]
        grad_out = cotangents[stream][0].astype(jnp.float32)
        mlp_out = mlp_sums[stream].reshape(branch.shape) + down_bias[stream]
        added = piece[stream][2] * branch + piece[stream][5] * mlp_out
        outputs[stream] = join_rows(
            inputs[stream].astype(jnp.float32) + share(added, tensor_size), reals[stream]
        )
        mod_grads[stream][5] = jnp.sum(grad_out * mlp_out, axis=1)
        normed, inverse = stats1[stream]
        grad_hidden = first_sums[stream].reshape(normed.shape)
        added = resid_grads[stream] + norm_back(
            grad_hidden * (1.0 + piece[stream][1]), normed, inverse
        )
        grad_inputs[stream] = join_rows(
            cotangents[stream].astype(jnp.float32) + share(added, tensor_size), reals[stream]
        )
        mod_grads[stream][0] = jnp.sum(grad_hidden, axis=1)
        mod_grads[stream][1] = jnp.sum(grad_hidden * normed, axis=1)

    row_share = 2.0 / tensor_size
    sums = mod_backward(
        jnp.stack(mod_grads[0] + mod_grads[1]),
        conditioning,
        ada_weight,
        [qkv_bias_sums, jnp.stack([state[0]["up_bias"], state[1]["up_bias"]])],
        [
            gain_sums,
            jnp.stack(proj_sums) * row_share,
            jnp.stack([state[0]["down_bias"], state[1]["down_bias"]]) * row_share,
        ],
        data_size,
        tensor_size,
    )
    grad_ada_weight, grad_ada_bias, silu_rows, qkv_bias_sums, up_bias_sums = sums[:5]
    gain_sums, proj_sums, down_sums = sums[5:]
    own_cond = lax.dynamic_slice_in_dim(
        conditioning, lax.axis_index("dp") * seqs, seqs, axis=0
    ).astype(jnp.float32)
    own_sig = jax.nn.sigmoid(own_cond)
    grad_conditioning = silu_rows * own_sig * (1.0 + own_cond * (1.0 - own_sig))
    down_rings, up_rings = ([mlp_rings[0][index], mlp_rings[1][index]] for index in range(2))
    return (
        outputs[0],
        outputs[1],
        grad_inputs[0],
        grad_inputs[1],
        grad_conditioning,
        grad_ada_weight.transpose(0, 2, 1),
        grad_ada_bias,
        jnp.stack(qkv_rings).transpose(0, 2, 1, 3),
        qkv_bias_sums.reshape(2, 3, -1),
        gain_sums.reshape(norm_gain.shape),
        jnp.concatenate(proj_rings).transpose(0, 2, 1),
        proj_sums,
        jnp.concatenate(up_rings),
        up_bias_sums,
        jnp.concatenate(down_rings).transpose(0, 2, 1),
        down_sums,
    )


def solution(mesh):
    in_specs = (
        P("dp", None, None),
        P("dp", None, None),
        P(),
        P(None, None, ("dp", "tensor")),
        P(None, ("dp", "tensor")),
        P(None, None, None, "tensor"),
        P(None, None, "tensor"),
        P(),
        P(None, "tensor", None),
        P(),
        P(None, None, "tensor"),
        P(None, "tensor"),
        P(None, "tensor", None),
        P(),
        P("dp", None, None),
        P("dp", None, None),
    )
    out_specs = (
        P("dp", None, None),
        P("dp", None, None),
        P("dp", None, None),
        P("dp", None, None),
        P("dp", None),
        P(None, None, ("dp", "tensor")),
        P(None, ("dp", "tensor")),
        P(None, "dp", None, "tensor"),
        P(None, None, "tensor"),
        P(),
        P(None, "tensor", "dp"),
        P(),
        P(None, "dp", "tensor"),
        P(None, "tensor"),
        P(None, "tensor", "dp"),
        P(),
    )
    return jax.shard_map(
        functools.partial(on_device, ring_order(mesh), mesh.shape["tensor"]),
        mesh=mesh,
        in_specs=in_specs,
        out_specs=out_specs,
        check_vma=False,
    )
```

```python
import functools

import jax
import jax.numpy as jnp
from jax import lax
from jax.experimental import pallas as pl
from jax.experimental.pallas import tpu as pltpu
from jax.sharding import PartitionSpec as P


epsilon = 1e-06
GELU_C = 0.7978845608028654
GELU_A = 0.044715
ROW_TILE = 16
NEG = -1e30
RESTS = (1, 2, 2)


def dot_plain(first_op, second_op):
    return jnp.dot(first_op, second_op, preferred_element_type=jnp.float32)


def dot_right_t(first_op, second_op):
    return lax.dot_general(
        first_op, second_op, (((1,), (1,)), ((), ())), preferred_element_type=jnp.float32
    )


def dot_left_t(first_op, second_op):
    return lax.dot_general(
        first_op, second_op, (((0,), (0,)), ((), ())), preferred_element_type=jnp.float32
    )


def layer_norm(values):
    center = values - jnp.mean(values, axis=-1, keepdims=True)
    inverse = lax.rsqrt(jnp.mean(center * center, axis=-1, keepdims=True) + epsilon)
    return (center * inverse, inverse)


def norm_back(grad_normed, normed, inverse):
    return inverse * (
        grad_normed
        - jnp.mean(grad_normed, axis=-1, keepdims=True)
        - normed * jnp.mean(grad_normed * normed, axis=-1, keepdims=True)
    )


def gelu_both(values):
    inner = jnp.tanh(GELU_C * (values + GELU_A * values * values * values))
    active = 0.5 * values * (1.0 + inner)
    slope = 0.5 * (1.0 + inner) + 0.5 * values * (1.0 - inner * inner) * GELU_C * (
        1.0 + 3.0 * GELU_A * values * values
    )
    return active, slope


def head_norm(values, gain):
    head_dim = values.shape[1] // 2
    lower = lax.broadcasted_iota(jnp.int32, values.shape, 1) < head_dim
    square = values * values
    first = jnp.sum(jnp.where(lower, square, 0.0), axis=-1, keepdims=True) / head_dim
    second = jnp.sum(jnp.where(lower, 0.0, square), axis=-1, keepdims=True) / head_dim
    factor = jnp.where(lower, lax.rsqrt(first + epsilon), lax.rsqrt(second + epsilon))
    return values * factor * gain, factor


def rows_of(img_ref, txt_ref, cols):
    return jnp.concatenate(
        [img_ref[0, 0, :, cols], img_ref[1, 0, :, cols], txt_ref[0, 0, :, cols], txt_ref[1, 0, :, cols]],
        axis=0,
    )


def put_rows(img_ref, txt_ref, cols, values):
    img, txt = img_ref.shape[2], txt_ref.shape[2]
    img_ref[0, 0, :, cols] = values[:img]
    img_ref[1, 0, :, cols] = values[img : 2 * img]
    txt_ref[0, 0, :, cols] = values[2 * img : 2 * img + txt]
    txt_ref[1, 0, :, cols] = values[2 * img + txt :]


def gain_rows(gain_ref, which, img, txt):
    width = gain_ref.shape[2]
    return jnp.concatenate(
        [
            jnp.broadcast_to(gain_ref[0, which : which + 1, :], (2 * img, width)),
            jnp.broadcast_to(gain_ref[1, which : which + 1, :], (2 * txt, width)),
        ],
        axis=0,
    )


def key_bias(img, txt, real):
    where = lax.broadcasted_iota(jnp.int32, (1, 2 * (img + txt)), 1)
    first = where - 2 * img
    gone = ((first >= real) & (first < txt)) | (first >= txt + real)
    return jnp.where(gone, NEG, 0.0).astype(jnp.float32)


def probs(q_head, k_low, bias):
    scores = dot_right_t(q_head, k_low) + bias
    top = jnp.max(scores, axis=-1, keepdims=True)
    weights = jnp.exp(scores - top)
    return weights * (1.0 / jnp.sum(weights, axis=-1, keepdims=True))


def attn_forward_kernel(real, gain_ref, *refs):
    raw_refs, (out_img_ref, out_txt_ref) = (refs[:3], refs[3:6]), refs[6:]
    img, txt = out_img_ref.shape[2], out_txt_ref.shape[2]
    local = out_img_ref.shape[3]
    pair = gain_ref.shape[2]
    q_gain, k_gain = gain_rows(gain_ref, 0, img, txt), gain_rows(gain_ref, 1, img, txt)
    bias = key_bias(img, txt, real)
    scale = (pair // 2) ** (-0.5)
    for start in range(0, local, pair):
        q_raw, k_raw, v_raw = (
            rows_of(raw_refs[0][part], raw_refs[1][part], slice(start, start + pair))
            for part in range(3)
        )
        q_low = head_norm(q_raw, q_gain)[0].astype(jnp.bfloat16) * jnp.bfloat16(scale)
        k_low = head_norm(k_raw, k_gain)[0].astype(jnp.bfloat16)
        v_low = v_raw.astype(jnp.bfloat16)
        lower = lax.broadcasted_iota(jnp.int32, q_raw.shape, 1) < pair // 2
        results = []
        for head in range(2):
            mine = lower if head == 0 else jnp.logical_not(lower)
            q_head = jnp.where(mine, q_low, jnp.bfloat16(0))
            results.append(dot_plain(probs(q_head, k_low, bias).astype(jnp.bfloat16), v_low))
        out = jnp.where(lower, results[0], results[1]).astype(jnp.bfloat16)
        put_rows(out_img_ref, out_txt_ref, slice(start, start + pair), out)


def attn_backward_kernel(real, gain_ref, *refs):
    raw_refs = (refs[:3], refs[3:6])
    d_img_ref, d_txt_ref, o_img_ref, o_txt_ref, bias_ref, dgain_ref = refs[6:]
    img, txt = d_img_ref.shape[2], d_txt_ref.shape[2]
    local = d_img_ref.shape[3]
    pair = gain_ref.shape[2]
    head_dim = pair // 2
    q_gain, k_gain = gain_rows(gain_ref, 0, img, txt), gain_rows(gain_ref, 1, img, txt)
    bias = key_bias(img, txt, real)
    scale = head_dim ** (-0.5)
    gain_sums = [[None, None], [None, None]]
    for start in range(0, local, pair):
        q_raw, k_raw, v_raw = (
            rows_of(raw_refs[0][part], raw_refs[1][part], slice(start, start + pair))
            for part in range(3)
        )
        q_wide, q_factor = head_norm(q_raw, q_gain)
        k_wide, k_factor = head_norm(k_raw, k_gain)
        q_low = q_wide.astype(jnp.bfloat16) * jnp.bfloat16(scale)
        k_low = k_wide.astype(jnp.bfloat16)
        v_low = v_raw.astype(jnp.bfloat16)
        grad_out = rows_of(d_img_ref, d_txt_ref, slice(start, start + pair))
        lower = lax.broadcasted_iota(jnp.int32, q_raw.shape, 1) < head_dim
        parts = []
        for head in range(2):
            mine = lower if head == 0 else jnp.logical_not(lower)
            prob = probs(jnp.where(mine, q_low, jnp.bfloat16(0)), k_low, bias)
            grad_v = dot_left_t(prob.astype(jnp.bfloat16), grad_out)
            grad_prob = dot_right_t(jnp.where(mine, grad_out, jnp.bfloat16(0)), v_low)
            delta = jnp.sum(prob * grad_prob, axis=-1, keepdims=True)
            grad_scores = (prob * (grad_prob - delta)).astype(jnp.bfloat16)
            parts.append((dot_plain(grad_scores, k_low), dot_left_t(grad_scores, q_low), grad_v))
        grad_qn = jnp.where(lower, parts[0][0], parts[1][0]) * scale
        grad_kn = jnp.where(lower, parts[0][1], parts[1][1])
        grad_vn = jnp.where(lower, parts[0][2], parts[1][2])

        def raw_grad(grad_normed, raw, factor, gain, which):
            gained = grad_normed * gain
            product = gained * raw
            first = jnp.sum(jnp.where(lower, product, 0.0), axis=-1, keepdims=True) / head_dim
            second = jnp.sum(jnp.where(lower, 0.0, product), axis=-1, keepdims=True) / head_dim
            inner = jnp.where(lower, first, second)
            terms = grad_normed * raw * factor
            for stream, rows in enumerate((slice(0, 2 * img), slice(2 * img, 2 * (img + txt)))):
                total = jnp.sum(terms[rows], axis=0, keepdims=True)
                old = gain_sums[stream][which]
                gain_sums[stream][which] = total if old is None else old + total
            return factor * gained - raw * (factor * factor * factor) * inner

        grads = (
            raw_grad(grad_qn, q_raw, q_factor, q_gain, 0),
            raw_grad(grad_kn, k_raw, k_factor, k_gain, 1),
            grad_vn,
        )
        for part, grad in enumerate(grads):
            cols = slice(part * local + start, part * local + start + pair)
            bias_ref[0, 0:1, cols] = jnp.sum(grad[: 2 * img], axis=0, keepdims=True)
            bias_ref[0, 1:2, cols] = jnp.sum(grad[2 * img :], axis=0, keepdims=True)
            put_rows(o_img_ref, o_txt_ref, cols, grad.astype(jnp.bfloat16))
    for stream in range(2):
        for which in range(2):
            row = stream * 2 + which
            dgain_ref[0, row : row + 1, :] = gain_sums[stream][which]


def block_of(array):
    shape = array.shape
    return pl.BlockSpec((shape[0], 1) + shape[2:], lambda seq: (0, seq, 0, 0))


def whole_of(array):
    return pl.BlockSpec(array.shape, lambda seq: (0,) * array.ndim)


def attn_forward(gain_pair, raw_img, raw_txt, real):
    seqs, local = raw_img[0].shape[1], raw_img[0].shape[3]
    outs = [jax.ShapeDtypeStruct(raw[0].shape, jnp.bfloat16) for raw in (raw_img, raw_txt)]
    rows = 2 * (raw_img[0].shape[2] + raw_txt[0].shape[2])
    return pl.pallas_call(
        functools.partial(attn_forward_kernel, real),
        grid=(seqs,),
        out_shape=outs,
        in_specs=[whole_of(gain_pair)] + [block_of(raw) for raw in raw_img + raw_txt],
        out_specs=[block_of(out) for out in outs],
        compiler_params=pltpu.CompilerParams(vmem_limit_bytes=48 << 20),
        cost_estimate=pl.CostEstimate(
            flops=seqs * rows * rows * local * 4,
            bytes_accessed=seqs * rows * local * 14,
            transcendentals=seqs * rows * rows * (local // 64),
        ),
        name="attn_forward",
    )(gain_pair, *raw_img, *raw_txt)


def attn_backward(gain_pair, raw_img, raw_txt, grad_img, grad_txt, real):
    seqs, local = raw_img[0].shape[1], raw_img[0].shape[3]
    outs = [
        jax.ShapeDtypeStruct(raw_img[0].shape[:3] + (3 * local,), jnp.bfloat16),
        jax.ShapeDtypeStruct(raw_txt[0].shape[:3] + (3 * local,), jnp.bfloat16),
        jax.ShapeDtypeStruct((seqs, 2, 3 * local), jnp.float32),
        jax.ShapeDtypeStruct((seqs, 4, gain_pair.shape[2]), jnp.float32),
    ]
    rows = 2 * (raw_img[0].shape[2] + raw_txt[0].shape[2])
    return pl.pallas_call(
        functools.partial(attn_backward_kernel, real),
        grid=(seqs,),
        out_shape=outs,
        in_specs=[whole_of(gain_pair)]
        + [block_of(each) for each in raw_img + raw_txt + [grad_img, grad_txt]],
        out_specs=[
            block_of(outs[0]),
            block_of(outs[1]),
            pl.BlockSpec((1, 2, 3 * local), lambda seq: (seq, 0, 0)),
            pl.BlockSpec((1, 4, gain_pair.shape[2]), lambda seq: (seq, 0, 0)),
        ],
        compiler_params=pltpu.CompilerParams(vmem_limit_bytes=56 << 20),
        cost_estimate=pl.CostEstimate(
            flops=seqs * rows * rows * local * 10,
            bytes_accessed=seqs * rows * local * 20,
            transcendentals=seqs * rows * rows * (local // 64),
        ),
        name="attn_backward",
    )(gain_pair, *raw_img, *raw_txt, grad_img, grad_txt)


def xor_index(index, distance):
    return index + distance - 2 * distance * ((index // distance) % 2)


def peers_of(data_size, tensor_size):
    row, col = lax.axis_index("dp"), lax.axis_index("tensor")
    around = [(lax.rem(row + step, data_size), col) for step in range(1, data_size)]
    across = []
    distance = 1
    while distance < tensor_size:
        across.append((row, xor_index(col, distance)))
        distance *= 2
    return row, col, around, across


def greet(partners):
    barrier = pltpu.get_barrier_semaphore()
    for partner in partners:
        pl.semaphore_signal(barrier, inc=1, device_id=partner, device_id_type=pl.DeviceIdType.MESH)
    pl.semaphore_wait(barrier, len(partners))


def remote(source, target, sems, index, partner):
    copy = pltpu.make_async_remote_copy(
        src_ref=source,
        dst_ref=target,
        send_sem=sems.at[0, index],
        recv_sem=sems.at[1, index],
        device_id=partner,
        device_id_type=pl.DeviceIdType.MESH,
    )
    copy.start()
    return copy


def silu_of(cond_ref):
    wide = cond_ref[...].astype(jnp.float32)
    return (wide * (1.0 / (1.0 + jnp.exp(-wide)))).astype(jnp.bfloat16)


def mod_forward_kernel(
    data_size, tensor_size, cond_ref, weight_ref, bias_ref, out_ref, outgoing, blocks, sems
):
    row, col, around, across = peers_of(data_size, tensor_size)
    seqs, feat = out_ref.shape[1], out_ref.shape[2]
    silu_cond = silu_of(cond_ref)
    for stream in range(2):
        values = dot_right_t(silu_cond, weight_ref[stream]) + bias_ref[stream : stream + 1].astype(
            jnp.float32
        )
        for index in range(data_size):
            outgoing[index, stream * seqs : (stream + 1) * seqs] = values[
                index * seqs : (index + 1) * seqs
            ]
    blocks[col, row] = outgoing[row]
    greet(around + across)
    copies = [
        remote(outgoing.at[partner[0]], blocks.at[col, row], sems, index, partner)
        for index, partner in enumerate(around)
    ]
    for copy in copies:
        copy.wait()
    held, used = [0], len(around)
    for level in reversed(range(len(across))):
        distance = 1 << level
        copies = []
        for offset in held:
            index = col
            for bit in range(len(across)):
                if offset >> bit & 1:
                    index = xor_index(index, 1 << bit)
            copies.append(remote(blocks.at[index], blocks.at[index], sems, used, across[level]))
            used += 1
        for copy in copies:
            copy.wait()
        held = held + [offset | distance for offset in held]
    for stream in range(2):
        full = jnp.concatenate(
            [
                blocks[second, first, stream * seqs : (stream + 1) * seqs]
                for first in range(data_size)
                for second in range(tensor_size)
            ],
            axis=1,
        )
        for index in range(6):
            out_ref[stream * 6 + index] = full[:, index * feat : (index + 1) * feat]


def mod_forward(conditioning, ada_weight, ada_bias, seqs, feat, data_size, tensor_size):
    cols = ada_weight.shape[1]
    vmem = pl.BlockSpec(memory_space=pltpu.VMEM)
    return pl.pallas_call(
        functools.partial(mod_forward_kernel, data_size, tensor_size),
        out_shape=jax.ShapeDtypeStruct((12, seqs, feat), jnp.float32),
        in_specs=[vmem] * 3,
        out_specs=vmem,
        scratch_shapes=[
            pltpu.VMEM((data_size, 2 * seqs, cols), jnp.float32),
            pltpu.VMEM((tensor_size, data_size, 2 * seqs, cols), jnp.float32),
            pltpu.SemaphoreType.DMA((2, data_size + tensor_size)),
        ],
        compiler_params=pltpu.CompilerParams(
            collective_id=0, has_side_effects=True, vmem_limit_bytes=32 << 20
        ),
        name="mod_forward",
    )(conditioning, ada_weight, ada_bias)


def mod_backward_kernel(
    data_size,
    tensor_size,
    mod_ref,
    cond_ref,
    weight_ref,
    *refs,
):
    refs = list(refs)

    def take(number):
        taken = refs[:number]
        del refs[:number]
        return taken

    group_refs, all_refs = take(2), take(3)
    weight_out, bias_out, silu_out = take(3)
    group_outs, all_outs = take(2), take(3)
    blocks, core_in, outgoing, cols_in, lines, lines_in, lines_own, lines_all = take(8)
    silu_blocks, silu_in, silu_send, silu_recv, all_send, all_recv, sems = take(7)
    row, col, around, across = peers_of(data_size, tensor_size)
    seqs, feat = silu_out.shape
    cols = bias_out.shape[1]
    for stream in range(2):
        full = jnp.concatenate([mod_ref[stream * 6 + index] for index in range(6)], axis=1)
        for first in range(data_size):
            for second in range(tensor_size):
                start = (first * tensor_size + second) * cols
                blocks[second, first, stream * seqs : (stream + 1) * seqs] = full[
                    :, start : start + cols
                ]
    silu_cond = silu_of(cond_ref)
    half = lines.shape[1] // 2
    width = lines.shape[2]

    def line_up(sources):
        padded = [
            jnp.pad(ref[...], ((0, 0), (0, feat - ref.shape[1]))) for ref in sources
        ]
        short = half - sum(ref.shape[0] for ref in sources)
        if short:
            padded.append(jnp.zeros((short, feat), jnp.float32))
        return jnp.concatenate(padded, axis=0)

    every_line = jnp.concatenate([line_up(group_refs), line_up(all_refs)], axis=0)
    for index in range(data_size):
        lines[index] = every_line[:, index * width : (index + 1) * width]
    greet(around + across)

    used = 0
    copy = remote(blocks.at[xor_index(col, 1)], core_in, sems, used, across[0])
    used += 1
    copy.wait()
    for first in range(data_size):
        outgoing[first] = blocks[col, first] + core_in[first]

    cols_in[row] = outgoing[row]
    lines_in[row] = lines[row]
    copies = []
    for partner in around:
        for source, target in ((lines, lines_in), (outgoing, cols_in)):
            copies.append(
                remote(source.at[partner[0]], target.at[row], sems, used, partner)
            )
            used += 1
    for copy in copies:
        copy.wait()
    lines_own[...] = functools.reduce(jnp.add, [lines_in[index] for index in range(data_size)])
    low = []
    for stream in range(2):
        wide = jnp.concatenate(
            [cols_in[index, stream * seqs : (stream + 1) * seqs] for index in range(data_size)],
            axis=0,
        )
        bias_out[stream : stream + 1] = jnp.sum(wide, axis=0, keepdims=True)
        low.append(wide.astype(jnp.bfloat16))
    silu_grad = dot_plain(low[0], weight_ref[0]) + dot_plain(low[1], weight_ref[1])
    for index in range(data_size):
        silu_blocks[index] = silu_grad[index * seqs : (index + 1) * seqs]
    for stream in range(2):
        weight_out[stream] = dot_left_t(low[stream], silu_cond)

    silu_in[row] = silu_blocks[row]
    lines_all[row] = lines_own[...]
    copies = []
    for partner in around:
        for source, target in (
            (silu_blocks.at[partner[0]], silu_in.at[row]),
            (lines_own, lines_all.at[row]),
        ):
            copies.append(remote(source, target, sems, used, partner))
            used += 1
    for copy in copies:
        copy.wait()
    silu_send[0] = functools.reduce(jnp.add, [silu_in[index] for index in range(data_size)])
    every_line = jnp.concatenate([lines_all[index] for index in range(data_size)], axis=1)
    all_send[0] = every_line[half:]

    def hand_out(values, targets):
        start = 0
        for target in targets:
            count, size = target.shape
            target[...] = values[start : start + count, :size]
            start += count

    hand_out(every_line[:half], group_outs)

    for level, partner in enumerate(across):
        copies = [
            remote(silu_send.at[level], silu_recv.at[level], sems, used, partner),
            remote(all_send.at[level], all_recv.at[level], sems, used + 1, partner),
        ]
        used += 2
        for copy in copies:
            copy.wait()
        silu_send[level + 1] = silu_send[level] + silu_recv[level]
        all_send[level + 1] = all_send[level] + all_recv[level]
    silu_out[...] = silu_send[len(across)]
    hand_out(all_send[len(across)], all_outs)


def mod_backward(mod_grads, conditioning, ada_weight, group, every, data_size, tensor_size):
    _, seqs, feat = mod_grads.shape
    cols = ada_weight.shape[1]
    levels = tensor_size.bit_length() - 1
    vmem = pl.BlockSpec(memory_space=pltpu.VMEM)
    lines, width = 16, feat // data_size

    def wide(*shape):
        return pltpu.VMEM(shape, jnp.float32)

    return pl.pallas_call(
        functools.partial(mod_backward_kernel, data_size, tensor_size),
        out_shape=[
            jax.ShapeDtypeStruct(ada_weight.shape, jnp.float32),
            jax.ShapeDtypeStruct((2, cols), jnp.float32),
            jax.ShapeDtypeStruct((seqs, feat), jnp.float32),
        ]
        + [jax.ShapeDtypeStruct(each.shape, jnp.float32) for each in group + every],
        in_specs=[vmem] * (3 + len(group) + len(every)),
        out_specs=[vmem] * (3 + len(group) + len(every)),
        scratch_shapes=[
            wide(tensor_size, data_size, 2 * seqs, cols),
            wide(data_size, 2 * seqs, cols),
            wide(data_size, 2 * seqs, cols),
            wide(data_size, 2 * seqs, cols),
            wide(data_size, lines, width),
            wide(data_size, lines, width),
            wide(lines, width),
            wide(data_size, lines, width),
            wide(data_size, seqs, feat),
            wide(data_size, seqs, feat),
            wide(levels + 1, seqs, feat),
            wide(levels, seqs, feat),
            wide(levels + 1, lines // 2, feat),
            wide(levels, lines // 2, feat),
            pltpu.SemaphoreType.DMA((2, 1 + 4 * (data_size - 1) + 2 * levels)),
        ],
        compiler_params=pltpu.CompilerParams(
            collective_id=1, has_side_effects=True, vmem_limit_bytes=48 << 20
        ),
        name="mod_backward",
    )(mod_grads, conditioning, ada_weight, *group, *every)


def norm_of(values):
    center = values - jnp.mean(values, axis=-1, keepdims=True)
    inverse = lax.rsqrt(jnp.mean(center * center, axis=-1, keepdims=True) + epsilon)
    return center * inverse, inverse


def swap_pairs(size, distance):
    return [(index, index ^ distance) for index in range(size)]


def core_sum(own_part, other_part, tensor_size):
    return own_part + lax.ppermute(other_part, "tensor", swap_pairs(tensor_size, 1))


def share(own_rows, tensor_size):
    other = lax.ppermute(own_rows, "tensor", swap_pairs(tensor_size, 1))
    return jnp.stack([own_rows, other])


def ring_order(mesh):
    size = mesh.shape["dp"]
    fallback = list(range(0, size, 2)) + list(range(1, size, 2))[::-1]
    axis = list(mesh.axis_names).index("dp")
    devices = mesh.devices
    line = [devices[(slice(None),) * axis + (index,)].flatten()[0] for index in range(size)]
    coords = [getattr(device, "coords", None) for device in line]
    if any(place is None for place in coords):
        return fallback
    near = [
        [
            other
            for other in range(size)
            if sum(abs(a - b) for a, b in zip(coords[index], coords[other])) == 1
        ]
        for index in range(size)
    ]
    path, seen, budget = [0], {0}, [200000]

    def extend():
        budget[0] -= 1
        if budget[0] < 0:
            return False
        if len(path) == size:
            return path[0] in near[path[-1]]
        choices = [index for index in near[path[-1]] if index not in seen]
        choices.sort(key=lambda index: (sum(o not in seen for o in near[index]), index))
        for index in choices:
            path.append(index)
            seen.add(index)
            if extend():
                return True
            path.pop()
            seen.remove(index)
        return False

    return path if extend() else fallback


def entry_of(table, index):
    value = jnp.int32(table[0])
    for place in range(1, len(table)):
        value = jnp.where(index == place, jnp.int32(table[place]), value)
    return value


class Ring:
    def __init__(self, order, rest, lefts, rights, slots, terms, turned, sems):
        self.order, self.size, self.rest = order, len(order), rest
        self.lefts, self.rights, self.slots, self.terms = lefts, rights, slots, terms
        self.turned, self.sems = turned, sems
        row, col = lax.axis_index("dp"), lax.axis_index("tensor")
        size = self.size
        self.place = entry_of([order.index(index) for index in range(size)], row)
        self.after = entry_of(order, lax.rem(self.place + 1, size))
        self.before = entry_of(order, lax.rem(self.place + size - 1, size))
        self.targets = ((self.after, col), (self.before, col))
        self.half = slots[0].shape[2]
        self.chains = [(which, way) for which in range(len(lefts)) for way in range(2)]
        self.last = size - 2 - rest

    def term(self, which, way, index):
        start = pl.multiple_of((2 * index + way) * self.half, 8)
        return dot_plain(
            self.turned[which][pl.ds(start, self.half), :], self.rights[which][...]
        )

    def work_out(self, indices):
        for which, way in self.chains:
            self.terms[which][way] = self.term(which, way, indices[way])

    def copy_of(self, which, way, step, source, target):
        return pltpu.make_async_remote_copy(
            src_ref=source,
            dst_ref=self.slots[which].at[way, target],
            send_sem=self.sems.at[0, which, way, step],
            recv_sem=self.sems.at[1, which, way, step],
            device_id=self.targets[way],
            device_id_type=pl.DeviceIdType.MESH,
        )

    def blocks_at(self, step):
        size = self.size
        return (
            entry_of(self.order, lax.rem(self.place + 2 * size - 2 - step, size)),
            entry_of(self.order, lax.rem(self.place + 2 + step, size)),
        )

    def arrive(self, which, way, step):
        slot = self.slots[which].at[way, step]
        self.copy_of(which, way, step, slot, step).wait_recv()

    def begin(self):
        for which, left in enumerate(self.lefts):
            self.turned[which][...] = left[...].T
            for way in range(2):
                first = self.slots[which].at[way, self.size - 1]
                first[...] = self.term(which, way, (self.before, self.after)[way])
                self.copy_of(which, way, 0, first, 0).start()

    def rounds(self):
        def round_of(step, carry):
            self.work_out(self.blocks_at(step))
            for which, way in self.chains:
                self.arrive(which, way, step)
                slot = self.slots[which].at[way, step]
                slot[...] = slot[...] + self.terms[which][way]
                self.copy_of(which, way, step + 1, slot, step + 1).start()
            return carry

        lax.fori_loop(0, self.last, round_of, 0)

    def finish(self, put_later, put_total):
        for later in range(self.rest):
            indices = self.blocks_at(self.last + 1 + later)
            for which, way in self.chains:
                put_later(later, which, way, self.term(which, way, indices[way]))
        self.work_out(self.blocks_at(self.last))
        for which, way in self.chains:
            self.arrive(which, way, self.last)
            put_total(which, way, self.slots[which][way, self.last] + self.terms[which][way])

        def sent(step, carry):
            for which, way in self.chains:
                slot = self.slots[which].at[way, self.size - 1]
                self.copy_of(which, way, step, slot, step).wait_send()
            return carry

        lax.fori_loop(0, self.last + 1, sent, 0)


def taker(refs):
    refs = list(refs)

    def take(number):
        taken = refs[:number]
        del refs[:number]
        return taken

    return take


def ring_scratch(size, halves, lefts, count_kind=jnp.bfloat16):
    return (
        [pltpu.VMEM((2, size) + half, jnp.float32) for half in halves]
        + [pltpu.VMEM((2,) + half, jnp.float32) for half in halves]
        + [pltpu.VMEM(shape[::-1], count_kind) for shape in lefts]
        + [pltpu.SemaphoreType.DMA((2, len(halves), 2, size - 1))]
    )


def grad_ring_kernel(order, count, swaps, rest, *refs):
    take = taker(refs)
    lefts, rights, gives = take(count), take(count), take(swaps)
    outs = take(2 * (rest + 1)) if rest else take(count)
    gets = take(swaps)
    slots, terms, turned = take(count), take(count), take(count)
    sems, swap_sems = take(2)
    ring = Ring(order, rest, lefts, rights, slots, terms, turned, sems)
    facing = (lax.axis_index("dp"), xor_index(lax.axis_index("tensor"), 2))
    greet(ring.targets + (facing,))
    swapped = [
        remote(gives[index], gets[index], swap_sems, index, facing) for index in range(swaps)
    ]
    widths = [right.shape[1] for right in rights]
    starts = [sum(widths[:which]) for which in range(count)]

    def put_later(later, which, way, values):
        columns = slice(starts[which], starts[which] + widths[which])
        outs[2 * (later + 1) + way][:, columns] = values

    def put_total(which, way, values):
        if rest:
            outs[way][:, starts[which] : starts[which] + widths[which]] = values
            return
        parts, _, width = outs[which].shape
        for part in range(parts):
            outs[which][part, way * ring.half : (way + 1) * ring.half] = values[
                :, part * width : (part + 1) * width
            ]

    ring.begin()
    ring.rounds()
    ring.finish(put_later, put_total)
    for copy in swapped:
        copy.wait()


def mlp_ring_kernel(order, stream, seqs, block, swaps, rest, *refs):
    take = taker(refs)
    mod_ref, proj_bias_ref, up_bias_ref = take(3)
    mine_hbm, got_hbm, input_hbm, cot_hbm, up_hbm, down_hbm = take(6)
    gives = take(swaps)
    outs = take(2 * (rest + 1)) if rest else take(2)
    gets = take(swaps)
    inverse_ref, up_sum_ref, down_sum_ref = take(3)
    branch_hbm, normed_hbm, hidden_sum_hbm, hidden_got_hbm, mlp_sum_hbm, mlp_got_hbm = take(6)
    slots, terms, turned = take(2), take(2), take(2)
    (ring_sems,) = take(1)
    up_ref, down_ref, input_ref, hidden_ref, active_ref, grad_up_ref, grad_mlp_ref = take(7)
    mine_ref, got_ref, branch_ref, normed_ref, normed_in, spare = take(6)
    load_sems, core_sems, swap_sems, out_sems = take(4)
    rows, feat = mine_ref.shape
    units = active_ref.shape[1]
    length = rows // seqs
    ring = Ring(
        order, rest, (grad_mlp_ref, hidden_ref), (active_ref, grad_up_ref), slots, terms, turned, ring_sems
    )
    partner = (lax.axis_index("dp"), xor_index(lax.axis_index("tensor"), 1))
    facing = (lax.axis_index("dp"), xor_index(lax.axis_index("tensor"), 2))

    loads = []
    for source, target in (
        (mine_hbm, mine_ref),
        (got_hbm, got_ref),
        (input_hbm, input_ref),
        (cot_hbm, grad_mlp_ref),
        (up_hbm.at[stream], up_ref),
        (down_hbm.at[stream], down_ref),
    ):
        loads.append(pltpu.make_async_copy(source, target, load_sems.at[len(loads)]))
        loads[-1].start()
    greet(ring.targets + (facing, partner))
    swapped = [
        remote(gives[index], gets[index], swap_sems, index, facing) for index in range(swaps)
    ]

    def mod(index, seq):
        return mod_ref[stream * 6 + index, seq : seq + 1, :]

    stored = []

    def store(source, target):
        copy = pltpu.make_async_copy(source, target, out_sems.at[len(stored)])
        copy.start()
        stored.append(copy)
        return copy

    for load in loads[:3]:
        load.wait()
    copies = []
    for seq in range(seqs):
        span = slice(seq * length, (seq + 1) * length)
        branch = mine_ref[span] + got_ref[span] + proj_bias_ref[stream : stream + 1].astype(jnp.float32)
        branch_ref[span] = branch
        normed, inverse = norm_of(input_ref[span].astype(jnp.float32) + mod(2, seq) * branch)
        normed_ref[span] = normed
        inverse_ref[span] = inverse
        hidden_ref[span] = (normed * (1.0 + mod(4, seq)) + mod(3, seq)).astype(jnp.bfloat16)
        copies.append(remote(normed_ref.at[span], normed_in.at[span], core_sems, seq, partner))
    kept = [store(branch_ref, branch_hbm), store(normed_ref, normed_hbm)]
    loads[3].wait()
    down_total = None
    for half in range(2):
        for seq in range(seqs):
            span = slice(half * rows + seq * length, half * rows + (seq + 1) * length)
            grad_mlp = grad_mlp_ref[span].astype(jnp.float32) * mod(5, seq)
            grad_mlp_ref[span] = grad_mlp.astype(jnp.bfloat16)
            if half == 0:
                total = jnp.sum(grad_mlp, axis=0, keepdims=True)
                down_total = total if down_total is None else down_total + total
    down_sum_ref[...] = down_total
    for seq, copy in enumerate(copies):
        copy.wait()
        span = slice(seq * length, (seq + 1) * length)
        hidden_ref[rows + seq * length : rows + (seq + 1) * length] = (
            normed_in[span] * (1.0 + mod(4, seq)) + mod(3, seq)
        ).astype(jnp.bfloat16)
    for load in loads[4:]:
        load.wait()

    def unit_block(index, carry):
        cols = pl.ds(pl.multiple_of(index * block, block), block)
        upward = dot_plain(hidden_ref[...], up_ref[:, cols]) + up_bias_ref[
            stream : stream + 1, cols
        ].astype(jnp.float32)
        active, slope = gelu_both(upward)
        active_ref[:, cols] = active.astype(jnp.bfloat16)
        grad_up = dot_right_t(grad_mlp_ref[...], down_ref[cols, :]) * slope
        up_sum_ref[:, cols] = jnp.sum(grad_up, axis=0, keepdims=True)
        grad_up_ref[:, cols] = grad_up.astype(jnp.bfloat16)
        return carry

    lax.fori_loop(0, units // block, unit_block, 0)
    ring.begin()

    for copy in kept:
        copy.wait()
    count = feat // block
    sums = ((branch_ref, mine_ref, normed_in), (normed_ref, got_ref, spare))
    copies = []
    for kind, (outgoing, incoming, own) in enumerate(sums):
        for index in range(count):
            cols = slice(index * block, (index + 1) * block)
            if kind == 0:
                both = dot_right_t(grad_up_ref[...], up_ref[cols, :])
            else:
                both = dot_plain(active_ref[...], down_ref[:, cols])
            own[:, cols] = both[:rows]
            outgoing[:, cols] = both[rows:]
            copies.append(
                remote(
                    outgoing.at[:, cols],
                    incoming.at[:, cols],
                    core_sems,
                    seqs + kind * count + index,
                    partner,
                )
            )
    for kind, (target, swap) in enumerate(
        ((hidden_sum_hbm, hidden_got_hbm), (mlp_sum_hbm, mlp_got_hbm))
    ):
        _, incoming, own = sums[kind]
        for copy in copies[kind * count : (kind + 1) * count]:
            copy.wait()
        own[...] = own[...] + incoming[...]
        store(own, target)
        swapped.append(remote(own, swap, swap_sems, swaps + kind, facing))
    ring.rounds()

    buffers = (mine_ref, got_ref, branch_ref, normed_ref)
    each = rows // (2 * ring.half)

    def piece_of(index):
        start = index % each * 2 * ring.half
        return buffers[index // each].at[start : start + 2 * ring.half]

    def put_later(later, which, way, values):
        piece_of(2 * (later + 1) + way)[which * ring.half : (which + 1) * ring.half] = values

    def put_total(which, way, values):
        if rest:
            piece_of(way)[which * ring.half : (which + 1) * ring.half] = values
        else:
            outs[which][0, way * ring.half : (way + 1) * ring.half] = values

    ring.finish(put_later, put_total)
    if rest:
        for index, out in enumerate(outs):
            store(piece_of(index), out)
    for copy in swapped:
        copy.wait()
    for copy in stored[len(kept) :]:
        copy.wait()


def mlp_ring(
    stream, mine, got, inputs, cots, modulate, proj_bias, up_bias, up_weight, down_weight, gives, order, rest,
    collective_id,
):
    _, seqs, length, feat = inputs.shape
    rows, units, size, swaps = seqs * length, up_weight.shape[2], len(order), len(gives)
    block = 256
    half = feat // (2 * size)
    vmem = pl.BlockSpec(memory_space=pltpu.VMEM)
    anywhere = pl.BlockSpec(memory_space=pl.ANY)

    def shape(kind, *dims):
        return jax.ShapeDtypeStruct(dims, kind)

    def low(*dims):
        return pltpu.VMEM(dims, jnp.bfloat16)

    ring_outs = (
        [shape(jnp.float32, 2 * half, units)] * (2 * (rest + 1))
        if rest
        else [shape(jnp.float32, 1, 2 * half, units)] * 2
    )
    gets = [shape(give.dtype, *give.shape) for give in gives]
    small = [
        shape(jnp.float32, rows, 1),
        shape(jnp.float32, 1, units),
        shape(jnp.float32, 1, feat),
    ]
    large = [shape(jnp.float32, rows, feat)] * 6
    moved = 4 * 2 * 2 * (size - 1) * half * units
    blocks = 2 * feat // block
    results = pl.pallas_call(
        functools.partial(mlp_ring_kernel, order, stream, seqs, block, swaps, rest),
        out_shape=ring_outs + gets + small + large,
        in_specs=[vmem] * 3 + [anywhere] * (6 + swaps),
        out_specs=[anywhere if rest else vmem] * len(ring_outs)
        + [anywhere] * swaps
        + [vmem] * 3
        + [anywhere] * 6,
        scratch_shapes=ring_scratch(size, [(half, units)] * 2, [(2 * rows, feat)] * 2)
        + [
            low(feat, units),
            low(units, feat),
            low(rows, feat),
            low(2 * rows, feat),
            low(2 * rows, units),
            low(2 * rows, units),
            low(2 * rows, feat),
        ]
        + [pltpu.VMEM((rows, feat), jnp.float32)] * 6
        + [
            pltpu.SemaphoreType.DMA((6,)),
            pltpu.SemaphoreType.DMA((2, seqs + blocks)),
            pltpu.SemaphoreType.DMA((2, swaps + 2)),
            pltpu.SemaphoreType.DMA((4 + len(ring_outs),)),
        ],
        compiler_params=pltpu.CompilerParams(
            collective_id=collective_id, has_side_effects=True, vmem_limit_bytes=67043328
        ),
        cost_estimate=pl.CostEstimate(flops=moved * 10000, bytes_accessed=moved, transcendentals=0),
        name="mlp_ring",
    )(
        modulate,
        proj_bias,
        up_bias,
        mine,
        got,
        inputs[0].reshape(rows, feat),
        cots.reshape(2 * rows, feat),
        up_weight,
        down_weight,
        *gives,
    )
    ring_parts, results = results[: len(ring_outs)], results[len(ring_outs) :]
    names = ("inverse", "up_bias", "down_bias", "branch", "normed", "hidden_sum", "hidden_got", "mlp_sum", "mlp_got")
    made = dict(zip(names, results[swaps:]))
    for name in ("inverse", "branch", "normed"):
        made[name] = made[name].reshape(seqs, length, -1)
    made["ring"], made["gets"] = ring_parts, results[:swaps]
    return made


def grad_ring(pairs, gives, order, rest, collective_id):
    size, count, swaps = len(order), len(pairs), len(gives)
    vmem = pl.BlockSpec(memory_space=pltpu.VMEM)
    anywhere = pl.BlockSpec(memory_space=pl.ANY)
    halves = [(left.shape[1] // (2 * size), right.shape[1]) for left, right, _ in pairs]
    moved = sum(4 * 2 * (size - 1) * rows * cols for rows, cols in halves)
    if rest:
        whole = (halves[0][0], sum(cols for _, cols in halves))
        shapes = [whole] * (2 * (rest + 1))
    else:
        shapes = [
            (parts, 2 * rows, cols // parts) for (rows, cols), (_, _, parts) in zip(halves, pairs)
        ]
    results = pl.pallas_call(
        functools.partial(grad_ring_kernel, order, count, swaps, rest),
        out_shape=[jax.ShapeDtypeStruct(shape, jnp.float32) for shape in shapes]
        + [jax.ShapeDtypeStruct(give.shape, give.dtype) for give in gives],
        in_specs=[vmem] * (2 * count) + [anywhere] * swaps,
        out_specs=[vmem] * len(shapes) + [anywhere] * swaps,
        scratch_shapes=ring_scratch(size, halves, [left.shape for left, _, _ in pairs])
        + [pltpu.SemaphoreType.DMA((2, swaps))],
        compiler_params=pltpu.CompilerParams(
            collective_id=collective_id, has_side_effects=True, vmem_limit_bytes=58 << 20
        ),
        cost_estimate=pl.CostEstimate(flops=moved * 10000, bytes_accessed=moved, transcendentals=0),
    )(*[left for left, _, _ in pairs], *[right for _, right, _ in pairs], *gives)
    return results[: len(shapes)], results[len(shapes) :]


def ring_rest(parts, order, rest):
    size = len(order)
    ahead = [(order[index], order[(index + 1) % size]) for index in range(size)]
    ways = (ahead, [(second, first) for first, second in ahead])
    totals = list(parts[:2])
    for later in range(rest):
        for way in range(2):
            totals[way] = lax.ppermute(totals[way], "dp", ways[way])
        for way in range(2):
            totals[way] = totals[way] + parts[2 * (later + 1) + way]
    return totals


def by_columns(totals, pairs):
    blocks, start = [], 0
    for _, right, split in pairs:
        width = right.shape[1] // split
        blocks.append(
            jnp.stack(
                [
                    jnp.concatenate(
                        [total[:, start + part * width : start + (part + 1) * width] for total in totals]
                    )
                    for part in range(split)
                ]
            )
        )
        start += right.shape[1]
    return blocks


def by_rows(totals):
    half = totals[0].shape[0] // 2
    return [
        jnp.concatenate([total[which * half : (which + 1) * half] for total in totals])[None]
        for which in range(2)
    ]


def on_device(
    order,
    tensor_size,
    input_img,
    input_txt,
    conditioning,
    ada_weight,
    ada_bias,
    qkv_weight,
    qkv_bias,
    norm_gain,
    proj_weight,
    proj_bias,
    up_weight,
    up_bias,
    down_weight,
    down_bias,
    cotangent_img,
    cotangent_txt,
):
    data_size = len(order)
    seqs, _, feat = input_img.shape
    core = lax.axis_index("tensor") % 2
    reals = (input_img.shape[1] // 2, input_txt.shape[1] // 2)

    def split_rows(array):
        half = array.shape[1] // 2
        pad = -half % ROW_TILE
        lower, upper = (
            jnp.pad(part, ((0, 0), (0, pad), (0, 0))) for part in (array[:, :half], array[:, half:])
        )
        first = core == 0
        return jnp.stack([jnp.where(first, lower, upper), jnp.where(first, upper, lower)])

    def join_rows(halves, real):
        own, other = halves.astype(jnp.bfloat16)
        first = core == 0
        lower, upper = jnp.where(first, own, other), jnp.where(first, other, own)
        return jnp.concatenate([lower[:, :real], upper[:, :real]], axis=1)

    ada_weight = ada_weight.transpose(0, 2, 1)
    modulate = mod_forward(
        conditioning, ada_weight, ada_bias, seqs, feat, data_size, tensor_size
    )
    piece = [
        [modulate[stream * 6 + index][:, None, :] for index in range(6)] for stream in range(2)
    ]

    inputs = [split_rows(input_img), split_rows(input_txt)]
    cotangents = [split_rows(cotangent_img), split_rows(cotangent_txt)]
    shapes = [array.shape for array in inputs]
    gain_pair = jnp.concatenate([norm_gain, norm_gain], axis=2)

    hidden1, raw, stats1 = [], [], []
    for stream in range(2):
        normed, inverse = layer_norm(inputs[stream].astype(jnp.float32))
        hidden = (normed * (1.0 + piece[stream][1]) + piece[stream][0]).astype(jnp.bfloat16)
        hidden = hidden.reshape(-1, feat)
        flat = [
            dot_plain(hidden, qkv_weight[stream, :, part]) + qkv_bias[stream, part].astype(jnp.float32)
            for part in range(3)
        ]
        hidden1.append(hidden)
        raw.append([each.reshape(shapes[stream][:3] + (-1,)) for each in flat])
        stats1.append((normed[0], inverse[0]))
    attn = attn_forward(gain_pair, raw[0], raw[1], reals[1])
    local = attn[0].shape[3]

    def mlp_stage(stream, got, gives, rest, collective_id):
        made = mlp_ring(
            stream,
            branch_sums[stream],
            got,
            inputs[stream],
            cotangents[stream],
            modulate,
            proj_bias,
            up_bias,
            up_weight,
            down_weight,
            gives,
            order,
            rest,
            collective_id,
        )
        if rest:
            made["ring"] = by_rows(ring_rest(made["ring"], order, rest))
        return made

    branch_sums = [None, None]
    for stream in (1, 0):
        rows = attn[stream].reshape(2, -1, local)
        branch_sums[stream] = core_sum(
            dot_plain(rows[0], proj_weight[stream]),
            dot_plain(rows[1], proj_weight[stream]),
            tensor_size,
        )
    state = [None, None]
    got = lax.ppermute(branch_sums[1], "tensor", swap_pairs(tensor_size, 2))
    state[1] = mlp_stage(1, got, [branch_sums[0]], RESTS[0], 2)
    state[0] = mlp_stage(0, state[1]["gets"][0], [], RESTS[1], 3)
    mlp_rings = [state[stream]["ring"] for stream in range(2)]
    hidden_sums = [state[stream]["hidden_sum"] + state[stream]["hidden_got"] for stream in range(2)]
    mlp_sums = [state[stream]["mlp_sum"] + state[stream]["mlp_got"] for stream in range(2)]

    grad_attn, proj_pairs, proj_sums, resid_grads, mod_grads = ([None, None] for _ in range(5))
    outputs = [None, None]
    for stream in (1, 0):
        branch, normed, inverse = (state[stream][key] for key in ("branch", "normed", "inverse"))
        grad_out = cotangents[stream][0].astype(jnp.float32)
        grad_hidden = hidden_sums[stream].reshape(normed.shape)
        through = norm_back(grad_hidden * (1.0 + piece[stream][4]), normed, inverse)
        grad_resid = grad_out + through
        grad_branch = share(grad_resid, tensor_size) * piece[stream][2]
        branch_low = grad_branch.astype(jnp.bfloat16).reshape(-1, feat)
        grad_attn[stream] = (
            dot_right_t(branch_low, proj_weight[stream])
            .astype(jnp.bfloat16)
            .reshape(attn[stream].shape)
        )
        proj_pairs[stream] = (branch_low, attn[stream].reshape(-1, local), 1)
        proj_sums[stream] = jnp.sum(grad_resid * piece[stream][2], axis=(0, 1))
        resid_grads[stream] = through
        mod_grads[stream] = [
            None,
            None,
            jnp.sum(grad_resid * branch, axis=1),
            jnp.sum(grad_hidden, axis=1),
            jnp.sum(grad_hidden * normed, axis=1),
            None,
        ]
    grad_packed = attn_backward(gain_pair, raw[0], raw[1], grad_attn[0], grad_attn[1], reals[1])
    qkv_bias_sums = jnp.sum(grad_packed[2], axis=0)
    gain_sums = jnp.sum(grad_packed[3], axis=0)
    head_dim = norm_gain.shape[2]
    gain_sums = gain_sums[:, :head_dim] + gain_sums[:, head_dim:]
    qkv_pairs, first_sums = [None, None], [None, None]
    for stream in (1, 0):
        packed_low = grad_packed[stream].reshape(-1, 3 * local)
        half = packed_low.shape[0] // 2

        def through_weights(rows):
            return sum(
                dot_right_t(
                    packed_low[rows, part * local : (part + 1) * local], qkv_weight[stream, :, part]
                )
                for part in range(3)
            )

        first_sums[stream] = core_sum(
            through_weights(slice(None, half)),
            through_weights(slice(half, None)),
            tensor_size,
        )
        qkv_pairs[stream] = (hidden1[stream], packed_low, 3)
    pairs = qkv_pairs + proj_pairs
    rings, swapped = grad_ring(pairs, first_sums, order, RESTS[2], 4)
    if RESTS[2]:
        rings = by_columns(ring_rest(rings, order, RESTS[2]), pairs)
    qkv_rings, proj_rings = rings[:2], rings[2:]
    first_sums = [give + get for give, get in zip(first_sums, swapped)]

    grad_inputs = [None, None]
    for stream in (1, 0):
        branch = state[stream]["branch"]
        grad_out = cotangents[stream][0].astype(jnp.float32)
        mlp_out = mlp_sums[stream].reshape(branch.shape) + down_bias[stream]
        added = piece[stream][2] * branch + piece[stream][5] * mlp_out
        outputs[stream] = join_rows(
            inputs[stream].astype(jnp.float32) + share(added, tensor_size), reals[stream]
        )
        mod_grads[stream][5] = jnp.sum(grad_out * mlp_out, axis=1)
        normed, inverse = stats1[stream]
        grad_hidden = first_sums[stream].reshape(normed.shape)
        added = resid_grads[stream] + norm_back(
            grad_hidden * (1.0 + piece[stream][1]), normed, inverse
        )
        grad_inputs[stream] = join_rows(
            cotangents[stream].astype(jnp.float32) + share(added, tensor_size), reals[stream]
        )
        mod_grads[stream][0] = jnp.sum(grad_hidden, axis=1)
        mod_grads[stream][1] = jnp.sum(grad_hidden * normed, axis=1)

    row_share = 2.0 / tensor_size
    sums = mod_backward(
        jnp.stack(mod_grads[0] + mod_grads[1]),
        conditioning,
        ada_weight,
        [qkv_bias_sums, jnp.concatenate([state[0]["up_bias"], state[1]["up_bias"]])],
        [
            gain_sums,
            jnp.stack(proj_sums) * row_share,
            jnp.concatenate([state[0]["down_bias"], state[1]["down_bias"]]) * row_share,
        ],
        data_size,
        tensor_size,
    )
    grad_ada_weight, grad_ada_bias, silu_rows, qkv_bias_sums, up_bias_sums = sums[:5]
    gain_sums, proj_sums, down_sums = sums[5:]
    own_cond = lax.dynamic_slice_in_dim(
        conditioning, lax.axis_index("dp") * seqs, seqs, axis=0
    ).astype(jnp.float32)
    own_sig = jax.nn.sigmoid(own_cond)
    grad_conditioning = silu_rows * own_sig * (1.0 + own_cond * (1.0 - own_sig))
    down_rings, up_rings = ([mlp_rings[0][index], mlp_rings[1][index]] for index in range(2))
    return (
        outputs[0],
        outputs[1],
        grad_inputs[0],
        grad_inputs[1],
        grad_conditioning,
        grad_ada_weight.transpose(0, 2, 1),
        grad_ada_bias,
        jnp.stack(qkv_rings).transpose(0, 2, 1, 3),
        qkv_bias_sums.reshape(2, 3, -1),
        gain_sums.reshape(norm_gain.shape),
        jnp.concatenate(proj_rings).transpose(0, 2, 1),
        proj_sums,
        jnp.concatenate(up_rings),
        up_bias_sums,
        jnp.concatenate(down_rings).transpose(0, 2, 1),
        down_sums,
    )


def solution(mesh):
    in_specs = (
        P("dp", None, None),
        P("dp", None, None),
        P(),
        P(None, None, ("dp", "tensor")),
        P(None, ("dp", "tensor")),
        P(None, None, None, "tensor"),
        P(None, None, "tensor"),
        P(),
        P(None, "tensor", None),
        P(),
        P(None, None, "tensor"),
        P(None, "tensor"),
        P(None, "tensor", None),
        P(),
        P("dp", None, None),
        P("dp", None, None),
    )
    out_specs = (
        P("dp", None, None),
        P("dp", None, None),
        P("dp", None, None),
        P("dp", None, None),
        P("dp", None),
        P(None, None, ("dp", "tensor")),
        P(None, ("dp", "tensor")),
        P(None, "dp", None, "tensor"),
        P(None, None, "tensor"),
        P(),
        P(None, "tensor", "dp"),
        P(),
        P(None, "dp", "tensor"),
        P(None, "tensor"),
        P(None, "tensor", "dp"),
        P(),
    )

    def step(*arrays):
        return on_device(ring_order(mesh), mesh.shape["tensor"], *arrays)

    return jax.shard_map(step, mesh=mesh, in_specs=in_specs, out_specs=out_specs, check_vma=False)
```

```python
import functools

import jax
import jax.numpy as jnp
from jax import lax
from jax.experimental import pallas as pl
from jax.experimental.pallas import tpu as pltpu
from jax.sharding import PartitionSpec as P


epsilon = 1e-06
GELU_C = 0.7978845608028654
GELU_A = 0.044715
ROW_TILE = 16
NEG = -1e30
RESTS = (1, 1)


def dot_plain(first_op, second_op):
    return jnp.dot(first_op, second_op, preferred_element_type=jnp.float32)


def dot_right_t(first_op, second_op):
    return lax.dot_general(
        first_op, second_op, (((1,), (1,)), ((), ())), preferred_element_type=jnp.float32
    )


def dot_left_t(first_op, second_op):
    return lax.dot_general(
        first_op, second_op, (((0,), (0,)), ((), ())), preferred_element_type=jnp.float32
    )


def layer_norm(values):
    center = values - jnp.mean(values, axis=-1, keepdims=True)
    inverse = lax.rsqrt(jnp.mean(center * center, axis=-1, keepdims=True) + epsilon)
    return (center * inverse, inverse)


def norm_back(grad_normed, normed, inverse):
    return inverse * (
        grad_normed
        - jnp.mean(grad_normed, axis=-1, keepdims=True)
        - normed * jnp.mean(grad_normed * normed, axis=-1, keepdims=True)
    )


def gelu_both(values):
    inner = jnp.tanh(GELU_C * (values + GELU_A * values * values * values))
    active = 0.5 * values * (1.0 + inner)
    slope = 0.5 * (1.0 + inner) + 0.5 * values * (1.0 - inner * inner) * GELU_C * (
        1.0 + 3.0 * GELU_A * values * values
    )
    return active, slope


def head_norm(values, gain):
    head_dim = values.shape[1] // 2
    lower = lax.broadcasted_iota(jnp.int32, values.shape, 1) < head_dim
    square = values * values
    first = jnp.sum(jnp.where(lower, square, 0.0), axis=-1, keepdims=True) / head_dim
    second = jnp.sum(jnp.where(lower, 0.0, square), axis=-1, keepdims=True) / head_dim
    factor = jnp.where(lower, lax.rsqrt(first + epsilon), lax.rsqrt(second + epsilon))
    return values * factor * gain, factor


def rows_of(img_ref, txt_ref, cols):
    return jnp.concatenate(
        [img_ref[0, 0, :, cols], img_ref[1, 0, :, cols], txt_ref[0, 0, :, cols], txt_ref[1, 0, :, cols]],
        axis=0,
    )


def put_rows(img_ref, txt_ref, cols, values):
    img, txt = img_ref.shape[2], txt_ref.shape[2]
    img_ref[0, 0, :, cols] = values[:img]
    img_ref[1, 0, :, cols] = values[img : 2 * img]
    txt_ref[0, 0, :, cols] = values[2 * img : 2 * img + txt]
    txt_ref[1, 0, :, cols] = values[2 * img + txt :]


def gain_rows(gain_ref, which, img, txt):
    width = gain_ref.shape[2]
    return jnp.concatenate(
        [
            jnp.broadcast_to(gain_ref[0, which : which + 1, :], (2 * img, width)),
            jnp.broadcast_to(gain_ref[1, which : which + 1, :], (2 * txt, width)),
        ],
        axis=0,
    )


def key_bias(img, txt, real):
    where = lax.broadcasted_iota(jnp.int32, (1, 2 * (img + txt)), 1)
    first = where - 2 * img
    gone = ((first >= real) & (first < txt)) | (first >= txt + real)
    return jnp.where(gone, NEG, 0.0).astype(jnp.float32)


def probs(q_head, k_low, bias):
    scores = dot_right_t(q_head, k_low) + bias
    top = jnp.max(scores, axis=-1, keepdims=True)
    weights = jnp.exp(scores - top)
    return weights * (1.0 / jnp.sum(weights, axis=-1, keepdims=True))


def attn_forward_kernel(real, gain_ref, *refs):
    raw_refs, (out_img_ref, out_txt_ref) = (refs[:3], refs[3:6]), refs[6:]
    img, txt = out_img_ref.shape[2], out_txt_ref.shape[2]
    local = out_img_ref.shape[3]
    pair = gain_ref.shape[2]
    q_gain, k_gain = gain_rows(gain_ref, 0, img, txt), gain_rows(gain_ref, 1, img, txt)
    bias = key_bias(img, txt, real)
    scale = (pair // 2) ** (-0.5)
    for start in range(0, local, pair):
        q_raw, k_raw, v_raw = (
            rows_of(raw_refs[0][part], raw_refs[1][part], slice(start, start + pair))
            for part in range(3)
        )
        q_low = head_norm(q_raw, q_gain)[0].astype(jnp.bfloat16) * jnp.bfloat16(scale)
        k_low = head_norm(k_raw, k_gain)[0].astype(jnp.bfloat16)
        v_low = v_raw.astype(jnp.bfloat16)
        lower = lax.broadcasted_iota(jnp.int32, q_raw.shape, 1) < pair // 2
        results = []
        for head in range(2):
            mine = lower if head == 0 else jnp.logical_not(lower)
            q_head = jnp.where(mine, q_low, jnp.bfloat16(0))
            results.append(dot_plain(probs(q_head, k_low, bias).astype(jnp.bfloat16), v_low))
        out = jnp.where(lower, results[0], results[1]).astype(jnp.bfloat16)
        put_rows(out_img_ref, out_txt_ref, slice(start, start + pair), out)


def attn_backward_kernel(real, gain_ref, *refs):
    raw_refs = (refs[:3], refs[3:6])
    d_img_ref, d_txt_ref, o_img_ref, o_txt_ref, bias_ref, dgain_ref = refs[6:]
    img, txt = d_img_ref.shape[2], d_txt_ref.shape[2]
    local = d_img_ref.shape[3]
    pair = gain_ref.shape[2]
    head_dim = pair // 2
    q_gain, k_gain = gain_rows(gain_ref, 0, img, txt), gain_rows(gain_ref, 1, img, txt)
    bias = key_bias(img, txt, real)
    scale = head_dim ** (-0.5)
    gain_sums = [[None, None], [None, None]]
    for start in range(0, local, pair):
        q_raw, k_raw, v_raw = (
            rows_of(raw_refs[0][part], raw_refs[1][part], slice(start, start + pair))
            for part in range(3)
        )
        q_wide, q_factor = head_norm(q_raw, q_gain)
        k_wide, k_factor = head_norm(k_raw, k_gain)
        q_low = q_wide.astype(jnp.bfloat16) * jnp.bfloat16(scale)
        k_low = k_wide.astype(jnp.bfloat16)
        v_low = v_raw.astype(jnp.bfloat16)
        grad_out = rows_of(d_img_ref, d_txt_ref, slice(start, start + pair))
        lower = lax.broadcasted_iota(jnp.int32, q_raw.shape, 1) < head_dim
        parts = []
        for head in range(2):
            mine = lower if head == 0 else jnp.logical_not(lower)
            prob = probs(jnp.where(mine, q_low, jnp.bfloat16(0)), k_low, bias)
            grad_v = dot_left_t(prob.astype(jnp.bfloat16), grad_out)
            grad_prob = dot_right_t(jnp.where(mine, grad_out, jnp.bfloat16(0)), v_low)
            delta = jnp.sum(prob * grad_prob, axis=-1, keepdims=True)
            grad_scores = (prob * (grad_prob - delta)).astype(jnp.bfloat16)
            parts.append((dot_plain(grad_scores, k_low), dot_left_t(grad_scores, q_low), grad_v))
        grad_qn = jnp.where(lower, parts[0][0], parts[1][0]) * scale
        grad_kn = jnp.where(lower, parts[0][1], parts[1][1])
        grad_vn = jnp.where(lower, parts[0][2], parts[1][2])

        def raw_grad(grad_normed, raw, factor, gain, which):
            gained = grad_normed * gain
            product = gained * raw
            first = jnp.sum(jnp.where(lower, product, 0.0), axis=-1, keepdims=True) / head_dim
            second = jnp.sum(jnp.where(lower, 0.0, product), axis=-1, keepdims=True) / head_dim
            inner = jnp.where(lower, first, second)
            terms = grad_normed * raw * factor
            for stream, rows in enumerate((slice(0, 2 * img), slice(2 * img, 2 * (img + txt)))):
                total = jnp.sum(terms[rows], axis=0, keepdims=True)
                old = gain_sums[stream][which]
                gain_sums[stream][which] = total if old is None else old + total
            return factor * gained - raw * (factor * factor * factor) * inner

        grads = (
            raw_grad(grad_qn, q_raw, q_factor, q_gain, 0),
            raw_grad(grad_kn, k_raw, k_factor, k_gain, 1),
            grad_vn,
        )
        for part, grad in enumerate(grads):
            cols = slice(part * local + start, part * local + start + pair)
            bias_ref[0, 0:1, cols] = jnp.sum(grad[: 2 * img], axis=0, keepdims=True)
            bias_ref[0, 1:2, cols] = jnp.sum(grad[2 * img :], axis=0, keepdims=True)
            put_rows(o_img_ref, o_txt_ref, cols, grad.astype(jnp.bfloat16))
    for stream in range(2):
        for which in range(2):
            row = stream * 2 + which
            dgain_ref[0, row : row + 1, :] = gain_sums[stream][which]


def block_of(array):
    shape = array.shape
    return pl.BlockSpec((shape[0], 1) + shape[2:], lambda seq: (0, seq, 0, 0))


def whole_of(array):
    return pl.BlockSpec(array.shape, lambda seq: (0,) * array.ndim)


def attn_forward(gain_pair, raw_img, raw_txt, real):
    seqs, local = raw_img[0].shape[1], raw_img[0].shape[3]
    outs = [jax.ShapeDtypeStruct(raw[0].shape, jnp.bfloat16) for raw in (raw_img, raw_txt)]
    rows = 2 * (raw_img[0].shape[2] + raw_txt[0].shape[2])
    return pl.pallas_call(
        functools.partial(attn_forward_kernel, real),
        grid=(seqs,),
        out_shape=outs,
        in_specs=[whole_of(gain_pair)] + [block_of(raw) for raw in raw_img + raw_txt],
        out_specs=[block_of(out) for out in outs],
        compiler_params=pltpu.CompilerParams(vmem_limit_bytes=48 << 20),
        cost_estimate=pl.CostEstimate(
            flops=seqs * rows * rows * local * 4,
            bytes_accessed=seqs * rows * local * 14,
            transcendentals=seqs * rows * rows * (local // 64),
        ),
        name="attn_forward",
    )(gain_pair, *raw_img, *raw_txt)


def attn_backward(gain_pair, raw_img, raw_txt, grad_img, grad_txt, real):
    seqs, local = raw_img[0].shape[1], raw_img[0].shape[3]
    outs = [
        jax.ShapeDtypeStruct(raw_img[0].shape[:3] + (3 * local,), jnp.bfloat16),
        jax.ShapeDtypeStruct(raw_txt[0].shape[:3] + (3 * local,), jnp.bfloat16),
        jax.ShapeDtypeStruct((seqs, 2, 3 * local), jnp.float32),
        jax.ShapeDtypeStruct((seqs, 4, gain_pair.shape[2]), jnp.float32),
    ]
    rows = 2 * (raw_img[0].shape[2] + raw_txt[0].shape[2])
    return pl.pallas_call(
        functools.partial(attn_backward_kernel, real),
        grid=(seqs,),
        out_shape=outs,
        in_specs=[whole_of(gain_pair)]
        + [block_of(each) for each in raw_img + raw_txt + [grad_img, grad_txt]],
        out_specs=[
            block_of(outs[0]),
            block_of(outs[1]),
            pl.BlockSpec((1, 2, 3 * local), lambda seq: (seq, 0, 0)),
            pl.BlockSpec((1, 4, gain_pair.shape[2]), lambda seq: (seq, 0, 0)),
        ],
        compiler_params=pltpu.CompilerParams(vmem_limit_bytes=56 << 20),
        cost_estimate=pl.CostEstimate(
            flops=seqs * rows * rows * local * 10,
            bytes_accessed=seqs * rows * local * 20,
            transcendentals=seqs * rows * rows * (local // 64),
        ),
        name="attn_backward",
    )(gain_pair, *raw_img, *raw_txt, grad_img, grad_txt)


def xor_index(index, distance):
    return index + distance - 2 * distance * ((index // distance) % 2)


def peers_of(data_size, tensor_size):
    row, col = lax.axis_index("dp"), lax.axis_index("tensor")
    around = [(lax.rem(row + step, data_size), col) for step in range(1, data_size)]
    across = []
    distance = 1
    while distance < tensor_size:
        across.append((row, xor_index(col, distance)))
        distance *= 2
    return row, col, around, across


def greet(partners):
    barrier = pltpu.get_barrier_semaphore()
    for partner in partners:
        pl.semaphore_signal(barrier, inc=1, device_id=partner, device_id_type=pl.DeviceIdType.MESH)
    pl.semaphore_wait(barrier, len(partners))


def remote(source, target, sems, index, partner):
    copy = pltpu.make_async_remote_copy(
        src_ref=source,
        dst_ref=target,
        send_sem=sems.at[0, index],
        recv_sem=sems.at[1, index],
        device_id=partner,
        device_id_type=pl.DeviceIdType.MESH,
    )
    copy.start()
    return copy


def silu_of(cond_ref):
    wide = cond_ref[...].astype(jnp.float32)
    return (wide * (1.0 / (1.0 + jnp.exp(-wide)))).astype(jnp.bfloat16)


def mod_forward_kernel(
    data_size, tensor_size, cond_ref, weight_ref, bias_ref, out_ref, outgoing, blocks, sems
):
    row, col, around, across = peers_of(data_size, tensor_size)
    seqs, feat = out_ref.shape[1], out_ref.shape[2]
    silu_cond = silu_of(cond_ref)
    for stream in range(2):
        values = dot_right_t(silu_cond, weight_ref[stream]) + bias_ref[stream : stream + 1].astype(
            jnp.float32
        )
        for index in range(data_size):
            outgoing[index, stream * seqs : (stream + 1) * seqs] = values[
                index * seqs : (index + 1) * seqs
            ]
    blocks[col, row] = outgoing[row]
    greet(around + across)
    copies = [
        remote(outgoing.at[partner[0]], blocks.at[col, row], sems, index, partner)
        for index, partner in enumerate(around)
    ]
    for copy in copies:
        copy.wait()
    held, used = [0], len(around)
    for level in reversed(range(len(across))):
        distance = 1 << level
        copies = []
        for offset in held:
            index = col
            for bit in range(len(across)):
                if offset >> bit & 1:
                    index = xor_index(index, 1 << bit)
            copies.append(remote(blocks.at[index], blocks.at[index], sems, used, across[level]))
            used += 1
        for copy in copies:
            copy.wait()
        held = held + [offset | distance for offset in held]
    for stream in range(2):
        full = jnp.concatenate(
            [
                blocks[second, first, stream * seqs : (stream + 1) * seqs]
                for first in range(data_size)
                for second in range(tensor_size)
            ],
            axis=1,
        )
        for index in range(6):
            out_ref[stream * 6 + index] = full[:, index * feat : (index + 1) * feat]


def mod_forward(conditioning, ada_weight, ada_bias, seqs, feat, data_size, tensor_size):
    cols = ada_weight.shape[1]
    vmem = pl.BlockSpec(memory_space=pltpu.VMEM)
    return pl.pallas_call(
        functools.partial(mod_forward_kernel, data_size, tensor_size),
        out_shape=jax.ShapeDtypeStruct((12, seqs, feat), jnp.float32),
        in_specs=[vmem] * 3,
        out_specs=vmem,
        scratch_shapes=[
            pltpu.VMEM((data_size, 2 * seqs, cols), jnp.float32),
            pltpu.VMEM((tensor_size, data_size, 2 * seqs, cols), jnp.float32),
            pltpu.SemaphoreType.DMA((2, data_size + tensor_size)),
        ],
        compiler_params=pltpu.CompilerParams(
            collective_id=0, has_side_effects=True, vmem_limit_bytes=32 << 20
        ),
        name="mod_forward",
    )(conditioning, ada_weight, ada_bias)


def mod_backward_steps(data_size, tensor_size, mod_rows, cond_ref, weight_of, lines_of, put, scratch, sems):
    blocks, core_in, outgoing, cols_in, lines, lines_in, lines_own, lines_all = scratch[:8]
    silu_blocks, silu_in, silu_send, silu_recv, all_send, all_recv = scratch[8:]
    row, col, around, across = peers_of(data_size, tensor_size)
    seqs, cols = outgoing.shape[1] // 2, outgoing.shape[2]
    half, width = lines.shape[1] // 2, lines.shape[2]
    for stream in range(2):
        full = mod_rows(stream)
        for first in range(data_size):
            for second in range(tensor_size):
                start = (first * tensor_size + second) * cols
                blocks[second, first, stream * seqs : (stream + 1) * seqs] = full[
                    :, start : start + cols
                ]
    every_line = lines_of()
    for index in range(data_size):
        lines[index] = every_line[:, index * width : (index + 1) * width]

    used = 0
    copy = remote(blocks.at[xor_index(col, 1)], core_in, sems, used, across[0])
    used += 1
    yield
    copy.wait()
    for first in range(data_size):
        outgoing[first] = blocks[col, first] + core_in[first]

    cols_in[row] = outgoing[row]
    lines_in[row] = lines[row]
    copies = []
    for partner in around:
        for source, target in ((lines, lines_in), (outgoing, cols_in)):
            copies.append(
                remote(source.at[partner[0]], target.at[row], sems, used, partner)
            )
            used += 1
    silu_cond = silu_of(cond_ref)
    yield
    for copy in copies:
        copy.wait()
    lines_own[...] = functools.reduce(jnp.add, [lines_in[index] for index in range(data_size)])
    low = []
    for stream in range(2):
        wide = jnp.concatenate(
            [cols_in[index, stream * seqs : (stream + 1) * seqs] for index in range(data_size)],
            axis=0,
        )
        put(("ada_bias", stream), jnp.sum(wide, axis=0, keepdims=True))
        low.append(wide.astype(jnp.bfloat16))
    silu_grad = dot_plain(low[0], weight_of(0)) + dot_plain(low[1], weight_of(1))
    for index in range(data_size):
        silu_blocks[index] = silu_grad[index * seqs : (index + 1) * seqs]
    for stream in range(2):
        put(("ada_weight", stream), lambda span: dot_left_t(low[stream], silu_cond[:, span]))

    silu_in[row] = silu_blocks[row]
    lines_all[row] = lines_own[...]
    copies = []
    for partner in around:
        for source, target in (
            (silu_blocks.at[partner[0]], silu_in.at[row]),
            (lines_own, lines_all.at[row]),
        ):
            copies.append(remote(source, target, sems, used, partner))
            used += 1
    yield
    for copy in copies:
        copy.wait()
    silu_send[0] = functools.reduce(jnp.add, [silu_in[index] for index in range(data_size)])
    every_line = jnp.concatenate([lines_all[index] for index in range(data_size)], axis=1)
    all_send[0] = every_line[half:]
    put("group", every_line[:half])

    for level, partner in enumerate(across):
        copies = [
            remote(silu_send.at[level], silu_recv.at[level], sems, used, partner),
            remote(all_send.at[level], all_recv.at[level], sems, used + 1, partner),
        ]
        used += 2
        yield
        for copy in copies:
            copy.wait()
        silu_send[level + 1] = silu_send[level] + silu_recv[level]
        all_send[level + 1] = all_send[level] + all_recv[level]
    put("silu", silu_send[len(across)])
    put("every", all_send[len(across)])


def mod_scratch(data_size, tensor_size, seqs, feat, cols):
    levels, lines = tensor_size.bit_length() - 1, 16
    width = feat // data_size

    def wide(*shape):
        return pltpu.VMEM(shape, jnp.float32)

    return [
        wide(tensor_size, data_size, 2 * seqs, cols),
        wide(data_size, 2 * seqs, cols),
        wide(data_size, 2 * seqs, cols),
        wide(data_size, 2 * seqs, cols),
        wide(data_size, lines, width),
        wide(data_size, lines, width),
        wide(lines, width),
        wide(data_size, lines, width),
        wide(data_size, seqs, feat),
        wide(data_size, seqs, feat),
        wide(levels + 1, seqs, feat),
        wide(levels, seqs, feat),
        wide(levels + 1, lines // 2, feat),
        wide(levels, lines // 2, feat),
    ], pltpu.SemaphoreType.DMA((2, 1 + 4 * (data_size - 1) + 2 * levels))


def norm_of(values):
    center = values - jnp.mean(values, axis=-1, keepdims=True)
    inverse = lax.rsqrt(jnp.mean(center * center, axis=-1, keepdims=True) + epsilon)
    return center * inverse, inverse


def swap_pairs(size, distance):
    return [(index, index ^ distance) for index in range(size)]


def core_sum(own_part, other_part, tensor_size):
    return own_part + lax.ppermute(other_part, "tensor", swap_pairs(tensor_size, 1))


def ring_order(mesh):
    size = mesh.shape["dp"]
    fallback = list(range(0, size, 2)) + list(range(1, size, 2))[::-1]
    axis = list(mesh.axis_names).index("dp")
    devices = mesh.devices
    line = [devices[(slice(None),) * axis + (index,)].flatten()[0] for index in range(size)]
    coords = [getattr(device, "coords", None) for device in line]
    if any(place is None for place in coords):
        return fallback
    near = [
        [
            other
            for other in range(size)
            if sum(abs(a - b) for a, b in zip(coords[index], coords[other])) == 1
        ]
        for index in range(size)
    ]
    path, seen, budget = [0], {0}, [200000]

    def extend():
        budget[0] -= 1
        if budget[0] < 0:
            return False
        if len(path) == size:
            return path[0] in near[path[-1]]
        choices = [index for index in near[path[-1]] if index not in seen]
        choices.sort(key=lambda index: (sum(o not in seen for o in near[index]), index))
        for index in choices:
            path.append(index)
            seen.add(index)
            if extend():
                return True
            path.pop()
            seen.remove(index)
        return False

    return path if extend() else fallback


def entry_of(table, index):
    value = jnp.int32(table[0])
    for place in range(1, len(table)):
        value = jnp.where(index == place, jnp.int32(table[place]), value)
    return value


def over_rows(base, length, feat, count, body):
    tile = ROW_TILE
    group = next(size for size in (4, 5, 3, 2, 1) if length // tile % size == 0)

    def step(index, carry):
        for place in range(group):
            start = pl.multiple_of(base + (index * group + place) * tile, tile)
            adds = body(pl.ds(start, tile))
            carry = tuple(
                total + add[: tile // 2] + add[tile // 2 :] for total, add in zip(carry, adds)
            )
        return carry

    zero = jnp.zeros((tile // 2, feat), jnp.float32)
    totals = lax.fori_loop(0, length // (tile * group), step, (zero,) * count)
    return [jnp.sum(total, axis=0, keepdims=True) for total in totals]


def shifted(rows, by):
    return pl.ds(pl.multiple_of(rows.start + by, ROW_TILE), rows.size)


class Ring:
    def __init__(self, order, rest, lefts, rights, slots, terms, turned, sems):
        self.order, self.size, self.rest = order, len(order), rest
        self.lefts, self.rights, self.slots, self.terms = lefts, rights, slots, terms
        self.turned, self.sems = turned, sems
        row, col = lax.axis_index("dp"), lax.axis_index("tensor")
        size = self.size
        self.place = entry_of([order.index(index) for index in range(size)], row)
        self.after = entry_of(order, lax.rem(self.place + 1, size))
        self.before = entry_of(order, lax.rem(self.place + size - 1, size))
        self.targets = ((self.after, col), (self.before, col))
        self.half = slots[0].shape[2]
        self.chains = [(which, way) for which in range(len(lefts)) for way in range(2)]
        self.last = size - 2 - rest

    def term(self, which, way, index):
        start = pl.multiple_of((2 * index + way) * self.half, 8)
        return dot_plain(
            self.turned[which][pl.ds(start, self.half), :], self.rights[which][...]
        )

    def work_out(self, indices):
        for which, way in self.chains:
            self.terms[which][way] = self.term(which, way, indices[way])

    def copy_of(self, which, way, step, source, target):
        return pltpu.make_async_remote_copy(
            src_ref=source,
            dst_ref=self.slots[which].at[way, target],
            send_sem=self.sems.at[0, which, way, step],
            recv_sem=self.sems.at[1, which, way, step],
            device_id=self.targets[way],
            device_id_type=pl.DeviceIdType.MESH,
        )

    def blocks_at(self, step):
        size = self.size
        return (
            entry_of(self.order, lax.rem(self.place + 2 * size - 2 - step, size)),
            entry_of(self.order, lax.rem(self.place + 2 + step, size)),
        )

    def arrive(self, which, way, step):
        slot = self.slots[which].at[way, step]
        self.copy_of(which, way, step, slot, step).wait_recv()

    def begin(self, which):
        width = 256
        for start in range(0, self.turned[which].shape[0], width):
            self.turned[which][start : start + width] = self.lefts[which][:, start : start + width].T
        for way in range(2):
            first = self.slots[which].at[way, self.size - 1]
            first[...] = self.term(which, way, (self.before, self.after)[way])
            self.copy_of(which, way, 0, first, 0).start()

    def rounds(self, first, last):
        def round_of(step, carry):
            self.work_out(self.blocks_at(step))
            for which, way in self.chains:
                self.arrive(which, way, step)
                slot = self.slots[which].at[way, step]
                slot[...] = slot[...] + self.terms[which][way]
                self.copy_of(which, way, step + 1, slot, step + 1).start()
            return carry

        lax.fori_loop(first, last, round_of, 0)

    def finish(self, put_later, put_total):
        for later in range(self.rest):
            indices = self.blocks_at(self.last + 1 + later)
            for which, way in self.chains:
                put_later(later, which, way, self.term(which, way, indices[way]))
        self.work_out(self.blocks_at(self.last))
        for which, way in self.chains:
            self.arrive(which, way, self.last)
            put_total(which, way, self.slots[which][way, self.last] + self.terms[which][way])

        def sent(step, carry):
            for which, way in self.chains:
                slot = self.slots[which].at[way, self.size - 1]
                self.copy_of(which, way, step, slot, step).wait_send()
            return carry

        lax.fori_loop(0, self.last + 1, sent, 0)


def taker(refs):
    refs = list(refs)

    def take(number):
        taken = refs[:number]
        del refs[:number]
        return taken

    return take


def ring_scratch(size, halves, lefts, count_kind=jnp.bfloat16):
    return (
        [pltpu.VMEM((2, size) + half, jnp.float32) for half in halves]
        + [pltpu.VMEM((2,) + half, jnp.float32) for half in halves]
        + [pltpu.VMEM(shape[::-1], count_kind) for shape in lefts]
        + [pltpu.SemaphoreType.DMA((2, len(halves), 2, size - 1))]
    )


def mlp_ring_kernel(order, stream, seqs, block, swaps, rest, *refs):
    take = taker(refs)
    mod_ref, proj_bias_ref, up_bias_ref, down_bias_ref = take(4)
    mine_hbm, got_hbm, input_hbm, cot_hbm, up_hbm, down_hbm, proj_hbm = take(7)
    gives = take(swaps)
    outs = take(2 * (rest + 1)) if rest else take(2)
    gets = take(swaps)
    up_sum_ref, down_sum_ref, proj_sum_ref, mod_sum_ref = take(4)
    branch_hbm, normed_hbm, hidden_got_hbm, mlp_got_hbm, through_hbm = take(5)
    grad_branch_hbm, grad_attn_hbm, out_hbm = take(3)
    slots, terms, turned = take(2), take(2), take(2)
    (ring_sems,) = take(1)
    up_ref, down_ref, input_ref, hidden_ref, active_ref, grad_up_ref, grad_mlp_ref = take(7)
    proj_ref, grad_attn_ref, inverse_ref = take(3)
    mine_ref, got_ref, branch_ref, normed_ref, normed_in, spare = take(6)
    load_sems, core_sems, swap_sems, out_sems, again_sems, ready_sem = take(6)
    rows, feat = mine_ref.shape
    units = active_ref.shape[1]
    length = rows // seqs
    ring = Ring(
        order, rest, (grad_mlp_ref, hidden_ref), (active_ref, grad_up_ref), slots, terms, turned, ring_sems
    )
    partner = (lax.axis_index("dp"), xor_index(lax.axis_index("tensor"), 1))
    facing = (lax.axis_index("dp"), xor_index(lax.axis_index("tensor"), 2))

    loads = []
    for source, target in (
        (mine_hbm, mine_ref),
        (got_hbm, got_ref),
        (input_hbm, input_ref),
        (cot_hbm, grad_mlp_ref),
        (up_hbm.at[stream], up_ref),
        (down_hbm.at[stream], down_ref),
        (proj_hbm.at[stream], proj_ref),
    ):
        loads.append(pltpu.make_async_copy(source, target, load_sems.at[len(loads)]))
        loads[-1].start()
    greet(ring.targets + (facing, partner))
    swapped = [
        remote(gives[index], gets[index], swap_sems, index, facing) for index in range(swaps)
    ]
    spans = [slice(seq * length, (seq + 1) * length) for seq in range(seqs)]
    other_spans = [slice(rows + seq * length, rows + (seq + 1) * length) for seq in range(seqs)]

    def mod(index, seq):
        return mod_ref[stream * 6 + index, seq : seq + 1, :]

    stored = []

    def store(source, target):
        copy = pltpu.make_async_copy(source, target, out_sems.at[len(stored)])
        copy.start()
        stored.append(copy)
        return copy

    loaded = []

    def load_again(source, target):
        copy = pltpu.make_async_copy(source, target, again_sems.at[len(loaded)])
        copy.start()
        loaded.append(copy)
        return copy

    def row_sum(values):
        return jnp.sum(values, axis=0, keepdims=True)

    for load in loads[:3]:
        load.wait()
    copies = []
    proj_bias = proj_bias_ref[stream : stream + 1].astype(jnp.float32)
    for seq, span in enumerate(spans):
        gate, shift, scale = mod(2, seq), mod(3, seq), 1.0 + mod(4, seq)

        def second_norm(at):
            branch = mine_ref[at] + got_ref[at] + proj_bias
            branch_ref[at] = branch
            normed, inverse = norm_of(input_ref[at].astype(jnp.float32) + gate * branch)
            normed_ref[at] = normed
            inverse_ref[at] = inverse
            hidden_ref[at] = (normed * scale + shift).astype(jnp.bfloat16)
            return ()

        over_rows(span.start, length, feat, 0, second_norm)
        copies.append(remote(normed_ref.at[span], normed_in.at[span], core_sems, seq, partner))
    kept = [store(branch_ref, branch_hbm), store(normed_ref, normed_hbm)]
    loads[3].wait()
    down_total = 0.0
    for half_spans in (spans, other_spans):
        for seq, span in enumerate(half_spans):
            gate = mod(5, seq)

            def gated(at):
                grad_mlp = grad_mlp_ref[at].astype(jnp.float32) * gate
                grad_mlp_ref[at] = grad_mlp.astype(jnp.bfloat16)
                return (grad_mlp,)

            (total,) = over_rows(span.start, length, feat, 1, gated)
            if half_spans is spans:
                down_total = down_total + total
    down_sum_ref[...] = down_total
    for seq, copy in enumerate(copies):
        copy.wait()
        shift, scale = mod(3, seq), 1.0 + mod(4, seq)

        def other_hidden(at):
            hidden_ref[shifted(at, rows)] = (normed_in[at] * scale + shift).astype(jnp.bfloat16)
            return ()

        over_rows(spans[seq].start, length, feat, 0, other_hidden)
    for load in loads[4:]:
        load.wait()

    def unit_block(index, carry):
        cols = pl.ds(pl.multiple_of(index * block, block), block)
        upward = dot_plain(hidden_ref[...], up_ref[:, cols]) + up_bias_ref[
            stream : stream + 1, cols
        ].astype(jnp.float32)
        active, slope = gelu_both(upward)
        active_ref[:, cols] = active.astype(jnp.bfloat16)
        grad_up = dot_right_t(grad_mlp_ref[...], down_ref[cols, :]) * slope
        up_sum_ref[:, cols] = row_sum(grad_up)
        grad_up_ref[:, cols] = grad_up.astype(jnp.bfloat16)
        return carry

    lax.fori_loop(0, units // block, unit_block, 0)
    for which in range(2):
        ring.begin(which)

    for copy in kept:
        copy.wait()
    count = feat // block
    sums = ((branch_ref, mine_ref, normed_in), (normed_ref, got_ref, spare))
    copies = []
    for kind, (outgoing, incoming, own) in enumerate(sums):
        for index in range(count):
            cols = slice(index * block, (index + 1) * block)
            if kind == 0:
                both = dot_right_t(grad_up_ref[...], up_ref[cols, :])
            else:
                both = dot_plain(active_ref[...], down_ref[:, cols])
            own[:, cols] = both[:rows]
            outgoing[:, cols] = both[rows:]
            copies.append(
                remote(
                    outgoing.at[:, cols],
                    incoming.at[:, cols],
                    core_sems,
                    seqs + kind * count + index,
                    partner,
                )
            )
    exchanges = []
    for kind, got in enumerate((hidden_got_hbm, mlp_got_hbm)):
        _, incoming, own = sums[kind]
        for index in range(count):
            copies[kind * count + index].wait()
            cols = slice(index * block, (index + 1) * block)
            own[:, cols] = own[:, cols] + incoming[:, cols]
        exchanges.append(remote(own, got, swap_sems, swaps + kind, facing))
    pl.semaphore_signal(ready_sem, inc=1, device_id=partner, device_id_type=pl.DeviceIdType.MESH)
    again = [load_again(branch_hbm, branch_ref), load_again(normed_hbm, normed_ref)]
    cot_again = load_again(cot_hbm, hidden_ref)
    middle = min(3, ring.last)
    ring.rounds(0, middle)

    exchanges[0].wait()
    again.append(load_again(hidden_got_hbm, mine_ref))
    for copy in again + [cot_again]:
        copy.wait()
    pl.semaphore_wait(ready_sem, 1)
    copies, proj_total = [], 0.0
    for seq, span in enumerate(spans):
        gate, scale = mod(2, seq), 1.0 + mod(4, seq)

        def back(at):
            grad_hidden = normed_in[at] + mine_ref[at]
            normed = normed_ref[at]
            through = norm_back(grad_hidden * scale, normed, inverse_ref[at])
            grad_resid = hidden_ref[at].astype(jnp.float32) + through
            branch = branch_ref[at]
            normed_in[at] = through
            branch_ref[at] = grad_resid
            grad_mlp_ref[at] = (grad_resid * gate).astype(jnp.bfloat16)
            return grad_resid * branch, grad_hidden, grad_hidden * normed, grad_resid

        totals = over_rows(span.start, length, feat, 4, back)
        for index in range(3):
            mod_sum_ref[index, seq : seq + 1] = totals[index]
        proj_total = proj_total + totals[3] * gate
        copies.append(
            remote(branch_ref.at[span], got_ref.at[span], core_sems, seqs + 2 * count + seq, partner)
        )
    proj_sum_ref[...] = proj_total
    store(normed_in, through_hbm)
    for seq, copy in enumerate(copies):
        copy.wait()
        gate = mod(2, seq)

        def other_back(at):
            grad_mlp_ref[shifted(at, rows)] = (got_ref[at] * gate).astype(jnp.bfloat16)
            return ()

        over_rows(spans[seq].start, length, feat, 0, other_back)
    grad_attn_ref[...] = dot_right_t(grad_mlp_ref[...], proj_ref[...]).astype(jnp.bfloat16)
    store(grad_mlp_ref, grad_branch_hbm)
    store(grad_attn_ref, grad_attn_hbm)
    pl.semaphore_signal(ready_sem, inc=1, device_id=partner, device_id_type=pl.DeviceIdType.MESH)
    again = [load_again(branch_hbm, branch_ref)]
    ring.rounds(middle, ring.last)

    exchanges[1].wait()
    again.append(load_again(mlp_got_hbm, mine_ref))
    for copy in again:
        copy.wait()
    pl.semaphore_wait(ready_sem, 1)
    copies = []
    down_bias = down_bias_ref[stream : stream + 1].astype(jnp.float32)
    for seq, span in enumerate(spans):
        first_gate, second_gate = mod(2, seq), mod(5, seq)

        def finish_rows(at):
            mlp_out = spare[at] + mine_ref[at] + down_bias
            added = first_gate * branch_ref[at] + second_gate * mlp_out
            normed_ref[at] = added
            input_ref[at] = (input_ref[at].astype(jnp.float32) + added).astype(jnp.bfloat16)
            return (hidden_ref[at].astype(jnp.float32) * mlp_out,)

        (mod_sum_ref[3, seq : seq + 1],) = over_rows(span.start, length, feat, 1, finish_rows)
        copies.append(
            remote(normed_ref.at[span], got_ref.at[span], core_sems, 2 * seqs + 2 * count + seq, partner)
        )

    def other_rows(at):
        there = shifted(at, rows)
        input_ref[there] = (input_ref[there].astype(jnp.float32) + got_ref[at]).astype(jnp.bfloat16)
        return ()

    for seq, copy in enumerate(copies):
        copy.wait()
        over_rows(spans[seq].start, length, feat, 0, other_rows)
    store(input_ref, out_hbm)

    buffers = (mine_ref, got_ref, branch_ref, normed_ref)
    each = rows // (2 * ring.half)

    def piece_of(index):
        start = index % each * 2 * ring.half
        return buffers[index // each].at[start : start + 2 * ring.half]

    def put_later(later, which, way, values):
        piece_of(2 * (later + 1) + way)[which * ring.half : (which + 1) * ring.half] = values

    def put_total(which, way, values):
        if rest:
            piece_of(way)[which * ring.half : (which + 1) * ring.half] = values
        else:
            outs[which][0, way * ring.half : (way + 1) * ring.half] = values

    ring.finish(put_later, put_total)
    if rest:
        for index, out in enumerate(outs):
            store(piece_of(index), out)
    for copy in swapped:
        copy.wait()
    for copy in stored[len(kept) :]:
        copy.wait()


def mlp_ring(
    stream, mine, got, inputs, cots, modulate, proj_bias, up_bias, down_bias, up_weight, down_weight,
    proj_weight, gives, order, rest, collective_id,
):
    _, seqs, length, feat = inputs.shape
    rows, units, size, swaps = seqs * length, up_weight.shape[2], len(order), len(gives)
    local = proj_weight.shape[1]
    block = 256
    half = feat // (2 * size)
    vmem = pl.BlockSpec(memory_space=pltpu.VMEM)
    anywhere = pl.BlockSpec(memory_space=pl.ANY)

    def wide(*dims):
        return jax.ShapeDtypeStruct(dims, jnp.float32)

    def narrow(*dims):
        return jax.ShapeDtypeStruct(dims, jnp.bfloat16)

    def low(*dims):
        return pltpu.VMEM(dims, jnp.bfloat16)

    ring_outs = [wide(2 * half, units)] * (2 * (rest + 1)) if rest else [wide(1, 2 * half, units)] * 2
    gets = [jax.ShapeDtypeStruct(give.shape, give.dtype) for give in gives]
    small = {
        "up_bias": wide(1, units),
        "down_bias": wide(1, feat),
        "proj_bias": wide(1, feat),
        "mod_sums": wide(4, seqs, feat),
    }
    large = {name: wide(rows, feat) for name in ("branch", "normed", "hidden_got", "mlp_got", "through")}
    large |= {
        "grad_branch": narrow(2 * rows, feat),
        "grad_attn": narrow(2 * rows, local),
        "out": narrow(2 * rows, feat),
    }
    moved = 4 * 2 * 2 * (size - 1) * half * units
    blocks = 2 * feat // block
    results = pl.pallas_call(
        functools.partial(mlp_ring_kernel, order, stream, seqs, block, swaps, rest),
        out_shape=ring_outs + gets + list(small.values()) + list(large.values()),
        in_specs=[vmem] * 4 + [anywhere] * (7 + swaps),
        out_specs=[anywhere if rest else vmem] * len(ring_outs)
        + [anywhere] * swaps
        + [vmem] * len(small)
        + [anywhere] * len(large),
        scratch_shapes=ring_scratch(size, [(half, units)] * 2, [(2 * rows, feat)] * 2)
        + [
            low(feat, units),
            low(units, feat),
            low(2 * rows, feat),
            low(2 * rows, feat),
            low(2 * rows, units),
            low(2 * rows, units),
            low(2 * rows, feat),
            low(local, feat),
            low(2 * rows, local),
            pltpu.VMEM((rows, 1), jnp.float32),
        ]
        + [pltpu.VMEM((rows, feat), jnp.float32)] * 6
        + [
            pltpu.SemaphoreType.DMA((7,)),
            pltpu.SemaphoreType.DMA((2, 3 * seqs + blocks)),
            pltpu.SemaphoreType.DMA((2, swaps + 2)),
            pltpu.SemaphoreType.DMA((6 + len(ring_outs),)),
            pltpu.SemaphoreType.DMA((6,)),
            pltpu.SemaphoreType.REGULAR,
        ],
        compiler_params=pltpu.CompilerParams(
            collective_id=collective_id, has_side_effects=True, vmem_limit_bytes=67043328
        ),
        cost_estimate=pl.CostEstimate(flops=moved * 10000, bytes_accessed=moved, transcendentals=0),
        name="mlp_ring",
    )(
        modulate,
        proj_bias,
        up_bias,
        down_bias,
        mine,
        got,
        inputs.reshape(2 * rows, feat),
        cots.reshape(2 * rows, feat),
        up_weight,
        down_weight,
        proj_weight,
        *gives,
    )
    ring_parts, results = results[: len(ring_outs)], results[len(ring_outs) :]
    made = dict(zip(list(small) + list(large), results[swaps:]))
    made["ring"], made["gets"] = ring_parts, results[:swaps]
    return made


def attn_ring_kernel(order, tensor_size, seqs, block, row_share, *refs):
    take = taker(refs)
    mod_ref, cond_ref, own_cond_ref, gain_sum_ref, bias_sum_ref = take(5)
    small_sums = (take(4), take(4))
    packed_hbm, attn_hbm, hidden_hbm, branch_hbm = take(2), take(2), take(2), take(2)
    through_hbm, input_hbm, cot_hbm = take(2), take(2), take(2)
    weight_hbm, ada_hbm = take(2)
    out_hbm, got_hbm = take(2), take(2)
    qkv_out, proj_out, ada_out = take(3)
    cond_out, ada_bias_out, qkv_bias_out, up_bias_out, gain_out, proj_bias_out, down_bias_out = take(7)
    slots, terms, turned = take(4), take(4), take(4)
    (ring_sems,) = take(1)
    packed, attn, left, inputs = take(2), take(2), take(2), take(2)
    (weight_ref,) = take(1)
    outgoing, incoming, own = take(2), take(2), take(2)
    (edge_sums,) = take(1)
    load_sems, core_sems, swap_sems, out_sems, ready_sem = take(5)
    scratch = take(14)
    (mod_sems,) = take(1)
    size = len(order)
    feat = mod_ref.shape[2]
    local = attn[0].shape[1]
    cols = ada_hbm.shape[1]
    rows = [ref.shape[0] for ref in own]
    lengths = [count // seqs for count in rows]
    _, _, around, across = peers_of(size, tensor_size)
    partner, facing = across[0], across[1]
    ring = Ring(
        order, 0, (left[0], left[1], left[0], left[1]), packed + attn, slots, terms, turned, ring_sems
    )
    started = []

    def load(source, target):
        copy = pltpu.make_async_copy(source, target, load_sems.at[len(started)])
        copy.start()
        started.append(copy)
        return copy

    stored = []

    def store(source, target):
        copy = pltpu.make_async_copy(source, target, out_sems.at[len(stored)])
        copy.start()
        stored.append(copy)
        return copy

    first = [
        (load(hidden_hbm[stream], left[stream]), load(packed_hbm[stream], packed[stream]))
        for stream in range(2)
    ]
    second = [load(attn_hbm[stream], attn[stream]) for stream in range(2)]
    weight_load = load(weight_hbm, weight_ref)
    input_loads = [
        load(input_hbm[stream].at[: rows[stream]], inputs[stream]) for stream in range(2)
    ]
    greet(around + across)
    again = []
    for stream in range(2):
        for copy in first[stream]:
            copy.wait()
        ring.begin(stream)
        again.append(load(branch_hbm[stream], left[stream]))
    for stream in range(2):
        again[stream].wait()
        second[stream].wait()
        ring.begin(2 + stream)
    cot_loads = [load(cot_hbm[stream], left[stream]) for stream in range(2)]

    weight_load.wait()
    count = feat // block
    exchanges = []
    copies = {}
    for stream in (1, 0):
        for index in range(count):
            span = slice(index * block, (index + 1) * block)
            both = sum(
                dot_right_t(
                    packed[stream][:, part * local : (part + 1) * local], weight_ref[stream, part, span, :]
                )
                for part in range(3)
            )
            own[stream][:, span] = both[: rows[stream]]
            outgoing[stream][:, span] = both[rows[stream] :]
            copies[stream, index] = remote(
                outgoing[stream].at[:, span],
                incoming[stream].at[:, span],
                core_sems,
                stream * count + index,
                partner,
            )
    for stream in (1, 0):
        for index in range(count):
            copies[stream, index].wait()
            span = slice(index * block, (index + 1) * block)
            own[stream][:, span] = own[stream][:, span] + incoming[stream][:, span]
        exchanges.append(remote(own[stream], got_hbm[stream], swap_sems, stream, facing))
    through_loads = [load(through_hbm[stream], incoming[stream]) for stream in range(2)]
    middle = max(ring.last - 2, 0)
    ring.rounds(0, middle)

    for copy in exchanges:
        copy.wait()
    got_loads = [load(got_hbm[stream], outgoing[stream]) for stream in range(2)]
    for stream in range(2):
        input_loads[stream].wait()
        through_loads[stream].wait()
        cot_loads[stream].wait()
    for stream in (1, 0):
        got_loads[stream].wait()
        for seq in range(seqs):
            scale = 1.0 + mod_ref[stream * 6 + 1, seq : seq + 1, :]

            def back(at):
                normed, inverse = norm_of(inputs[stream][at].astype(jnp.float32))
                grad_hidden = own[stream][at] + outgoing[stream][at]
                added = incoming[stream][at] + norm_back(grad_hidden * scale, normed, inverse)
                own[stream][at] = added
                left[stream][at] = (left[stream][at].astype(jnp.float32) + added).astype(jnp.bfloat16)
                return grad_hidden, grad_hidden * normed

            totals = over_rows(seq * lengths[stream], lengths[stream], feat, 2, back)
            for index in range(2):
                edge_sums[2 * stream + index, seq : seq + 1] = totals[index]
    pl.semaphore_signal(ready_sem, inc=1, device_id=partner, device_id_type=pl.DeviceIdType.MESH)

    def mod_rows(stream):
        inner = small_sums[stream][3]
        return jnp.concatenate(
            [edge_sums[2 * stream], edge_sums[2 * stream + 1]] + [inner[index] for index in range(4)],
            axis=1,
        )

    def lines_of():
        def wide(values):
            return jnp.pad(values, ((0, 0), (0, feat - values.shape[1])))

        bias = functools.reduce(jnp.add, [bias_sum_ref[seq] for seq in range(seqs)])
        gain = functools.reduce(jnp.add, [gain_sum_ref[seq] for seq in range(seqs)])
        gain = gain[:, : gain.shape[1] // 2] + gain[:, gain.shape[1] // 2 :]
        group = [wide(bias)] + [wide(small_sums[stream][0][...]) for stream in range(2)]
        every = [wide(gain)]
        every += [small_sums[stream][1][...] * row_share for stream in range(2)]
        every += [small_sums[stream][2][...] * row_share for stream in range(2)]
        return jnp.concatenate(group + [jnp.zeros((4, feat), jnp.float32)] + every, axis=0)

    def put(name, values):
        if name == "group":
            for part in range(3):
                qkv_bias_out[part] = values[0:2, part * local : (part + 1) * local]
            up_bias_out[...] = values[2:4, : up_bias_out.shape[1]]
        elif name == "every":
            for stream in range(2):
                gain_out[stream] = values[2 * stream : 2 * stream + 2, : gain_out.shape[2]]
            proj_bias_out[...] = values[4:6]
            down_bias_out[...] = values[6:8]
        elif name == "silu":
            cond = own_cond_ref[...]
            sig = 1.0 / (1.0 + jnp.exp(-cond))
            cond_out[...] = values * sig * (1.0 + cond * (1.0 - sig))
        elif name[0] == "ada_bias":
            ada_bias_out[name[1] : name[1] + 1] = values
        else:
            target = own[0] if name[1] == 0 else incoming[0]
            for start in range(0, feat, block):
                target[:cols, start : start + block] = values(slice(start, start + block))
            store(target.at[:cols], ada_out.at[name[1]])

    def weight_of(stream):
        return left[0][stream * cols : (stream + 1) * cols]

    steps = mod_backward_steps(
        size, tensor_size, mod_rows, cond_ref, weight_of, lines_of, put, scratch, mod_sems
    )
    next(steps)
    pl.semaphore_wait(ready_sem, 1)
    shares = [
        remote(own[stream], outgoing[stream], core_sems, 2 * count + stream, partner)
        for stream in range(2)
    ]
    next(steps)
    for copy in shares:
        copy.wait()
    results = []
    for stream in (1, 0):
        def other_rows(at):
            there = shifted(at, rows[stream])
            left[stream][there] = (
                left[stream][there].astype(jnp.float32) + outgoing[stream][at]
            ).astype(jnp.bfloat16)
            return ()

        for seq in range(seqs):
            over_rows(seq * lengths[stream], lengths[stream], feat, 0, other_rows)
        results.append(store(left[stream], out_hbm[stream]))
    ring.rounds(middle, ring.last - 1)
    results[1].wait()
    ada_loads = [
        load(ada_hbm.at[stream], left[0].at[stream * cols : (stream + 1) * cols]) for stream in range(2)
    ]
    for copy in ada_loads:
        copy.wait()
    next(steps)
    ring.rounds(ring.last - 1, ring.last)
    for _ in range(len(across)):
        next(steps)

    def put_total(which, way, values):
        slot = slots[which].at[way, ring.last]
        slot[...] = values
        place = slice(way * ring.half, (way + 1) * ring.half)
        if which < 2:
            for part in range(3):
                store(slot.at[:, part * local : (part + 1) * local], qkv_out.at[which, part, place])
        else:
            store(slot, proj_out.at[which - 2, place])

    ring.finish(None, put_total)
    for _ in steps:
        pass
    for copy in [results[0]] + stored[2:]:
        copy.wait()


def attn_ring(
    modulate, conditioning, own_cond, gain_sums, bias_sums, states, packed, attn, hidden, inputs, cots, weight,
    ada_weight, order, tensor_size, row_share, collective_id,
):
    seqs, feat = inputs[0].shape[1], inputs[0].shape[3]
    size, local, cols = len(order), attn[0].shape[1], ada_weight.shape[1]
    rows = [array.shape[1] * array.shape[2] for array in inputs]
    units = states[0]["up_bias"].shape[1]
    block = 256
    half = feat // (2 * size)
    vmem = pl.BlockSpec(memory_space=pltpu.VMEM)
    anywhere = pl.BlockSpec(memory_space=pl.ANY)

    def wide(*dims):
        return jax.ShapeDtypeStruct(dims, jnp.float32)

    def low(*dims):
        return pltpu.VMEM(dims, jnp.bfloat16)

    large = [jax.ShapeDtypeStruct((2 * count, feat), jnp.bfloat16) for count in rows]
    large += [wide(count, feat) for count in rows]
    large += [wide(2, 3, 2 * half, local), wide(2, 2 * half, local), wide(2, cols, feat)]
    small = [
        wide(seqs, feat),
        wide(2, cols),
        wide(3, 2, local),
        wide(2, units),
        wide(2, 2, gain_sums.shape[2] // 2),
        wide(2, feat),
        wide(2, feat),
    ]
    halves = [(half, 3 * local)] * 2 + [(half, local)] * 2
    doubled = [(2 * count, feat) for count in rows]
    mod_refs, mod_sems = mod_scratch(size, tensor_size, seqs, feat, cols)
    moved = 4 * 2 * (size - 1) * half * 8 * local
    blocks = feat // block
    sums = [
        state[name] for state in states for name in ("up_bias", "proj_bias", "down_bias", "mod_sums")
    ]
    pairs = [
        packed,
        attn,
        hidden,
        [state["grad_branch"] for state in states],
        [state["through"] for state in states],
        [array.reshape(-1, feat) for array in inputs],
        [array.reshape(-1, feat) for array in cots],
    ]
    return pl.pallas_call(
        functools.partial(attn_ring_kernel, order, tensor_size, seqs, block, row_share),
        out_shape=large + small,
        in_specs=[vmem] * (5 + len(sums)) + [anywhere] * (2 * len(pairs) + 2),
        out_specs=[anywhere] * len(large) + [vmem] * len(small),
        scratch_shapes=ring_scratch(size, halves, doubled + doubled)
        + [low(2 * count, 3 * local) for count in rows]
        + [low(2 * count, local) for count in rows]
        + [low(2 * count, feat) for count in rows]
        + [low(count, feat) for count in rows]
        + [low(2, 3, feat, local)]
        + [pltpu.VMEM((count, feat), jnp.float32) for count in rows] * 3
        + [
            pltpu.VMEM((4, seqs, feat), jnp.float32),
            pltpu.SemaphoreType.DMA((20,)),
            pltpu.SemaphoreType.DMA((2, 2 * blocks + 2)),
            pltpu.SemaphoreType.DMA((2, 2)),
            pltpu.SemaphoreType.DMA((20,)),
            pltpu.SemaphoreType.REGULAR,
        ]
        + mod_refs
        + [mod_sems],
        compiler_params=pltpu.CompilerParams(
            collective_id=collective_id, has_side_effects=True, vmem_limit_bytes=67043328
        ),
        cost_estimate=pl.CostEstimate(flops=moved * 10000, bytes_accessed=moved, transcendentals=0),
        name="attn_ring",
    )(
        modulate,
        conditioning,
        own_cond,
        gain_sums,
        bias_sums,
        *sums,
        *[array for pair in pairs for array in pair],
        weight,
        ada_weight,
    )


def ring_rest(parts, order, rest):
    size = len(order)
    ahead = [(order[index], order[(index + 1) % size]) for index in range(size)]
    ways = (ahead, [(second, first) for first, second in ahead])
    totals = list(parts[:2])
    for later in range(rest):
        for way in range(2):
            totals[way] = lax.ppermute(totals[way], "dp", ways[way])
        for way in range(2):
            totals[way] = totals[way] + parts[2 * (later + 1) + way]
    return totals


def by_rows(totals):
    half = totals[0].shape[0] // 2
    return [
        jnp.concatenate([total[which * half : (which + 1) * half] for total in totals])[None]
        for which in range(2)
    ]


def on_device(
    order,
    tensor_size,
    input_img,
    input_txt,
    conditioning,
    ada_weight,
    ada_bias,
    qkv_weight,
    qkv_bias,
    norm_gain,
    proj_weight,
    proj_bias,
    up_weight,
    up_bias,
    down_weight,
    down_bias,
    cotangent_img,
    cotangent_txt,
):
    data_size = len(order)
    seqs, _, feat = input_img.shape
    core = lax.axis_index("tensor") % 2
    reals = (input_img.shape[1] // 2, input_txt.shape[1] // 2)

    def split_rows(array):
        half = array.shape[1] // 2
        pad = -half % ROW_TILE
        lower, upper = (
            jnp.pad(part, ((0, 0), (0, pad), (0, 0))) for part in (array[:, :half], array[:, half:])
        )
        first = core == 0
        return jnp.stack([jnp.where(first, lower, upper), jnp.where(first, upper, lower)])

    def join_rows(halves, real):
        own, other = halves.astype(jnp.bfloat16)
        first = core == 0
        lower, upper = jnp.where(first, own, other), jnp.where(first, other, own)
        return jnp.concatenate([lower[:, :real], upper[:, :real]], axis=1)

    ada_weight = ada_weight.transpose(0, 2, 1)
    modulate = mod_forward(
        conditioning, ada_weight, ada_bias, seqs, feat, data_size, tensor_size
    )
    piece = [
        [modulate[stream * 6 + index][:, None, :] for index in range(6)] for stream in range(2)
    ]

    inputs = [split_rows(input_img), split_rows(input_txt)]
    cotangents = [split_rows(cotangent_img), split_rows(cotangent_txt)]
    shapes = [array.shape for array in inputs]
    gain_pair = jnp.concatenate([norm_gain, norm_gain], axis=2)

    hidden1, raw = [], []
    for stream in range(2):
        normed, _ = layer_norm(inputs[stream].astype(jnp.float32))
        hidden = (normed * (1.0 + piece[stream][1]) + piece[stream][0]).astype(jnp.bfloat16)
        hidden = hidden.reshape(-1, feat)
        flat = [
            dot_plain(hidden, qkv_weight[stream, :, part]) + qkv_bias[stream, part].astype(jnp.float32)
            for part in range(3)
        ]
        hidden1.append(hidden)
        raw.append([each.reshape(shapes[stream][:3] + (-1,)) for each in flat])
    attn = attn_forward(gain_pair, raw[0], raw[1], reals[1])
    local = attn[0].shape[3]

    def mlp_stage(stream, got, gives, rest, collective_id):
        made = mlp_ring(
            stream,
            branch_sums[stream],
            got,
            inputs[stream],
            cotangents[stream],
            modulate,
            proj_bias,
            up_bias,
            down_bias,
            up_weight,
            down_weight,
            proj_weight,
            gives,
            order,
            rest,
            collective_id,
        )
        if rest:
            made["ring"] = by_rows(ring_rest(made["ring"], order, rest))
        return made

    branch_sums = [None, None]
    for stream in (1, 0):
        rows = attn[stream].reshape(2, -1, local)
        branch_sums[stream] = core_sum(
            dot_plain(rows[0], proj_weight[stream]),
            dot_plain(rows[1], proj_weight[stream]),
            tensor_size,
        )
    state = [None, None]
    got = lax.ppermute(branch_sums[1], "tensor", swap_pairs(tensor_size, 2))
    state[1] = mlp_stage(1, got, [branch_sums[0]], RESTS[0], 2)
    state[0] = mlp_stage(0, state[1]["gets"][0], [], RESTS[1], 3)
    mlp_rings = [state[stream]["ring"] for stream in range(2)]

    grad_attn = [state[stream]["grad_attn"].reshape(attn[stream].shape) for stream in range(2)]
    grad_packed = attn_backward(gain_pair, raw[0], raw[1], grad_attn[0], grad_attn[1], reals[1])
    own_cond = lax.dynamic_slice_in_dim(
        conditioning, lax.axis_index("dp") * seqs, seqs, axis=0
    ).astype(jnp.float32)
    made = attn_ring(
        modulate,
        conditioning,
        own_cond,
        grad_packed[3],
        grad_packed[2],
        state,
        [grad_packed[stream].reshape(-1, 3 * local) for stream in range(2)],
        [attn[stream].reshape(-1, local) for stream in range(2)],
        hidden1,
        inputs,
        cotangents,
        qkv_weight.transpose(0, 2, 1, 3),
        ada_weight,
        order,
        tensor_size,
        2.0 / tensor_size,
        4,
    )
    grad_qkv, grad_proj, grad_ada_weight, grad_conditioning, grad_ada_bias = made[4:9]
    qkv_bias_sums, up_bias_sums, gain_sums, proj_sums, down_sums = made[9:]
    outputs = [
        join_rows(state[stream]["out"].reshape(shapes[stream]), reals[stream]) for stream in range(2)
    ]
    grad_inputs = [join_rows(made[stream].reshape(shapes[stream]), reals[stream]) for stream in range(2)]
    down_rings, up_rings = ([mlp_rings[0][index], mlp_rings[1][index]] for index in range(2))
    return (
        outputs[0],
        outputs[1],
        grad_inputs[0],
        grad_inputs[1],
        grad_conditioning,
        grad_ada_weight.transpose(0, 2, 1),
        grad_ada_bias,
        grad_qkv.transpose(0, 2, 1, 3),
        qkv_bias_sums.transpose(1, 0, 2),
        gain_sums,
        grad_proj.transpose(0, 2, 1),
        proj_sums,
        jnp.concatenate(up_rings),
        up_bias_sums,
        jnp.concatenate(down_rings).transpose(0, 2, 1),
        down_sums,
    )


def solution(mesh):
    in_specs = (
        P("dp", None, None),
        P("dp", None, None),
        P(),
        P(None, None, ("dp", "tensor")),
        P(None, ("dp", "tensor")),
        P(None, None, None, "tensor"),
        P(None, None, "tensor"),
        P(),
        P(None, "tensor", None),
        P(),
        P(None, None, "tensor"),
        P(None, "tensor"),
        P(None, "tensor", None),
        P(),
        P("dp", None, None),
        P("dp", None, None),
    )
    out_specs = (
        P("dp", None, None),
        P("dp", None, None),
        P("dp", None, None),
        P("dp", None, None),
        P("dp", None),
        P(None, None, ("dp", "tensor")),
        P(None, ("dp", "tensor")),
        P(None, "dp", None, "tensor"),
        P(None, None, "tensor"),
        P(),
        P(None, "tensor", "dp"),
        P(),
        P(None, "dp", "tensor"),
        P(None, "tensor"),
        P(None, "tensor", "dp"),
        P(),
    )

    def step(*arrays):
        return on_device(ring_order(mesh), mesh.shape["tensor"], *arrays)

    return jax.shard_map(step, mesh=mesh, in_specs=in_specs, out_specs=out_specs, check_vma=False)
```

```python
import functools

import jax
import jax.numpy as jnp
from jax import lax
from jax.experimental import pallas as pl
from jax.experimental.pallas import tpu as pltpu
from jax.sharding import PartitionSpec as P


epsilon = 1e-06
GELU_C = 0.7978845608028654
GELU_A = 0.044715
ROW_TILE = 16
NEG = -1e30
RESTS = (1, 1)


def dot_plain(first_op, second_op):
    return jnp.dot(first_op, second_op, preferred_element_type=jnp.float32)


def dot_right_t(first_op, second_op):
    return lax.dot_general(
        first_op, second_op, (((1,), (1,)), ((), ())), preferred_element_type=jnp.float32
    )


def dot_left_t(first_op, second_op):
    return lax.dot_general(
        first_op, second_op, (((0,), (0,)), ((), ())), preferred_element_type=jnp.float32
    )


def norm_back(grad_normed, normed, inverse):
    return inverse * (
        grad_normed
        - jnp.mean(grad_normed, axis=-1, keepdims=True)
        - normed * jnp.mean(grad_normed * normed, axis=-1, keepdims=True)
    )


def gelu_both(values):
    inner = jnp.tanh(GELU_C * (values + GELU_A * values * values * values))
    active = 0.5 * values * (1.0 + inner)
    slope = 0.5 * (1.0 + inner) + 0.5 * values * (1.0 - inner * inner) * GELU_C * (
        1.0 + 3.0 * GELU_A * values * values
    )
    return active, slope


def head_norm(values, gain):
    head_dim = values.shape[1] // 2
    lower = lax.broadcasted_iota(jnp.int32, values.shape, 1) < head_dim
    square = values * values
    first = jnp.sum(jnp.where(lower, square, 0.0), axis=-1, keepdims=True) / head_dim
    second = jnp.sum(jnp.where(lower, 0.0, square), axis=-1, keepdims=True) / head_dim
    factor = jnp.where(lower, lax.rsqrt(first + epsilon), lax.rsqrt(second + epsilon))
    return values * factor * gain, factor


def rows_of(img_ref, txt_ref, cols):
    return jnp.concatenate(
        [img_ref[0, 0, :, cols], img_ref[1, 0, :, cols], txt_ref[0, 0, :, cols], txt_ref[1, 0, :, cols]],
        axis=0,
    )


def put_rows(img_ref, txt_ref, cols, values):
    img, txt = img_ref.shape[2], txt_ref.shape[2]
    img_ref[0, 0, :, cols] = values[:img]
    img_ref[1, 0, :, cols] = values[img : 2 * img]
    txt_ref[0, 0, :, cols] = values[2 * img : 2 * img + txt]
    txt_ref[1, 0, :, cols] = values[2 * img + txt :]


def gain_rows(gain_ref, which, img, txt):
    width = gain_ref.shape[2]
    return jnp.concatenate(
        [
            jnp.broadcast_to(gain_ref[0, which : which + 1, :], (2 * img, width)),
            jnp.broadcast_to(gain_ref[1, which : which + 1, :], (2 * txt, width)),
        ],
        axis=0,
    )


def key_bias(img, txt, real):
    where = lax.broadcasted_iota(jnp.int32, (1, 2 * (img + txt)), 1)
    first = where - 2 * img
    gone = ((first >= real) & (first < txt)) | (first >= txt + real)
    return jnp.where(gone, NEG, 0.0).astype(jnp.float32)


def probs(q_head, k_low, bias):
    scores = dot_right_t(q_head, k_low) + bias
    top = jnp.max(scores, axis=-1, keepdims=True)
    weights = jnp.exp(scores - top)
    return weights * (1.0 / jnp.sum(weights, axis=-1, keepdims=True))


def attn_forward(real, gain_ref, raw_refs, out_img_ref, out_txt_ref):
    img, txt = out_img_ref.shape[2], out_txt_ref.shape[2]
    local = out_img_ref.shape[3]
    pair = gain_ref.shape[2]
    q_gain, k_gain = gain_rows(gain_ref, 0, img, txt), gain_rows(gain_ref, 1, img, txt)
    bias = key_bias(img, txt, real)
    scale = (pair // 2) ** (-0.5)
    for start in range(0, local, pair):
        q_raw, k_raw, v_raw = (
            rows_of(raw_refs[0][part], raw_refs[1][part], slice(start, start + pair))
            for part in range(3)
        )
        q_low = head_norm(q_raw, q_gain)[0].astype(jnp.bfloat16) * jnp.bfloat16(scale)
        k_low = head_norm(k_raw, k_gain)[0].astype(jnp.bfloat16)
        v_low = v_raw.astype(jnp.bfloat16)
        lower = lax.broadcasted_iota(jnp.int32, q_raw.shape, 1) < pair // 2
        results = []
        for head in range(2):
            mine = lower if head == 0 else jnp.logical_not(lower)
            q_head = jnp.where(mine, q_low, jnp.bfloat16(0))
            results.append(dot_plain(probs(q_head, k_low, bias).astype(jnp.bfloat16), v_low))
        out = jnp.where(lower, results[0], results[1]).astype(jnp.bfloat16)
        put_rows(out_img_ref, out_txt_ref, slice(start, start + pair), out)


def attn_backward_kernel(real, gain_ref, *refs):
    raw_refs = (refs[:3], refs[3:6])
    d_img_ref, d_txt_ref, o_img_ref, o_txt_ref, bias_ref, dgain_ref = refs[6:]
    img, txt = d_img_ref.shape[2], d_txt_ref.shape[2]
    local = d_img_ref.shape[3]
    pair = gain_ref.shape[2]
    head_dim = pair // 2
    q_gain, k_gain = gain_rows(gain_ref, 0, img, txt), gain_rows(gain_ref, 1, img, txt)
    bias = key_bias(img, txt, real)
    scale = head_dim ** (-0.5)
    gain_sums = [[None, None], [None, None]]
    for start in range(0, local, pair):
        q_raw, k_raw, v_raw = (
            rows_of(raw_refs[0][part], raw_refs[1][part], slice(start, start + pair))
            for part in range(3)
        )
        q_wide, q_factor = head_norm(q_raw, q_gain)
        k_wide, k_factor = head_norm(k_raw, k_gain)
        q_low = q_wide.astype(jnp.bfloat16) * jnp.bfloat16(scale)
        k_low = k_wide.astype(jnp.bfloat16)
        v_low = v_raw.astype(jnp.bfloat16)
        grad_out = rows_of(d_img_ref, d_txt_ref, slice(start, start + pair))
        lower = lax.broadcasted_iota(jnp.int32, q_raw.shape, 1) < head_dim
        parts = []
        for head in range(2):
            mine = lower if head == 0 else jnp.logical_not(lower)
            prob = probs(jnp.where(mine, q_low, jnp.bfloat16(0)), k_low, bias)
            grad_v = dot_left_t(prob.astype(jnp.bfloat16), grad_out)
            grad_prob = dot_right_t(jnp.where(mine, grad_out, jnp.bfloat16(0)), v_low)
            delta = jnp.sum(prob * grad_prob, axis=-1, keepdims=True)
            grad_scores = (prob * (grad_prob - delta)).astype(jnp.bfloat16)
            parts.append((dot_plain(grad_scores, k_low), dot_left_t(grad_scores, q_low), grad_v))
        grad_qn = jnp.where(lower, parts[0][0], parts[1][0]) * scale
        grad_kn = jnp.where(lower, parts[0][1], parts[1][1])
        grad_vn = jnp.where(lower, parts[0][2], parts[1][2])

        def raw_grad(grad_normed, raw, factor, gain, which):
            gained = grad_normed * gain
            product = gained * raw
            first = jnp.sum(jnp.where(lower, product, 0.0), axis=-1, keepdims=True) / head_dim
            second = jnp.sum(jnp.where(lower, 0.0, product), axis=-1, keepdims=True) / head_dim
            inner = jnp.where(lower, first, second)
            terms = grad_normed * raw * factor
            for stream, rows in enumerate((slice(0, 2 * img), slice(2 * img, 2 * (img + txt)))):
                total = jnp.sum(terms[rows], axis=0, keepdims=True)
                old = gain_sums[stream][which]
                gain_sums[stream][which] = total if old is None else old + total
            return factor * gained - raw * (factor * factor * factor) * inner

        grads = (
            raw_grad(grad_qn, q_raw, q_factor, q_gain, 0),
            raw_grad(grad_kn, k_raw, k_factor, k_gain, 1),
            grad_vn,
        )
        for part, grad in enumerate(grads):
            cols = slice(part * local + start, part * local + start + pair)
            bias_ref[0, 0:1, cols] = jnp.sum(grad[: 2 * img], axis=0, keepdims=True)
            bias_ref[0, 1:2, cols] = jnp.sum(grad[2 * img :], axis=0, keepdims=True)
            put_rows(o_img_ref, o_txt_ref, cols, grad.astype(jnp.bfloat16))
    for stream in range(2):
        for which in range(2):
            row = stream * 2 + which
            dgain_ref[0, row : row + 1, :] = gain_sums[stream][which]


def block_of(array):
    shape = array.shape
    return pl.BlockSpec((shape[0], 1) + shape[2:], lambda seq: (0, seq, 0, 0))


def whole_of(array):
    return pl.BlockSpec(array.shape, lambda seq: (0,) * array.ndim)


def attn_backward(gain_pair, raw_img, raw_txt, grad_img, grad_txt, real):
    seqs, local = raw_img[0].shape[1], raw_img[0].shape[3]
    outs = [
        jax.ShapeDtypeStruct(raw_img[0].shape[:3] + (3 * local,), jnp.bfloat16),
        jax.ShapeDtypeStruct(raw_txt[0].shape[:3] + (3 * local,), jnp.bfloat16),
        jax.ShapeDtypeStruct((seqs, 2, 3 * local), jnp.float32),
        jax.ShapeDtypeStruct((seqs, 4, gain_pair.shape[2]), jnp.float32),
    ]
    rows = 2 * (raw_img[0].shape[2] + raw_txt[0].shape[2])
    return pl.pallas_call(
        functools.partial(attn_backward_kernel, real),
        grid=(seqs,),
        out_shape=outs,
        in_specs=[whole_of(gain_pair)]
        + [block_of(each) for each in raw_img + raw_txt + [grad_img, grad_txt]],
        out_specs=[
            block_of(outs[0]),
            block_of(outs[1]),
            pl.BlockSpec((1, 2, 3 * local), lambda seq: (seq, 0, 0)),
            pl.BlockSpec((1, 4, gain_pair.shape[2]), lambda seq: (seq, 0, 0)),
        ],
        compiler_params=pltpu.CompilerParams(vmem_limit_bytes=56 << 20),
        cost_estimate=pl.CostEstimate(
            flops=seqs * rows * rows * local * 10,
            bytes_accessed=seqs * rows * local * 20,
            transcendentals=seqs * rows * rows * (local // 64),
        ),
        name="attn_backward",
    )(gain_pair, *raw_img, *raw_txt, grad_img, grad_txt)


def xor_index(index, distance):
    return index + distance - 2 * distance * ((index // distance) % 2)


def peers_of(data_size, tensor_size):
    row, col = lax.axis_index("dp"), lax.axis_index("tensor")
    around = [(lax.rem(row + step, data_size), col) for step in range(1, data_size)]
    across = []
    distance = 1
    while distance < tensor_size:
        across.append((row, xor_index(col, distance)))
        distance *= 2
    return row, col, around, across


def greet(partners):
    barrier = pltpu.get_barrier_semaphore()
    for partner in partners:
        pl.semaphore_signal(barrier, inc=1, device_id=partner, device_id_type=pl.DeviceIdType.MESH)
    pl.semaphore_wait(barrier, len(partners))


def remote(source, target, sems, index, partner):
    copy = pltpu.make_async_remote_copy(
        src_ref=source,
        dst_ref=target,
        send_sem=sems.at[0, index],
        recv_sem=sems.at[1, index],
        device_id=partner,
        device_id_type=pl.DeviceIdType.MESH,
    )
    copy.start()
    return copy


def silu_of(cond_ref):
    wide = cond_ref[...].astype(jnp.float32)
    return (wide * (1.0 / (1.0 + jnp.exp(-wide)))).astype(jnp.bfloat16)


def mod_forward_kernel(
    data_size, tensor_size, cond_ref, weight_ref, bias_ref, out_ref, outgoing, blocks, sems
):
    row, col, around, across = peers_of(data_size, tensor_size)
    seqs, feat = out_ref.shape[1], out_ref.shape[2]
    silu_cond = silu_of(cond_ref)
    for stream in range(2):
        values = dot_right_t(silu_cond, weight_ref[stream]) + bias_ref[stream : stream + 1].astype(
            jnp.float32
        )
        for index in range(data_size):
            outgoing[index, stream * seqs : (stream + 1) * seqs] = values[
                index * seqs : (index + 1) * seqs
            ]
    blocks[col, row] = outgoing[row]
    greet(around + across)
    copies = [
        remote(outgoing.at[partner[0]], blocks.at[col, row], sems, index, partner)
        for index, partner in enumerate(around)
    ]
    for copy in copies:
        copy.wait()
    held, used = [0], len(around)
    for level in reversed(range(len(across))):
        distance = 1 << level
        copies = []
        for offset in held:
            index = col
            for bit in range(len(across)):
                if offset >> bit & 1:
                    index = xor_index(index, 1 << bit)
            copies.append(remote(blocks.at[index], blocks.at[index], sems, used, across[level]))
            used += 1
        for copy in copies:
            copy.wait()
        held = held + [offset | distance for offset in held]
    for stream in range(2):
        full = jnp.concatenate(
            [
                blocks[second, first, stream * seqs : (stream + 1) * seqs]
                for first in range(data_size)
                for second in range(tensor_size)
            ],
            axis=1,
        )
        for index in range(6):
            out_ref[stream * 6 + index] = full[:, index * feat : (index + 1) * feat]


def mod_forward(conditioning, ada_weight, ada_bias, seqs, feat, data_size, tensor_size):
    cols = ada_weight.shape[1]
    vmem = pl.BlockSpec(memory_space=pltpu.VMEM)
    return pl.pallas_call(
        functools.partial(mod_forward_kernel, data_size, tensor_size),
        out_shape=jax.ShapeDtypeStruct((12, seqs, feat), jnp.float32),
        in_specs=[vmem] * 3,
        out_specs=vmem,
        scratch_shapes=[
            pltpu.VMEM((data_size, 2 * seqs, cols), jnp.float32),
            pltpu.VMEM((tensor_size, data_size, 2 * seqs, cols), jnp.float32),
            pltpu.SemaphoreType.DMA((2, data_size + tensor_size)),
        ],
        compiler_params=pltpu.CompilerParams(
            collective_id=0, has_side_effects=True, vmem_limit_bytes=32 << 20
        ),
        name="mod_forward",
    )(conditioning, ada_weight, ada_bias)


def mod_backward_steps(data_size, tensor_size, mod_rows, cond_ref, weight_of, lines_of, put, scratch, sems):
    blocks, core_in, outgoing, cols_in, lines, lines_in, lines_own, lines_all = scratch[:8]
    silu_blocks, silu_in, silu_send, silu_recv, all_send, all_recv = scratch[8:]
    row, col, around, across = peers_of(data_size, tensor_size)
    seqs, cols = outgoing.shape[1] // 2, outgoing.shape[2]
    half, width = lines.shape[1] // 2, lines.shape[2]
    for stream in range(2):
        full = mod_rows(stream)
        for first in range(data_size):
            for second in range(tensor_size):
                start = (first * tensor_size + second) * cols
                blocks[second, first, stream * seqs : (stream + 1) * seqs] = full[
                    :, start : start + cols
                ]
    every_line = lines_of()
    for index in range(data_size):
        lines[index] = every_line[:, index * width : (index + 1) * width]

    used = 0
    copy = remote(blocks.at[xor_index(col, 1)], core_in, sems, used, across[0])
    used += 1
    yield
    copy.wait()
    for first in range(data_size):
        outgoing[first] = blocks[col, first] + core_in[first]

    cols_in[row] = outgoing[row]
    lines_in[row] = lines[row]
    copies = []
    for partner in around:
        for source, target in ((lines, lines_in), (outgoing, cols_in)):
            copies.append(
                remote(source.at[partner[0]], target.at[row], sems, used, partner)
            )
            used += 1
    silu_cond = silu_of(cond_ref)
    yield
    for copy in copies:
        copy.wait()
    lines_own[...] = functools.reduce(jnp.add, [lines_in[index] for index in range(data_size)])
    low = []
    for stream in range(2):
        wide = jnp.concatenate(
            [cols_in[index, stream * seqs : (stream + 1) * seqs] for index in range(data_size)],
            axis=0,
        )
        put(("ada_bias", stream), jnp.sum(wide, axis=0, keepdims=True))
        low.append(wide.astype(jnp.bfloat16))
    silu_grad = dot_plain(low[0], weight_of(0)) + dot_plain(low[1], weight_of(1))
    for index in range(data_size):
        silu_blocks[index] = silu_grad[index * seqs : (index + 1) * seqs]
    for stream in range(2):
        put(("ada_weight", stream), lambda span: dot_left_t(low[stream], silu_cond[:, span]))

    silu_in[row] = silu_blocks[row]
    lines_all[row] = lines_own[...]
    copies = []
    for partner in around:
        for source, target in (
            (silu_blocks.at[partner[0]], silu_in.at[row]),
            (lines_own, lines_all.at[row]),
        ):
            copies.append(remote(source, target, sems, used, partner))
            used += 1
    yield
    for copy in copies:
        copy.wait()
    silu_send[0] = functools.reduce(jnp.add, [silu_in[index] for index in range(data_size)])
    every_line = jnp.concatenate([lines_all[index] for index in range(data_size)], axis=1)
    all_send[0] = every_line[half:]
    put("group", every_line[:half])

    for level, partner in enumerate(across):
        copies = [
            remote(silu_send.at[level], silu_recv.at[level], sems, used, partner),
            remote(all_send.at[level], all_recv.at[level], sems, used + 1, partner),
        ]
        used += 2
        yield
        for copy in copies:
            copy.wait()
        silu_send[level + 1] = silu_send[level] + silu_recv[level]
        all_send[level + 1] = all_send[level] + all_recv[level]
    put("silu", silu_send[len(across)])
    put("every", all_send[len(across)])


def mod_scratch(data_size, tensor_size, seqs, feat, cols):
    levels, lines = tensor_size.bit_length() - 1, 16
    width = feat // data_size

    def wide(*shape):
        return pltpu.VMEM(shape, jnp.float32)

    return [
        wide(tensor_size, data_size, 2 * seqs, cols),
        wide(data_size, 2 * seqs, cols),
        wide(data_size, 2 * seqs, cols),
        wide(data_size, 2 * seqs, cols),
        wide(data_size, lines, width),
        wide(data_size, lines, width),
        wide(lines, width),
        wide(data_size, lines, width),
        wide(data_size, seqs, feat),
        wide(data_size, seqs, feat),
        wide(levels + 1, seqs, feat),
        wide(levels, seqs, feat),
        wide(levels + 1, lines // 2, feat),
        wide(levels, lines // 2, feat),
    ], pltpu.SemaphoreType.DMA((2, 1 + 4 * (data_size - 1) + 2 * levels))


def norm_of(values):
    center = values - jnp.mean(values, axis=-1, keepdims=True)
    inverse = lax.rsqrt(jnp.mean(center * center, axis=-1, keepdims=True) + epsilon)
    return center * inverse, inverse


def ring_order(mesh):
    size = mesh.shape["dp"]
    fallback = list(range(0, size, 2)) + list(range(1, size, 2))[::-1]
    axis = list(mesh.axis_names).index("dp")
    devices = mesh.devices
    line = [devices[(slice(None),) * axis + (index,)].flatten()[0] for index in range(size)]
    coords = [getattr(device, "coords", None) for device in line]
    if any(place is None for place in coords):
        return fallback
    near = [
        [
            other
            for other in range(size)
            if sum(abs(a - b) for a, b in zip(coords[index], coords[other])) == 1
        ]
        for index in range(size)
    ]
    path, seen, budget = [0], {0}, [200000]

    def extend():
        budget[0] -= 1
        if budget[0] < 0:
            return False
        if len(path) == size:
            return path[0] in near[path[-1]]
        choices = [index for index in near[path[-1]] if index not in seen]
        choices.sort(key=lambda index: (sum(o not in seen for o in near[index]), index))
        for index in choices:
            path.append(index)
            seen.add(index)
            if extend():
                return True
            path.pop()
            seen.remove(index)
        return False

    return path if extend() else fallback


def entry_of(table, index):
    value = jnp.int32(table[0])
    for place in range(1, len(table)):
        value = jnp.where(index == place, jnp.int32(table[place]), value)
    return value


def over_rows(base, length, feat, count, body):
    tile = ROW_TILE
    group = next(size for size in (4, 5, 3, 2, 1) if length // tile % size == 0)

    def step(index, carry):
        for place in range(group):
            start = pl.multiple_of(base + (index * group + place) * tile, tile)
            adds = body(pl.ds(start, tile))
            carry = tuple(
                total + add[: tile // 2] + add[tile // 2 :] for total, add in zip(carry, adds)
            )
        return carry

    zero = jnp.zeros((tile // 2, feat), jnp.float32)
    totals = lax.fori_loop(0, length // (tile * group), step, (zero,) * count)
    return [jnp.sum(total, axis=0, keepdims=True) for total in totals]


def shifted(rows, by):
    return pl.ds(pl.multiple_of(rows.start + by, ROW_TILE), rows.size)


def half_of(array, half, seq, by_seq):
    return array.at[seq, half] if by_seq else array.at[half, seq]


def move_halves(move, array, rows_ref, seqs, by_seq, to_array=False, halves=2):
    core = lax.axis_index("tensor") % 2
    length = rows_ref.shape[0] // (halves * seqs)
    copies = []
    for half, position in enumerate((core, 1 - core)[:halves]):
        for seq in range(seqs):
            start = (half * seqs + seq) * length
            ends = (half_of(array, position, seq, by_seq), rows_ref.at[start : start + length])
            copies.append(move(*(ends[::-1] if to_array else ends)))
    return copies


def wait_all(copies):
    for copy in copies:
        copy.wait()


class Ring:
    def __init__(self, order, rest, lefts, rights, slots, terms, turned, sems):
        self.order, self.size, self.rest = order, len(order), rest
        self.lefts, self.rights, self.slots, self.terms = lefts, rights, slots, terms
        self.turned, self.sems = turned, sems
        row, col = lax.axis_index("dp"), lax.axis_index("tensor")
        size = self.size
        self.place = entry_of([order.index(index) for index in range(size)], row)
        self.after = entry_of(order, lax.rem(self.place + 1, size))
        self.before = entry_of(order, lax.rem(self.place + size - 1, size))
        self.targets = ((self.after, col), (self.before, col))
        self.half = slots[0].shape[2]
        self.chains = [(which, way) for which in range(len(lefts)) for way in range(2)]
        self.last = size - 2 - rest

    def term(self, which, way, index):
        start = pl.multiple_of((2 * index + way) * self.half, 8)
        return dot_plain(
            self.turned[which][pl.ds(start, self.half), :], self.rights[which][...]
        )

    def work_out(self, indices):
        for which, way in self.chains:
            self.terms[which][way] = self.term(which, way, indices[way])

    def copy_of(self, which, way, step, source, target):
        return pltpu.make_async_remote_copy(
            src_ref=source,
            dst_ref=self.slots[which].at[way, target],
            send_sem=self.sems.at[0, which, way, step],
            recv_sem=self.sems.at[1, which, way, step],
            device_id=self.targets[way],
            device_id_type=pl.DeviceIdType.MESH,
        )

    def blocks_at(self, step):
        size = self.size
        return (
            entry_of(self.order, lax.rem(self.place + 2 * size - 2 - step, size)),
            entry_of(self.order, lax.rem(self.place + 2 + step, size)),
        )

    def arrive(self, which, way, step):
        slot = self.slots[which].at[way, step]
        self.copy_of(which, way, step, slot, step).wait_recv()

    def begin(self, which):
        width = 256
        for start in range(0, self.turned[which].shape[0], width):
            self.turned[which][start : start + width] = self.lefts[which][:, start : start + width].T
        for way in range(2):
            first = self.slots[which].at[way, self.size - 1]
            first[...] = self.term(which, way, (self.before, self.after)[way])
            self.copy_of(which, way, 0, first, 0).start()

    def rounds(self, first, last):
        def round_of(step, carry):
            self.work_out(self.blocks_at(step))
            for which, way in self.chains:
                self.arrive(which, way, step)
                slot = self.slots[which].at[way, step]
                slot[...] = slot[...] + self.terms[which][way]
                self.copy_of(which, way, step + 1, slot, step + 1).start()
            return carry

        lax.fori_loop(first, last, round_of, 0)

    def finish(self, put_later, put_total):
        for later in range(self.rest):
            indices = self.blocks_at(self.last + 1 + later)
            for which, way in self.chains:
                put_later(later, which, way, self.term(which, way, indices[way]))
        self.work_out(self.blocks_at(self.last))
        for which, way in self.chains:
            self.arrive(which, way, self.last)
            put_total(which, way, self.slots[which][way, self.last] + self.terms[which][way])

        def sent(step, carry):
            for which, way in self.chains:
                slot = self.slots[which].at[way, self.size - 1]
                self.copy_of(which, way, step, slot, step).wait_send()
            return carry

        lax.fori_loop(0, self.last + 1, sent, 0)


def taker(refs):
    refs = list(refs)

    def take(number):
        taken = refs[:number]
        del refs[:number]
        return taken

    return take


def ring_scratch(size, halves, lefts, count_kind=jnp.bfloat16):
    return (
        [pltpu.VMEM((2, size) + half, jnp.float32) for half in halves]
        + [pltpu.VMEM((2,) + half, jnp.float32) for half in halves]
        + [pltpu.VMEM(shape[::-1], count_kind) for shape in lefts]
        + [pltpu.SemaphoreType.DMA((2, len(halves), 2, size - 1))]
    )


def front_kernel(seqs, real, block, by_seqs, *refs):
    take = taker(refs)
    mod_ref, gain_ref, bias_ref = take(3)
    input_hbm = take(2)
    weight_hbm, proj_hbm = take(2)
    hidden_hbm, raw_hbm, attn_hbm, sum_hbm = take(2), (take(3), take(3)), take(2), take(2)
    (got_hbm,) = take(1)
    inputs, hidden, raw, attn = take(2), take(2), (take(3), take(3)), take(2)
    weight_ref, proj_ref = take(2)
    outgoing, incoming, own = take(2), take(2), take(2)
    load_sems, core_sems, swap_sems, out_sems = take(4)
    feat = hidden[0].shape[1]
    lengths = [ref.shape[2] for ref in attn]
    partner = (lax.axis_index("dp"), xor_index(lax.axis_index("tensor"), 1))
    facing = (lax.axis_index("dp"), xor_index(lax.axis_index("tensor"), 2))
    started = []

    def load(source, target):
        copy = pltpu.make_async_copy(source, target, load_sems.at[len(started)])
        copy.start()
        started.append(copy)
        return copy

    input_loads = [
        move_halves(load, input_hbm[stream], inputs[stream], seqs, by_seqs[stream]) for stream in range(2)
    ]
    weight_loads = [load(weight_hbm, weight_ref), load(proj_hbm, proj_ref)]
    greet((partner, facing))
    for copies in input_loads:
        wait_all(copies)

    def core_copy(stream, seq):
        span = pl.ds(pl.multiple_of(seq * lengths[stream], ROW_TILE), lengths[stream])
        return pltpu.make_async_remote_copy(
            src_ref=outgoing[stream].at[span],
            dst_ref=incoming[stream].at[span],
            send_sem=core_sems.at[0, stream, seq],
            recv_sem=core_sems.at[1, stream, seq],
            device_id=partner,
            device_id_type=pl.DeviceIdType.MESH,
        )

    def chip_copy(seq):
        span = pl.ds(pl.multiple_of(seq * lengths[1], ROW_TILE), lengths[1])
        return pltpu.make_async_remote_copy(
            src_ref=own[1].at[span],
            dst_ref=got_hbm.at[span],
            send_sem=swap_sems.at[0, seq],
            recv_sem=swap_sems.at[1, seq],
            device_id=facing,
            device_id_type=pl.DeviceIdType.MESH,
        )

    def normalize(seq):
        for stream in range(2):
            shift = mod_ref[stream * 6, pl.ds(seq, 1), :]
            scale = 1.0 + mod_ref[stream * 6 + 1, pl.ds(seq, 1), :]

            def first_norm(at):
                normed, _ = norm_of(inputs[stream][at].astype(jnp.float32))
                hidden[stream][at] = (normed * scale + shift).astype(jnp.bfloat16)
                return ()

            for half in range(2):
                over_rows((half * seqs + seq) * lengths[stream], lengths[stream], feat, 0, first_norm)

    def attend(seq):
        for stream in range(2):
            length = lengths[stream]
            left = jnp.concatenate(
                [
                    hidden[stream][pl.ds(pl.multiple_of((half * seqs + seq) * length, ROW_TILE), length), :]
                    for half in range(2)
                ],
                axis=0,
            )
            for part in range(3):
                values = dot_plain(left, weight_ref[stream, part]) + bias_ref[stream, part : part + 1].astype(
                    jnp.float32
                )
                raw[stream][part][0, seq] = values[:length]
                raw[stream][part][1, seq] = values[length:]
        one = pl.ds(seq, 1)
        attn_forward(
            real,
            gain_ref,
            [[ref.at[:, one] for ref in raw[stream]] for stream in range(2)],
            attn[0].at[:, one],
            attn[1].at[:, one],
        )
        for stream in (1, 0):
            length = lengths[stream]
            span = pl.ds(pl.multiple_of(seq * length, ROW_TILE), length)
            left = jnp.concatenate([attn[stream][0, seq], attn[stream][1, seq]], axis=0)
            for start in range(0, feat, block):
                cols = slice(start, start + block)
                both = dot_plain(left, proj_ref[stream, :, cols])
                own[stream][span, cols] = both[:length]
                outgoing[stream][span, cols] = both[length:]
            core_copy(stream, seq).start()

    def pass_on(seq):
        for stream in (1, 0):
            core_copy(stream, seq).wait()

            def add(at):
                own[stream][at] = own[stream][at] + incoming[stream][at]
                return ()

            over_rows(seq * lengths[stream], lengths[stream], feat, 0, add)
            if stream == 1:
                chip_copy(seq).start()

    def one_sequence(seq, carry):
        normalize(seq)

        @pl.when(seq == 0)
        def _():
            wait_all(weight_loads)

        @pl.when(seq > 0)
        def _():
            pass_on(seq - 1)

        attend(seq)
        return carry

    lax.fori_loop(0, seqs, one_sequence, 0)
    stores = []
    for source, target in zip(
        list(hidden) + list(raw[0]) + list(raw[1]) + list(attn),
        list(hidden_hbm) + list(raw_hbm[0]) + list(raw_hbm[1]) + list(attn_hbm),
    ):
        stores.append(pltpu.make_async_copy(source, target, out_sems.at[len(stores)]))
        stores[-1].start()
    pass_on(seqs - 1)
    for source, target in zip(own, sum_hbm):
        stores.append(pltpu.make_async_copy(source, target, out_sems.at[len(stores)]))
        stores[-1].start()
    for copy in stores:
        copy.wait()

    def arrive(seq, carry):
        chip_copy(seq).wait()
        return carry

    lax.fori_loop(0, seqs, arrive, 0)


def front(modulate, gain_pair, inputs, by_seqs, weight, bias, proj_weight, real, collective_id):
    seqs, feat = modulate.shape[1:]
    local = weight.shape[3]
    lengths = [array.shape[2] for array in inputs]
    rows = [seqs * length for length in lengths]
    vmem = pl.BlockSpec(memory_space=pltpu.VMEM)
    anywhere = pl.BlockSpec(memory_space=pl.ANY)
    shapes = [((2 * count, feat), jnp.bfloat16) for count in rows]
    shapes += [((2, seqs, length, local), jnp.float32) for length in lengths for _ in range(3)]
    shapes += [((2, seqs, length, local), jnp.bfloat16) for length in lengths]
    sums = [((count, feat), jnp.float32) for count in rows]
    outs = shapes + sums + sums[1:]
    results = pl.pallas_call(
        functools.partial(front_kernel, seqs, real, 512, by_seqs),
        out_shape=[jax.ShapeDtypeStruct(*out) for out in outs],
        in_specs=[vmem] * 3 + [anywhere] * 4,
        out_specs=[anywhere] * len(outs),
        scratch_shapes=[pltpu.VMEM((2 * count, feat), jnp.bfloat16) for count in rows]
        + [pltpu.VMEM(*shape) for shape in shapes]
        + [pltpu.VMEM(weight.shape, jnp.bfloat16), pltpu.VMEM(proj_weight.shape, jnp.bfloat16)]
        + [pltpu.VMEM(*each) for each in sums] * 3
        + [
            pltpu.SemaphoreType.DMA((2 + 4 * seqs,)),
            pltpu.SemaphoreType.DMA((2, 2, seqs)),
            pltpu.SemaphoreType.DMA((2, seqs)),
            pltpu.SemaphoreType.DMA((len(shapes) + 2,)),
        ],
        compiler_params=pltpu.CompilerParams(
            collective_id=collective_id, has_side_effects=True, vmem_limit_bytes=60 << 20
        ),
        name="front",
    )(
        modulate,
        gain_pair,
        bias,
        *inputs,
        weight,
        proj_weight,
    )
    return results[:2], (results[2:5], results[5:8]), results[8:10], results[10:12], results[12]


def mlp_ring_kernel(order, stream, seqs, block, swaps, rest, direct, *refs):
    take = taker(refs)
    mod_ref, proj_bias_ref, up_bias_ref, down_bias_ref = take(4)
    mine_hbm, got_hbm, input_hbm, cot_hbm, up_hbm, down_hbm, proj_hbm = take(7)
    gives = take(swaps)
    outs = take(2 * (rest + 1)) if rest else take(2)
    gets = take(swaps)
    up_sum_ref, down_sum_ref, proj_sum_ref, mod_sum_ref = take(4)
    branch_hbm, normed_hbm, hidden_got_hbm, mlp_got_hbm, through_hbm = take(5)
    grad_branch_hbm, grad_attn_hbm, out_hbm = take(3)
    slots, terms, turned = take(2), take(2), take(2)
    (ring_sems,) = take(1)
    up_ref, down_ref, input_ref, hidden_ref, active_ref, grad_up_ref, grad_mlp_ref = take(7)
    proj_ref, grad_attn_ref, inverse_ref = take(3)
    mine_ref, got_ref, branch_ref, normed_ref, normed_in, spare = take(6)
    load_sems, core_sems, swap_sems, out_sems, ready_sem = take(5)
    rows, feat = mine_ref.shape
    units = active_ref.shape[1]
    length = rows // seqs
    ring = Ring(
        order, rest, (grad_mlp_ref, hidden_ref), (active_ref, grad_up_ref), slots, terms, turned, ring_sems
    )
    partner = (lax.axis_index("dp"), xor_index(lax.axis_index("tensor"), 1))
    facing = (lax.axis_index("dp"), xor_index(lax.axis_index("tensor"), 2))

    started = []

    def load(source, target):
        copy = pltpu.make_async_copy(source, target, load_sems.at[len(started)])
        copy.start()
        started.append(copy)
        return copy

    first_loads = [load(mine_hbm, mine_ref), load(got_hbm, got_ref)]
    first_loads += move_halves(load, input_hbm, input_ref, seqs, direct)
    cot_loads = move_halves(load, cot_hbm, grad_mlp_ref, seqs, direct)
    weight_loads = [
        load(up_hbm.at[stream], up_ref),
        load(down_hbm.at[stream], down_ref),
        load(proj_hbm.at[stream], proj_ref),
    ]
    greet(ring.targets + (facing, partner))
    swapped = [
        remote(gives[index], gets[index], swap_sems, index, facing) for index in range(swaps)
    ]
    spans = [slice(seq * length, (seq + 1) * length) for seq in range(seqs)]
    other_spans = [slice(rows + seq * length, rows + (seq + 1) * length) for seq in range(seqs)]

    def mod(index, seq):
        return mod_ref[stream * 6 + index, seq : seq + 1, :]

    stored = []

    def store(source, target):
        copy = pltpu.make_async_copy(source, target, out_sems.at[len(stored)])
        copy.start()
        stored.append(copy)
        return copy

    def row_sum(values):
        return jnp.sum(values, axis=0, keepdims=True)

    wait_all(first_loads)
    copies = []
    proj_bias = proj_bias_ref[stream : stream + 1].astype(jnp.float32)
    for seq, span in enumerate(spans):
        gate, shift, scale = mod(2, seq), mod(3, seq), 1.0 + mod(4, seq)

        def second_norm(at):
            branch = mine_ref[at] + got_ref[at] + proj_bias
            branch_ref[at] = branch
            normed, inverse = norm_of(input_ref[at].astype(jnp.float32) + gate * branch)
            normed_ref[at] = normed
            inverse_ref[at] = inverse
            hidden_ref[at] = (normed * scale + shift).astype(jnp.bfloat16)
            return ()

        over_rows(span.start, length, feat, 0, second_norm)
        copies.append(remote(normed_ref.at[span], normed_in.at[span], core_sems, seq, partner))
    kept = [store(branch_ref, branch_hbm), store(normed_ref, normed_hbm)]
    wait_all(cot_loads)
    down_total = 0.0
    for half_spans in (spans, other_spans):
        for seq, span in enumerate(half_spans):
            gate = mod(5, seq)

            def gated(at):
                grad_mlp = grad_mlp_ref[at].astype(jnp.float32) * gate
                grad_mlp_ref[at] = grad_mlp.astype(jnp.bfloat16)
                return (grad_mlp,)

            (total,) = over_rows(span.start, length, feat, 1, gated)
            if half_spans is spans:
                down_total = down_total + total
    down_sum_ref[...] = down_total
    for seq, copy in enumerate(copies):
        copy.wait()
        shift, scale = mod(3, seq), 1.0 + mod(4, seq)

        def other_hidden(at):
            hidden_ref[shifted(at, rows)] = (normed_in[at] * scale + shift).astype(jnp.bfloat16)
            return ()

        over_rows(spans[seq].start, length, feat, 0, other_hidden)
    wait_all(weight_loads)

    def unit_block(index, carry):
        cols = pl.ds(pl.multiple_of(index * block, block), block)
        upward = dot_plain(hidden_ref[...], up_ref[:, cols]) + up_bias_ref[
            stream : stream + 1, cols
        ].astype(jnp.float32)
        active, slope = gelu_both(upward)
        active_ref[:, cols] = active.astype(jnp.bfloat16)
        grad_up = dot_right_t(grad_mlp_ref[...], down_ref[cols, :]) * slope
        up_sum_ref[:, cols] = row_sum(grad_up)
        grad_up_ref[:, cols] = grad_up.astype(jnp.bfloat16)
        return carry

    lax.fori_loop(0, units // block, unit_block, 0)
    for which in range(2):
        ring.begin(which)

    for copy in kept:
        copy.wait()
    count = feat // block
    sums = ((branch_ref, mine_ref, normed_in), (normed_ref, got_ref, spare))
    copies = []
    for kind, (outgoing, incoming, own) in enumerate(sums):
        for index in range(count):
            cols = slice(index * block, (index + 1) * block)
            if kind == 0:
                both = dot_right_t(grad_up_ref[...], up_ref[cols, :])
            else:
                both = dot_plain(active_ref[...], down_ref[:, cols])
            own[:, cols] = both[:rows]
            outgoing[:, cols] = both[rows:]
            copies.append(
                remote(
                    outgoing.at[:, cols],
                    incoming.at[:, cols],
                    core_sems,
                    seqs + kind * count + index,
                    partner,
                )
            )
    exchanges = []
    for kind, got in enumerate((hidden_got_hbm, mlp_got_hbm)):
        _, incoming, own = sums[kind]
        for index in range(count):
            copies[kind * count + index].wait()
            cols = slice(index * block, (index + 1) * block)
            own[:, cols] = own[:, cols] + incoming[:, cols]
        exchanges.append(remote(own, got, swap_sems, swaps + kind, facing))
    pl.semaphore_signal(ready_sem, inc=1, device_id=partner, device_id_type=pl.DeviceIdType.MESH)
    again = [load(branch_hbm, branch_ref), load(normed_hbm, normed_ref)]
    again += move_halves(load, cot_hbm, hidden_ref.at[:rows], seqs, direct, halves=1)
    middle = min(3, ring.last)
    ring.rounds(0, middle)

    exchanges[0].wait()
    again.append(load(hidden_got_hbm, mine_ref))
    wait_all(again)
    pl.semaphore_wait(ready_sem, 1)
    copies, proj_total = [], 0.0
    for seq, span in enumerate(spans):
        gate, scale = mod(2, seq), 1.0 + mod(4, seq)

        def back(at):
            grad_hidden = normed_in[at] + mine_ref[at]
            normed = normed_ref[at]
            through = norm_back(grad_hidden * scale, normed, inverse_ref[at])
            grad_resid = hidden_ref[at].astype(jnp.float32) + through
            branch = branch_ref[at]
            normed_in[at] = through
            branch_ref[at] = grad_resid
            grad_mlp_ref[at] = (grad_resid * gate).astype(jnp.bfloat16)
            return grad_resid * branch, grad_hidden, grad_hidden * normed, grad_resid

        totals = over_rows(span.start, length, feat, 4, back)
        for index in range(3):
            mod_sum_ref[index, seq : seq + 1] = totals[index]
        proj_total = proj_total + totals[3] * gate
        copies.append(
            remote(branch_ref.at[span], got_ref.at[span], core_sems, seqs + 2 * count + seq, partner)
        )
    proj_sum_ref[...] = proj_total
    store(normed_in, through_hbm)
    for seq, copy in enumerate(copies):
        copy.wait()
        gate = mod(2, seq)

        def other_back(at):
            grad_mlp_ref[shifted(at, rows)] = (got_ref[at] * gate).astype(jnp.bfloat16)
            return ()

        over_rows(spans[seq].start, length, feat, 0, other_back)
    grad_attn_ref[...] = dot_right_t(grad_mlp_ref[...], proj_ref[...]).astype(jnp.bfloat16)
    store(grad_mlp_ref, grad_branch_hbm)
    store(grad_attn_ref, grad_attn_hbm)
    pl.semaphore_signal(ready_sem, inc=1, device_id=partner, device_id_type=pl.DeviceIdType.MESH)
    again = [load(branch_hbm, branch_ref)]
    ring.rounds(middle, ring.last)

    exchanges[1].wait()
    again.append(load(mlp_got_hbm, mine_ref))
    wait_all(again)
    pl.semaphore_wait(ready_sem, 1)
    copies = []
    down_bias = down_bias_ref[stream : stream + 1].astype(jnp.float32)
    for seq, span in enumerate(spans):
        first_gate, second_gate = mod(2, seq), mod(5, seq)

        def finish_rows(at):
            mlp_out = spare[at] + mine_ref[at] + down_bias
            added = first_gate * branch_ref[at] + second_gate * mlp_out
            normed_ref[at] = added
            input_ref[at] = (input_ref[at].astype(jnp.float32) + added).astype(jnp.bfloat16)
            return (hidden_ref[at].astype(jnp.float32) * mlp_out,)

        (mod_sum_ref[3, seq : seq + 1],) = over_rows(span.start, length, feat, 1, finish_rows)
        copies.append(
            remote(normed_ref.at[span], got_ref.at[span], core_sems, 2 * seqs + 2 * count + seq, partner)
        )

    def other_rows(at):
        there = shifted(at, rows)
        input_ref[there] = (input_ref[there].astype(jnp.float32) + got_ref[at]).astype(jnp.bfloat16)
        return ()

    for seq, copy in enumerate(copies):
        copy.wait()
        over_rows(spans[seq].start, length, feat, 0, other_rows)
    move_halves(store, out_hbm, input_ref, seqs, direct, to_array=True)

    buffers = (mine_ref, got_ref, branch_ref, normed_ref)
    each = rows // (2 * ring.half)

    def piece_of(index):
        start = index % each * 2 * ring.half
        return buffers[index // each].at[start : start + 2 * ring.half]

    def put_later(later, which, way, values):
        piece_of(2 * (later + 1) + way)[which * ring.half : (which + 1) * ring.half] = values

    def put_total(which, way, values):
        if rest:
            piece_of(way)[which * ring.half : (which + 1) * ring.half] = values
        else:
            outs[which][0, way * ring.half : (way + 1) * ring.half] = values

    ring.finish(put_later, put_total)
    if rest:
        for index, out in enumerate(outs):
            store(piece_of(index), out)
    for copy in swapped:
        copy.wait()
    for copy in stored[len(kept) :]:
        copy.wait()


def mlp_ring(
    stream, mine, got, inputs, cots, modulate, proj_bias, up_bias, down_bias, up_weight, down_weight,
    proj_weight, gives, order, rest, direct, collective_id,
):
    seqs, feat = modulate.shape[1:]
    length = inputs.shape[2]
    rows, units, size, swaps = seqs * length, up_weight.shape[2], len(order), len(gives)
    local = proj_weight.shape[1]
    block = 256
    half = feat // (2 * size)
    vmem = pl.BlockSpec(memory_space=pltpu.VMEM)
    anywhere = pl.BlockSpec(memory_space=pl.ANY)

    def wide(*dims):
        return jax.ShapeDtypeStruct(dims, jnp.float32)

    def narrow(*dims):
        return jax.ShapeDtypeStruct(dims, jnp.bfloat16)

    def low(*dims):
        return pltpu.VMEM(dims, jnp.bfloat16)

    ring_outs = [wide(2 * half, units)] * (2 * (rest + 1)) if rest else [wide(1, 2 * half, units)] * 2
    gets = [jax.ShapeDtypeStruct(give.shape, give.dtype) for give in gives]
    small = {
        "up_bias": wide(1, units),
        "down_bias": wide(1, feat),
        "proj_bias": wide(1, feat),
        "mod_sums": wide(4, seqs, feat),
    }
    large = {name: wide(rows, feat) for name in ("branch", "normed", "hidden_got", "mlp_got", "through")}
    large |= {
        "grad_branch": narrow(2 * rows, feat),
        "grad_attn": narrow(2 * rows, local),
        "out": narrow(*inputs.shape),
    }
    moved = 4 * 2 * 2 * (size - 1) * half * units
    blocks = 2 * feat // block
    results = pl.pallas_call(
        functools.partial(mlp_ring_kernel, order, stream, seqs, block, swaps, rest, direct),
        out_shape=ring_outs + gets + list(small.values()) + list(large.values()),
        in_specs=[vmem] * 4 + [anywhere] * (7 + swaps),
        out_specs=[anywhere if rest else vmem] * len(ring_outs)
        + [anywhere] * swaps
        + [vmem] * len(small)
        + [anywhere] * len(large),
        scratch_shapes=ring_scratch(size, [(half, units)] * 2, [(2 * rows, feat)] * 2)
        + [
            low(feat, units),
            low(units, feat),
            low(2 * rows, feat),
            low(2 * rows, feat),
            low(2 * rows, units),
            low(2 * rows, units),
            low(2 * rows, feat),
            low(local, feat),
            low(2 * rows, local),
            pltpu.VMEM((rows, 1), jnp.float32),
        ]
        + [pltpu.VMEM((rows, feat), jnp.float32)] * 6
        + [
            pltpu.SemaphoreType.DMA((10 + 5 * seqs,)),
            pltpu.SemaphoreType.DMA((2, 3 * seqs + blocks)),
            pltpu.SemaphoreType.DMA((2, swaps + 2)),
            pltpu.SemaphoreType.DMA((6 + 2 * seqs + len(ring_outs),)),
            pltpu.SemaphoreType.REGULAR,
        ],
        compiler_params=pltpu.CompilerParams(
            collective_id=collective_id, has_side_effects=True, vmem_limit_bytes=67043328
        ),
        cost_estimate=pl.CostEstimate(flops=moved * 10000, bytes_accessed=moved, transcendentals=0),
        name="mlp_ring",
    )(
        modulate,
        proj_bias,
        up_bias,
        down_bias,
        mine,
        got,
        inputs,
        cots,
        up_weight,
        down_weight,
        proj_weight,
        *gives,
    )
    ring_parts, results = results[: len(ring_outs)], results[len(ring_outs) :]
    made = dict(zip(list(small) + list(large), results[swaps:]))
    made["ring"], made["gets"] = ring_parts, results[:swaps]
    return made


def attn_ring_kernel(order, tensor_size, seqs, block, row_share, directs, *refs):
    take = taker(refs)
    mod_ref, cond_ref, own_cond_ref, gain_sum_ref, bias_sum_ref = take(5)
    small_sums = (take(4), take(4))
    packed_hbm, attn_hbm, hidden_hbm, branch_hbm = take(2), take(2), take(2), take(2)
    through_hbm, input_hbm, cot_hbm = take(2), take(2), take(2)
    weight_hbm, ada_hbm = take(2)
    arrived = (take(4), take(4))
    out_hbm, got_hbm = take(2), take(2)
    qkv_out, proj_out, ada_out = take(3)
    mlp_outs = take(2)
    cond_out, ada_bias_out, qkv_bias_out, up_bias_out, gain_out, proj_bias_out, down_bias_out = take(7)
    slots, terms, turned = take(4), take(4), take(4)
    (ring_sems,) = take(1)
    packed, attn, left, inputs = take(2), take(2), take(2), take(2)
    (weight_ref,) = take(1)
    outgoing, incoming, own = take(2), take(2), take(2)
    (edge_sums,) = take(1)
    load_sems, core_sems, swap_sems, out_sems, ready_sem = take(5)
    scratch = take(14)
    (mod_sems,) = take(1)
    size = len(order)
    feat = mod_ref.shape[2]
    local = attn[0].shape[1]
    cols = ada_hbm.shape[1]
    rows = [ref.shape[0] for ref in own]
    lengths = [count // seqs for count in rows]
    _, _, around, across = peers_of(size, tensor_size)
    partner, facing = across[0], across[1]
    ring = Ring(
        order, 0, (left[0], left[1], left[0], left[1]), packed + attn, slots, terms, turned, ring_sems
    )
    started = []

    def load(source, target):
        copy = pltpu.make_async_copy(source, target, load_sems.at[len(started)])
        copy.start()
        started.append(copy)
        return copy

    stored = []

    def store(source, target):
        copy = pltpu.make_async_copy(source, target, out_sems.at[len(stored)])
        copy.start()
        stored.append(copy)
        return copy

    first = [
        (load(hidden_hbm[stream], left[stream]), load(packed_hbm[stream], packed[stream]))
        for stream in range(2)
    ]
    second = [load(attn_hbm[stream], attn[stream]) for stream in range(2)]
    weight_load = load(weight_hbm, weight_ref)
    input_loads = [
        move_halves(load, input_hbm[stream], inputs[stream], seqs, directs[stream], halves=1)
        for stream in range(2)
    ]
    greet(around + across)
    again = []
    for stream in range(2):
        for copy in first[stream]:
            copy.wait()
        ring.begin(stream)
        again.append(load(branch_hbm[stream], left[stream]))
    for stream in range(2):
        again[stream].wait()
        second[stream].wait()
        ring.begin(2 + stream)
    cot_loads = [
        move_halves(load, cot_hbm[stream], left[stream], seqs, directs[stream]) for stream in range(2)
    ]

    weight_load.wait()
    count = feat // block
    exchanges = []
    copies = {}
    for stream in (1, 0):
        for index in range(count):
            span = slice(index * block, (index + 1) * block)
            both = sum(
                dot_right_t(
                    packed[stream][:, part * local : (part + 1) * local], weight_ref[stream, part, span, :]
                )
                for part in range(3)
            )
            own[stream][:, span] = both[: rows[stream]]
            outgoing[stream][:, span] = both[rows[stream] :]
            copies[stream, index] = remote(
                outgoing[stream].at[:, span],
                incoming[stream].at[:, span],
                core_sems,
                stream * count + index,
                partner,
            )
    for stream in (1, 0):
        for index in range(count):
            copies[stream, index].wait()
            span = slice(index * block, (index + 1) * block)
            own[stream][:, span] = own[stream][:, span] + incoming[stream][:, span]
        exchanges.append(remote(own[stream], got_hbm[stream], swap_sems, stream, facing))
    through_loads = [load(through_hbm[stream], incoming[stream]) for stream in range(2)]
    middle = max(ring.last - 2, 0)
    ring.rounds(0, middle)

    for copy in exchanges:
        copy.wait()
    got_loads = [load(got_hbm[stream], outgoing[stream]) for stream in range(2)]
    for stream in range(2):
        wait_all(input_loads[stream] + cot_loads[stream] + [through_loads[stream]])
    for stream in (1, 0):
        got_loads[stream].wait()
        for seq in range(seqs):
            scale = 1.0 + mod_ref[stream * 6 + 1, seq : seq + 1, :]

            def back(at):
                normed, inverse = norm_of(inputs[stream][at].astype(jnp.float32))
                grad_hidden = own[stream][at] + outgoing[stream][at]
                added = incoming[stream][at] + norm_back(grad_hidden * scale, normed, inverse)
                own[stream][at] = added
                left[stream][at] = (left[stream][at].astype(jnp.float32) + added).astype(jnp.bfloat16)
                return grad_hidden, grad_hidden * normed

            totals = over_rows(seq * lengths[stream], lengths[stream], feat, 2, back)
            for index in range(2):
                edge_sums[2 * stream + index, seq : seq + 1] = totals[index]
    pl.semaphore_signal(ready_sem, inc=1, device_id=partner, device_id_type=pl.DeviceIdType.MESH)

    def mod_rows(stream):
        inner = small_sums[stream][3]
        return jnp.concatenate(
            [edge_sums[2 * stream], edge_sums[2 * stream + 1]] + [inner[index] for index in range(4)],
            axis=1,
        )

    def lines_of():
        def wide(values):
            return jnp.pad(values, ((0, 0), (0, feat - values.shape[1])))

        bias = functools.reduce(jnp.add, [bias_sum_ref[seq] for seq in range(seqs)])
        gain = functools.reduce(jnp.add, [gain_sum_ref[seq] for seq in range(seqs)])
        gain = gain[:, : gain.shape[1] // 2] + gain[:, gain.shape[1] // 2 :]
        group = [wide(bias)] + [wide(small_sums[stream][0][...]) for stream in range(2)]
        every = [wide(gain)]
        every += [small_sums[stream][1][...] * row_share for stream in range(2)]
        every += [small_sums[stream][2][...] * row_share for stream in range(2)]
        return jnp.concatenate(group + [jnp.zeros((4, feat), jnp.float32)] + every, axis=0)

    def put(name, values):
        if name == "group":
            for part in range(3):
                qkv_bias_out[part] = values[0:2, part * local : (part + 1) * local]
            up_bias_out[...] = values[2:4, : up_bias_out.shape[1]]
        elif name == "every":
            for stream in range(2):
                gain_out[stream] = values[2 * stream : 2 * stream + 2, : gain_out.shape[2]]
            proj_bias_out[...] = values[4:6]
            down_bias_out[...] = values[6:8]
        elif name == "silu":
            cond = own_cond_ref[...]
            sig = 1.0 / (1.0 + jnp.exp(-cond))
            cond_out[...] = values * sig * (1.0 + cond * (1.0 - sig))
        elif name[0] == "ada_bias":
            ada_bias_out[name[1] : name[1] + 1] = values
        else:
            target = own[0] if name[1] == 0 else incoming[0]
            for start in range(0, feat, block):
                target[:cols, start : start + block] = values(slice(start, start + block))
            store(target.at[:cols], ada_out.at[name[1]])

    def weight_of(stream):
        return left[0][stream * cols : (stream + 1) * cols]

    steps = mod_backward_steps(
        size, tensor_size, mod_rows, cond_ref, weight_of, lines_of, put, scratch, mod_sems
    )
    next(steps)
    pl.semaphore_wait(ready_sem, 1)
    shares = [
        remote(own[stream], outgoing[stream], core_sems, 2 * count + stream, partner)
        for stream in range(2)
    ]
    next(steps)
    for copy in shares:
        copy.wait()
    results = []
    for stream in (1, 0):
        def other_rows(at):
            there = shifted(at, rows[stream])
            left[stream][there] = (
                left[stream][there].astype(jnp.float32) + outgoing[stream][at]
            ).astype(jnp.bfloat16)
            return ()

        for seq in range(seqs):
            over_rows(seq * lengths[stream], lengths[stream], feat, 0, other_rows)
        results.append(
            move_halves(store, out_hbm[stream], left[stream], seqs, directs[stream], to_array=True)
        )

    height = arrived[0][0].shape[0]
    sides = (
        (outgoing[0].at[:height], outgoing[0].at[height : 2 * height]),
        (outgoing[1].at[:height], incoming[1].at[:height]),
    )

    def fetch(stream):
        return [
            load(arrived[stream][2 * way + side], sides[way][side]) for way in range(2) for side in range(2)
        ]

    def add_up(stream, copies):
        puts = []
        for copy in copies:
            copy.wait()
        for way, (first, second) in enumerate(sides):
            first[...] = first[...] + second[...]
            for which in range(2):
                puts.append(
                    store(
                        first.at[which * ring.half : (which + 1) * ring.half],
                        mlp_outs[which].at[stream, way * ring.half : (way + 1) * ring.half],
                    )
                )
        return puts

    fetched = fetch(1)
    ring.rounds(middle, ring.last - 1)
    puts = add_up(1, fetched)
    for copy in results[1]:
        copy.wait()
    ada_loads = [
        load(ada_hbm.at[stream], left[0].at[stream * cols : (stream + 1) * cols]) for stream in range(2)
    ]
    for copy in ada_loads:
        copy.wait()
    next(steps)
    for copy in puts:
        copy.wait()
    fetched = fetch(0)
    ring.rounds(ring.last - 1, ring.last)
    add_up(0, fetched)
    for _ in range(len(across)):
        next(steps)

    def put_total(which, way, values):
        slot = slots[which].at[way, ring.last]
        slot[...] = values
        place = slice(way * ring.half, (way + 1) * ring.half)
        if which < 2:
            for part in range(3):
                store(slot.at[:, part * local : (part + 1) * local], qkv_out.at[which, part, place])
        else:
            store(slot, proj_out.at[which - 2, place])

    ring.finish(None, put_total)
    for _ in steps:
        pass
    waited = {id(copy) for copy in puts + results[1]}
    for copy in stored:
        if id(copy) not in waited:
            copy.wait()


def attn_ring(
    modulate, conditioning, own_cond, gain_sums, bias_sums, states, packed, attn, hidden, inputs, cots, weight,
    ada_weight, order, tensor_size, row_share, directs, collective_id,
):
    seqs, feat = modulate.shape[1:]
    size, local, cols = len(order), attn[0].shape[1], ada_weight.shape[1]
    rows = [seqs * array.shape[2] for array in inputs]
    units = states[0]["up_bias"].shape[1]
    block = 256
    half = feat // (2 * size)
    vmem = pl.BlockSpec(memory_space=pltpu.VMEM)
    anywhere = pl.BlockSpec(memory_space=pl.ANY)

    def wide(*dims):
        return jax.ShapeDtypeStruct(dims, jnp.float32)

    def low(*dims):
        return pltpu.VMEM(dims, jnp.bfloat16)

    large = [jax.ShapeDtypeStruct(array.shape, jnp.bfloat16) for array in inputs]
    large += [wide(count, feat) for count in rows]
    large += [wide(2, 3, 2 * half, local), wide(2, 2 * half, local), wide(2, cols, feat)]
    large += [wide(2, 2 * half, units)] * 2
    small = [
        wide(seqs, feat),
        wide(2, cols),
        wide(3, 2, local),
        wide(2, units),
        wide(2, 2, gain_sums.shape[2] // 2),
        wide(2, feat),
        wide(2, feat),
    ]
    halves = [(half, 3 * local)] * 2 + [(half, local)] * 2
    doubled = [(2 * count, feat) for count in rows]
    mod_refs, mod_sems = mod_scratch(size, tensor_size, seqs, feat, cols)
    moved = 4 * 2 * (size - 1) * half * 8 * local
    blocks = feat // block
    sums = [
        state[name] for state in states for name in ("up_bias", "proj_bias", "down_bias", "mod_sums")
    ]
    pairs = [
        packed,
        attn,
        hidden,
        [state["grad_branch"] for state in states],
        [state["through"] for state in states],
        inputs,
        cots,
    ]
    return pl.pallas_call(
        functools.partial(attn_ring_kernel, order, tensor_size, seqs, block, row_share, directs),
        out_shape=large + small,
        in_specs=[vmem] * (5 + len(sums)) + [anywhere] * (2 * len(pairs) + 10),
        out_specs=[anywhere] * len(large) + [vmem] * len(small),
        scratch_shapes=ring_scratch(size, halves, doubled + doubled)
        + [low(2 * count, 3 * local) for count in rows]
        + [low(2 * count, local) for count in rows]
        + [low(2 * count, feat) for count in rows]
        + [low(count, feat) for count in rows]
        + [low(2, 3, feat, local)]
        + [pltpu.VMEM((count, feat), jnp.float32) for count in rows] * 3
        + [
            pltpu.VMEM((4, seqs, feat), jnp.float32),
            pltpu.SemaphoreType.DMA((28 + 6 * seqs,)),
            pltpu.SemaphoreType.DMA((2, 2 * blocks + 2)),
            pltpu.SemaphoreType.DMA((2, 2)),
            pltpu.SemaphoreType.DMA((32 + 4 * seqs,)),
            pltpu.SemaphoreType.REGULAR,
        ]
        + mod_refs
        + [mod_sems],
        compiler_params=pltpu.CompilerParams(
            collective_id=collective_id, has_side_effects=True, vmem_limit_bytes=67043328
        ),
        cost_estimate=pl.CostEstimate(flops=moved * 10000, bytes_accessed=moved, transcendentals=0),
        name="attn_ring",
    )(
        modulate,
        conditioning,
        own_cond,
        gain_sums,
        bias_sums,
        *sums,
        *[array for pair in pairs for array in pair],
        weight,
        ada_weight,
        *[array for state in states for pair in state["ring"] for array in pair],
    )


def ring_rest(parts, order, rest):
    size = len(order)
    ahead = [(order[index], order[(index + 1) % size]) for index in range(size)]
    ways = (ahead, [(second, first) for first, second in ahead])
    totals = list(parts[:2])
    for later in range(rest):
        for way in range(2):
            if later:
                totals[way] = totals[way] + parts[2 * later + way]
            totals[way] = lax.ppermute(totals[way], "dp", ways[way])
    return [(totals[way], parts[2 * rest + way]) for way in range(2)]


def on_device(
    order,
    tensor_size,
    input_img,
    input_txt,
    conditioning,
    ada_weight,
    ada_bias,
    qkv_weight,
    qkv_bias,
    norm_gain,
    proj_weight,
    proj_bias,
    up_weight,
    up_bias,
    down_weight,
    down_bias,
    cotangent_img,
    cotangent_txt,
):
    data_size = len(order)
    seqs, _, feat = input_img.shape
    reals = (input_img.shape[1] // 2, input_txt.shape[1] // 2)
    directs = [
        shape[1] == 2 * real and real % ROW_TILE == 0
        for shape, real in zip((input_img.shape, input_txt.shape), reals)
    ]

    def split_rows(array, stream):
        real = reals[stream]
        if directs[stream]:
            return array.reshape(seqs, 2, real, feat)
        pad = -real % ROW_TILE
        return jnp.stack(
            [
                jnp.pad(part, ((0, 0), (0, pad), (0, 0)))
                for part in (array[:, :real], array[:, real:])
            ]
        )

    def join_rows(halves, stream):
        real = reals[stream]
        if directs[stream]:
            return halves.reshape(seqs, 2 * real, feat)
        return jnp.concatenate([halves[0][:, :real], halves[1][:, :real]], axis=1)

    ada_weight = ada_weight.transpose(0, 2, 1)
    modulate = mod_forward(
        conditioning, ada_weight, ada_bias, seqs, feat, data_size, tensor_size
    )
    inputs = [split_rows(input_img, 0), split_rows(input_txt, 1)]
    cotangents = [split_rows(cotangent_img, 0), split_rows(cotangent_txt, 1)]
    gain_pair = jnp.concatenate([norm_gain, norm_gain], axis=2)

    qkv_weight = qkv_weight.transpose(0, 2, 1, 3)
    hidden1, raw, attn, branch_sums, got = front(
        modulate, gain_pair, inputs, directs, qkv_weight, qkv_bias, proj_weight, reals[1], 5
    )
    local = attn[0].shape[3]

    def mlp_stage(stream, got, gives, rest, collective_id):
        made = mlp_ring(
            stream,
            branch_sums[stream],
            got,
            inputs[stream],
            cotangents[stream],
            modulate,
            proj_bias,
            up_bias,
            down_bias,
            up_weight,
            down_weight,
            proj_weight,
            gives,
            order,
            rest,
            directs[stream],
            collective_id,
        )
        made["ring"] = ring_rest(made["ring"], order, rest)
        return made

    state = [None, None]
    state[1] = mlp_stage(1, got, [branch_sums[0]], RESTS[0], 2)
    state[0] = mlp_stage(0, state[1]["gets"][0], [], RESTS[1], 3)

    grad_attn = [state[stream]["grad_attn"].reshape(attn[stream].shape) for stream in range(2)]
    grad_packed = attn_backward(gain_pair, list(raw[0]), list(raw[1]), grad_attn[0], grad_attn[1], reals[1])
    own_cond = lax.dynamic_slice_in_dim(
        conditioning, lax.axis_index("dp") * seqs, seqs, axis=0
    ).astype(jnp.float32)
    made = attn_ring(
        modulate,
        conditioning,
        own_cond,
        grad_packed[3],
        grad_packed[2],
        state,
        [grad_packed[stream].reshape(-1, 3 * local) for stream in range(2)],
        [attn[stream].reshape(-1, local) for stream in range(2)],
        hidden1,
        inputs,
        cotangents,
        qkv_weight,
        ada_weight,
        order,
        tensor_size,
        2.0 / tensor_size,
        directs,
        4,
    )
    grad_qkv, grad_proj, grad_ada_weight, grad_down, grad_up, grad_conditioning, grad_ada_bias = made[4:11]
    qkv_bias_sums, up_bias_sums, gain_sums, proj_sums, down_sums = made[11:]

    outputs = [join_rows(state[stream]["out"], stream) for stream in range(2)]
    grad_inputs = [join_rows(made[stream], stream) for stream in range(2)]
    return (
        outputs[0],
        outputs[1],
        grad_inputs[0],
        grad_inputs[1],
        grad_conditioning,
        grad_ada_weight.transpose(0, 2, 1),
        grad_ada_bias,
        grad_qkv.transpose(0, 2, 1, 3),
        qkv_bias_sums.transpose(1, 0, 2),
        gain_sums,
        grad_proj.transpose(0, 2, 1),
        proj_sums,
        grad_up,
        up_bias_sums,
        grad_down.transpose(0, 2, 1),
        down_sums,
    )


def solution(mesh):
    in_specs = (
        P("dp", None, None),
        P("dp", None, None),
        P(),
        P(None, None, ("dp", "tensor")),
        P(None, ("dp", "tensor")),
        P(None, None, None, "tensor"),
        P(None, None, "tensor"),
        P(),
        P(None, "tensor", None),
        P(),
        P(None, None, "tensor"),
        P(None, "tensor"),
        P(None, "tensor", None),
        P(),
        P("dp", None, None),
        P("dp", None, None),
    )
    out_specs = (
        P("dp", None, None),
        P("dp", None, None),
        P("dp", None, None),
        P("dp", None, None),
        P("dp", None),
        P(None, None, ("dp", "tensor")),
        P(None, ("dp", "tensor")),
        P(None, "dp", None, "tensor"),
        P(None, None, "tensor"),
        P(),
        P(None, "tensor", "dp"),
        P(),
        P(None, "dp", "tensor"),
        P(None, "tensor"),
        P(None, "tensor", "dp"),
        P(),
    )

    def step(*arrays):
        return on_device(ring_order(mesh), mesh.shape["tensor"], *arrays)

    return jax.shard_map(
        step, mesh=mesh, in_specs=in_specs, out_specs=out_specs, check_vma=False
    )
```

```python
import functools

import jax
import jax.numpy as jnp
from jax import lax
from jax.experimental import pallas as pl
from jax.experimental.pallas import tpu as pltpu
from jax.sharding import PartitionSpec as P


epsilon = 1e-06
GELU_C = 0.7978845608028654
GELU_A = 0.044715
ROW_TILE = 16
NEG = -1e30
LIGHT = (2, 3, 5, 1)
RESTS = (1, 1)


def dot_plain(first_op, second_op):
    return jnp.dot(first_op, second_op, preferred_element_type=jnp.float32)


def dot_right_t(first_op, second_op):
    return lax.dot_general(
        first_op, second_op, (((1,), (1,)), ((), ())), preferred_element_type=jnp.float32
    )


def dot_left_t(first_op, second_op):
    return lax.dot_general(
        first_op, second_op, (((0,), (0,)), ((), ())), preferred_element_type=jnp.float32
    )


def norm_back(grad_normed, normed, inverse):
    return inverse * (
        grad_normed
        - jnp.mean(grad_normed, axis=-1, keepdims=True)
        - normed * jnp.mean(grad_normed * normed, axis=-1, keepdims=True)
    )


def gelu_both(values):
    inner = jnp.tanh(GELU_C * (values + GELU_A * values * values * values))
    active = 0.5 * values * (1.0 + inner)
    slope = 0.5 * (1.0 + inner) + 0.5 * values * (1.0 - inner * inner) * GELU_C * (
        1.0 + 3.0 * GELU_A * values * values
    )
    return active, slope


def head_norm(values, gain):
    head_dim = values.shape[1] // 2
    lower = lax.broadcasted_iota(jnp.int32, values.shape, 1) < head_dim
    square = values * values
    first = jnp.sum(jnp.where(lower, square, 0.0), axis=-1, keepdims=True) / head_dim
    second = jnp.sum(jnp.where(lower, 0.0, square), axis=-1, keepdims=True) / head_dim
    factor = jnp.where(lower, lax.rsqrt(first + epsilon), lax.rsqrt(second + epsilon))
    return values * factor * gain, factor


def rows_of(img_ref, txt_ref, cols):
    return jnp.concatenate(
        [img_ref[0, 0, :, cols], img_ref[1, 0, :, cols], txt_ref[0, 0, :, cols], txt_ref[1, 0, :, cols]],
        axis=0,
    )


def put_rows(img_ref, txt_ref, cols, values):
    img, txt = img_ref.shape[2], txt_ref.shape[2]
    img_ref[0, 0, :, cols] = values[:img]
    img_ref[1, 0, :, cols] = values[img : 2 * img]
    txt_ref[0, 0, :, cols] = values[2 * img : 2 * img + txt]
    txt_ref[1, 0, :, cols] = values[2 * img + txt :]


def gain_rows(gain_ref, which, img, txt):
    width = gain_ref.shape[2]
    return jnp.concatenate(
        [
            jnp.broadcast_to(gain_ref[0, which : which + 1, :], (2 * img, width)),
            jnp.broadcast_to(gain_ref[1, which : which + 1, :], (2 * txt, width)),
        ],
        axis=0,
    )


def key_bias(img, txt, real):
    where = lax.broadcasted_iota(jnp.int32, (1, 2 * (img + txt)), 1)
    first = where - 2 * img
    gone = ((first >= real) & (first < txt)) | (first >= txt + real)
    return jnp.where(gone, NEG, 0.0).astype(jnp.float32)


def probs(q_head, k_low, bias):
    scores = dot_right_t(q_head, k_low) + bias
    top = jnp.max(scores, axis=-1, keepdims=True)
    weights = jnp.exp(scores - top)
    return weights * (1.0 / jnp.sum(weights, axis=-1, keepdims=True))


def attn_forward(real, gain_ref, raw_refs, out_img_ref, out_txt_ref):
    img, txt = out_img_ref.shape[2], out_txt_ref.shape[2]
    local = out_img_ref.shape[3]
    pair = gain_ref.shape[2]
    q_gain, k_gain = gain_rows(gain_ref, 0, img, txt), gain_rows(gain_ref, 1, img, txt)
    bias = key_bias(img, txt, real)
    scale = (pair // 2) ** (-0.5)

    def one_pair(index):
        lanes = slice(index * pair, (index + 1) * pair)
        q_raw, k_raw, v_raw = (
            rows_of(raw_refs[0][part], raw_refs[1][part], lanes) for part in range(3)
        )
        q_low = head_norm(q_raw, q_gain)[0].astype(jnp.bfloat16) * jnp.bfloat16(scale)
        k_low = head_norm(k_raw, k_gain)[0].astype(jnp.bfloat16)
        v_low = v_raw.astype(jnp.bfloat16)
        lower = lax.broadcasted_iota(jnp.int32, q_raw.shape, 1) < pair // 2
        results = []
        for head in range(2):
            mine = lower if head == 0 else jnp.logical_not(lower)
            q_head = jnp.where(mine, q_low, jnp.bfloat16(0))
            results.append(dot_plain(probs(q_head, k_low, bias).astype(jnp.bfloat16), v_low))
        out = jnp.where(lower, results[0], results[1]).astype(jnp.bfloat16)
        put_rows(out_img_ref, out_txt_ref, lanes, out)

    for index in range(local // pair):
        one_pair(index)


def attn_backward_kernel(real, gain_ref, *refs):
    raw_refs = (refs[:3], refs[3:6])
    d_img_ref, d_txt_ref, o_img_ref, o_txt_ref, bias_ref, dgain_ref = refs[6:]
    img, txt = d_img_ref.shape[2], d_txt_ref.shape[2]
    local = d_img_ref.shape[3]
    pair = gain_ref.shape[2]
    head_dim = pair // 2
    q_gain, k_gain = gain_rows(gain_ref, 0, img, txt), gain_rows(gain_ref, 1, img, txt)
    bias = key_bias(img, txt, real)
    scale = head_dim ** (-0.5)

    def one_pair(index, gain_sums):
        lanes = pl.ds(pl.multiple_of(index * pair, pair), pair)
        gain_sums = list(gain_sums)
        q_raw, k_raw, v_raw = (
            rows_of(raw_refs[0][part], raw_refs[1][part], lanes) for part in range(3)
        )
        q_wide, q_factor = head_norm(q_raw, q_gain)
        k_wide, k_factor = head_norm(k_raw, k_gain)
        q_low = q_wide.astype(jnp.bfloat16) * jnp.bfloat16(scale)
        k_low = k_wide.astype(jnp.bfloat16)
        v_low = v_raw.astype(jnp.bfloat16)
        grad_out = rows_of(d_img_ref, d_txt_ref, lanes)
        lower = lax.broadcasted_iota(jnp.int32, q_raw.shape, 1) < head_dim
        parts = []
        for head in range(2):
            mine = lower if head == 0 else jnp.logical_not(lower)
            prob = probs(jnp.where(mine, q_low, jnp.bfloat16(0)), k_low, bias)
            grad_v = dot_left_t(prob.astype(jnp.bfloat16), grad_out)
            grad_prob = dot_right_t(jnp.where(mine, grad_out, jnp.bfloat16(0)), v_low)
            delta = jnp.sum(prob * grad_prob, axis=-1, keepdims=True)
            grad_scores = (prob * (grad_prob - delta)).astype(jnp.bfloat16)
            parts.append((dot_plain(grad_scores, k_low), dot_left_t(grad_scores, q_low), grad_v))
        grad_qn = jnp.where(lower, parts[0][0], parts[1][0]) * scale
        grad_kn = jnp.where(lower, parts[0][1], parts[1][1])
        grad_vn = jnp.where(lower, parts[0][2], parts[1][2])

        def raw_grad(grad_normed, raw, factor, gain, which):
            gained = grad_normed * gain
            product = gained * raw
            first = jnp.sum(jnp.where(lower, product, 0.0), axis=-1, keepdims=True) / head_dim
            second = jnp.sum(jnp.where(lower, 0.0, product), axis=-1, keepdims=True) / head_dim
            inner = jnp.where(lower, first, second)
            terms = grad_normed * raw * factor
            for stream, rows in enumerate((slice(0, 2 * img), slice(2 * img, 2 * (img + txt)))):
                place = stream * 2 + which
                gain_sums[place] = gain_sums[place] + jnp.sum(terms[rows], axis=0, keepdims=True)
            return factor * gained - raw * (factor * factor * factor) * inner

        grads = (
            raw_grad(grad_qn, q_raw, q_factor, q_gain, 0),
            raw_grad(grad_kn, k_raw, k_factor, k_gain, 1),
            grad_vn,
        )
        for part, grad in enumerate(grads):
            cols = pl.ds(pl.multiple_of(part * local + index * pair, pair), pair)
            bias_ref[0, 0:1, cols] = jnp.sum(grad[: 2 * img], axis=0, keepdims=True)
            bias_ref[0, 1:2, cols] = jnp.sum(grad[2 * img :], axis=0, keepdims=True)
            put_rows(o_img_ref, o_txt_ref, cols, grad.astype(jnp.bfloat16))
        return tuple(gain_sums)

    zero = jnp.zeros((1, pair), jnp.float32)
    gain_sums = lax.fori_loop(0, local // pair, one_pair, (zero,) * 4)
    for row in range(4):
        dgain_ref[0, row : row + 1, :] = gain_sums[row]


def block_of(array):
    shape = array.shape
    return pl.BlockSpec((shape[0], 1) + shape[2:], lambda seq: (0, seq, 0, 0))


def whole_of(array):
    return pl.BlockSpec(array.shape, lambda seq: (0,) * array.ndim)


def attn_backward(gain_pair, raw_img, raw_txt, grad_img, grad_txt, real):
    seqs, local = raw_img[0].shape[1], raw_img[0].shape[3]
    outs = [
        jax.ShapeDtypeStruct(raw_img[0].shape[:3] + (3 * local,), jnp.bfloat16),
        jax.ShapeDtypeStruct(raw_txt[0].shape[:3] + (3 * local,), jnp.bfloat16),
        jax.ShapeDtypeStruct((seqs, 2, 3 * local), jnp.float32),
        jax.ShapeDtypeStruct((seqs, 4, gain_pair.shape[2]), jnp.float32),
    ]
    rows = 2 * (raw_img[0].shape[2] + raw_txt[0].shape[2])
    return pl.pallas_call(
        functools.partial(attn_backward_kernel, real),
        grid=(seqs,),
        out_shape=outs,
        in_specs=[whole_of(gain_pair)]
        + [block_of(each) for each in raw_img + raw_txt + [grad_img, grad_txt]],
        out_specs=[
            block_of(outs[0]),
            block_of(outs[1]),
            pl.BlockSpec((1, 2, 3 * local), lambda seq: (seq, 0, 0)),
            pl.BlockSpec((1, 4, gain_pair.shape[2]), lambda seq: (seq, 0, 0)),
        ],
        compiler_params=pltpu.CompilerParams(vmem_limit_bytes=56 << 20),
        cost_estimate=pl.CostEstimate(
            flops=seqs * rows * rows * local * 10,
            bytes_accessed=seqs * rows * local * 20,
            transcendentals=seqs * rows * rows * (local // 64),
        ),
        name="attn_backward",
    )(gain_pair, *raw_img, *raw_txt, grad_img, grad_txt)


def xor_index(index, distance):
    return index + distance - 2 * distance * ((index // distance) % 2)


def peers_of(data_size, tensor_size):
    row, col = lax.axis_index("dp"), lax.axis_index("tensor")
    around = [(lax.rem(row + step, data_size), col) for step in range(1, data_size)]
    across = []
    distance = 1
    while distance < tensor_size:
        across.append((row, xor_index(col, distance)))
        distance *= 2
    return row, col, around, across


def greet(partners):
    barrier = pltpu.get_barrier_semaphore()
    for partner in partners:
        pl.semaphore_signal(barrier, inc=1, device_id=partner, device_id_type=pl.DeviceIdType.MESH)
    pl.semaphore_wait(barrier, len(partners))


def remote(source, target, sems, index, partner):
    copy = pltpu.make_async_remote_copy(
        src_ref=source,
        dst_ref=target,
        send_sem=sems.at[0, index],
        recv_sem=sems.at[1, index],
        device_id=partner,
        device_id_type=pl.DeviceIdType.MESH,
    )
    copy.start()
    return copy


def silu_of(cond_ref):
    wide = cond_ref[...].astype(jnp.float32)
    return (wide * (1.0 / (1.0 + jnp.exp(-wide)))).astype(jnp.bfloat16)


def mod_forward_kernel(
    data_size, tensor_size, cond_ref, weight_ref, bias_ref, out_ref, outgoing, blocks, sems
):
    row, col, around, across = peers_of(data_size, tensor_size)
    seqs, feat = out_ref.shape[1], out_ref.shape[2]
    silu_cond = silu_of(cond_ref)
    for stream in range(2):
        values = dot_right_t(silu_cond, weight_ref[stream]) + bias_ref[stream : stream + 1].astype(
            jnp.float32
        )
        for index in range(data_size):
            outgoing[index, stream * seqs : (stream + 1) * seqs] = values[
                index * seqs : (index + 1) * seqs
            ]
    blocks[col, row] = outgoing[row]
    greet(around + across)
    copies = [
        remote(outgoing.at[partner[0]], blocks.at[col, row], sems, index, partner)
        for index, partner in enumerate(around)
    ]
    for copy in copies:
        copy.wait()
    held, used = [0], len(around)
    for level in reversed(range(len(across))):
        distance = 1 << level
        copies = []
        for offset in held:
            index = col
            for bit in range(len(across)):
                if offset >> bit & 1:
                    index = xor_index(index, 1 << bit)
            copies.append(remote(blocks.at[index], blocks.at[index], sems, used, across[level]))
            used += 1
        for copy in copies:
            copy.wait()
        held = held + [offset | distance for offset in held]
    for stream in range(2):
        full = jnp.concatenate(
            [
                blocks[second, first, stream * seqs : (stream + 1) * seqs]
                for first in range(data_size)
                for second in range(tensor_size)
            ],
            axis=1,
        )
        for index in range(6):
            out_ref[stream * 6 + index] = full[:, index * feat : (index + 1) * feat]


def mod_forward(conditioning, ada_weight, ada_bias, seqs, feat, data_size, tensor_size):
    cols = ada_weight.shape[1]
    vmem = pl.BlockSpec(memory_space=pltpu.VMEM)
    return pl.pallas_call(
        functools.partial(mod_forward_kernel, data_size, tensor_size),
        out_shape=jax.ShapeDtypeStruct((12, seqs, feat), jnp.float32),
        in_specs=[vmem] * 3,
        out_specs=vmem,
        scratch_shapes=[
            pltpu.VMEM((data_size, 2 * seqs, cols), jnp.float32),
            pltpu.VMEM((tensor_size, data_size, 2 * seqs, cols), jnp.float32),
            pltpu.SemaphoreType.DMA((2, data_size + tensor_size)),
        ],
        compiler_params=pltpu.CompilerParams(
            collective_id=0, has_side_effects=True, vmem_limit_bytes=32 << 20
        ),
        name="mod_forward",
    )(conditioning, ada_weight, ada_bias)


def mod_backward_steps(data_size, tensor_size, mod_rows, cond_ref, weight_of, lines_of, put, scratch, sems):
    blocks, core_in, outgoing, cols_in, lines, lines_in, lines_own, lines_all = scratch[:8]
    silu_blocks, silu_in, silu_send, silu_recv, all_send, all_recv = scratch[8:]
    row, col, around, across = peers_of(data_size, tensor_size)
    seqs, cols = outgoing.shape[1] // 2, outgoing.shape[2]
    half, width = lines.shape[1] // 2, lines.shape[2]
    for stream in range(2):
        full = mod_rows(stream)
        for first in range(data_size):
            for second in range(tensor_size):
                start = (first * tensor_size + second) * cols
                blocks[second, first, stream * seqs : (stream + 1) * seqs] = full[
                    :, start : start + cols
                ]
    every_line = lines_of()
    for index in range(data_size):
        lines[index] = every_line[:, index * width : (index + 1) * width]

    used = 0
    copy = remote(blocks.at[xor_index(col, 1)], core_in, sems, used, across[0])
    used += 1
    yield
    copy.wait()
    for first in range(data_size):
        outgoing[first] = blocks[col, first] + core_in[first]

    cols_in[row] = outgoing[row]
    lines_in[row] = lines[row]
    copies = []
    for partner in around:
        for source, target in ((lines, lines_in), (outgoing, cols_in)):
            copies.append(
                remote(source.at[partner[0]], target.at[row], sems, used, partner)
            )
            used += 1
    silu_cond = silu_of(cond_ref)
    yield
    for copy in copies:
        copy.wait()
    lines_own[...] = functools.reduce(jnp.add, [lines_in[index] for index in range(data_size)])
    low = []
    for stream in range(2):
        wide = jnp.concatenate(
            [cols_in[index, stream * seqs : (stream + 1) * seqs] for index in range(data_size)],
            axis=0,
        )
        put(("ada_bias", stream), jnp.sum(wide, axis=0, keepdims=True))
        low.append(wide.astype(jnp.bfloat16))
    silu_grad = dot_plain(low[0], weight_of(0)) + dot_plain(low[1], weight_of(1))
    for index in range(data_size):
        silu_blocks[index] = silu_grad[index * seqs : (index + 1) * seqs]
    for stream in range(2):
        put(("ada_weight", stream), lambda span: dot_left_t(low[stream], silu_cond[:, span]))

    silu_in[row] = silu_blocks[row]
    lines_all[row] = lines_own[...]
    copies = []
    for partner in around:
        for source, target in (
            (silu_blocks.at[partner[0]], silu_in.at[row]),
            (lines_own, lines_all.at[row]),
        ):
            copies.append(remote(source, target, sems, used, partner))
            used += 1
    yield
    for copy in copies:
        copy.wait()
    silu_send[0] = functools.reduce(jnp.add, [silu_in[index] for index in range(data_size)])
    every_line = jnp.concatenate([lines_all[index] for index in range(data_size)], axis=1)
    all_send[0] = every_line[half:]
    put("group", every_line[:half])

    for level, partner in enumerate(across):
        copies = [
            remote(silu_send.at[level], silu_recv.at[level], sems, used, partner),
            remote(all_send.at[level], all_recv.at[level], sems, used + 1, partner),
        ]
        used += 2
        yield
        for copy in copies:
            copy.wait()
        silu_send[level + 1] = silu_send[level] + silu_recv[level]
        all_send[level + 1] = all_send[level] + all_recv[level]
    put("silu", silu_send[len(across)])
    put("every", all_send[len(across)])


def mod_scratch(data_size, tensor_size, seqs, feat, cols):
    levels, lines = tensor_size.bit_length() - 1, 16
    width = feat // data_size

    def wide(*shape):
        return pltpu.VMEM(shape, jnp.float32)

    return [
        wide(tensor_size, data_size, 2 * seqs, cols),
        wide(data_size, 2 * seqs, cols),
        wide(data_size, 2 * seqs, cols),
        wide(data_size, 2 * seqs, cols),
        wide(data_size, lines, width),
        wide(data_size, lines, width),
        wide(lines, width),
        wide(data_size, lines, width),
        wide(data_size, seqs, feat),
        wide(data_size, seqs, feat),
        wide(levels + 1, seqs, feat),
        wide(levels, seqs, feat),
        wide(levels + 1, lines // 2, feat),
        wide(levels, lines // 2, feat),
    ], pltpu.SemaphoreType.DMA((2, 1 + 4 * (data_size - 1) + 2 * levels))


def norm_of(values):
    center = values - jnp.mean(values, axis=-1, keepdims=True)
    inverse = lax.rsqrt(jnp.mean(center * center, axis=-1, keepdims=True) + epsilon)
    return center * inverse, inverse


def ring_order(mesh):
    size = mesh.shape["dp"]
    fallback = list(range(0, size, 2)) + list(range(1, size, 2))[::-1]
    axis = list(mesh.axis_names).index("dp")
    devices = mesh.devices
    line = [devices[(slice(None),) * axis + (index,)].flatten()[0] for index in range(size)]
    coords = [getattr(device, "coords", None) for device in line]
    if any(place is None for place in coords):
        return fallback
    near = [
        [
            other
            for other in range(size)
            if sum(abs(a - b) for a, b in zip(coords[index], coords[other])) == 1
        ]
        for index in range(size)
    ]
    path, seen, budget = [0], {0}, [200000]

    def extend():
        budget[0] -= 1
        if budget[0] < 0:
            return False
        if len(path) == size:
            return path[0] in near[path[-1]]
        choices = [index for index in near[path[-1]] if index not in seen]
        choices.sort(key=lambda index: (sum(o not in seen for o in near[index]), index))
        for index in choices:
            path.append(index)
            seen.add(index)
            if extend():
                return True
            path.pop()
            seen.remove(index)
        return False

    return path if extend() else fallback


def entry_of(table, index):
    value = jnp.int32(table[0])
    for place in range(1, len(table)):
        value = jnp.where(index == place, jnp.int32(table[place]), value)
    return value


def over_rows(base, length, feat, count, body, groups=(4, 5, 3, 2, 1)):
    tile = ROW_TILE
    group = next(size for size in groups if length // tile % size == 0)

    def step(index, carry):
        for place in range(group):
            start = pl.multiple_of(base + (index * group + place) * tile, tile)
            adds = body(pl.ds(start, tile))
            carry = tuple(
                total + add[: tile // 2] + add[tile // 2 :] for total, add in zip(carry, adds)
            )
        return carry

    zero = jnp.zeros((tile // 2, feat), jnp.float32)
    totals = lax.fori_loop(0, length // (tile * group), step, (zero,) * count)
    return [jnp.sum(total, axis=0, keepdims=True) for total in totals]


def shifted(rows, by):
    return pl.ds(pl.multiple_of(rows.start + by, ROW_TILE), rows.size)


def half_of(array, half, seq, by_seq):
    return array.at[seq, half] if by_seq else array.at[half, seq]


def move_halves(move, array, rows_ref, seqs, by_seq, to_array=False, halves=2):
    core = lax.axis_index("tensor") % 2
    length = rows_ref.shape[0] // (halves * seqs)
    copies = []
    for half, position in enumerate((core, 1 - core)[:halves]):
        for seq in range(seqs):
            start = (half * seqs + seq) * length
            ends = (half_of(array, position, seq, by_seq), rows_ref.at[start : start + length])
            copies.append(move(*(ends[::-1] if to_array else ends)))
    return copies


def wait_all(copies):
    for copy in copies:
        copy.wait()


class Ring:
    def __init__(self, order, rest, lefts, rights, slots, terms, turned, sems):
        self.order, self.size, self.rest = order, len(order), rest
        self.lefts, self.rights, self.slots, self.terms = lefts, rights, slots, terms
        self.turned, self.sems = turned, sems
        row, col = lax.axis_index("dp"), lax.axis_index("tensor")
        size = self.size
        self.place = entry_of([order.index(index) for index in range(size)], row)
        self.after = entry_of(order, lax.rem(self.place + 1, size))
        self.before = entry_of(order, lax.rem(self.place + size - 1, size))
        self.targets = ((self.after, col), (self.before, col))
        self.half = slots[0].shape[2]
        self.chains = [(which, way) for which in range(len(lefts)) for way in range(2)]
        self.last = size - 2 - rest

    def term(self, which, way, index):
        start = pl.multiple_of((2 * index + way) * self.half, 8)
        return dot_plain(
            self.turned[which][pl.ds(start, self.half), :], self.rights[which][...]
        )

    def work_out(self, indices):
        for which in range(len(self.lefts)):

            def one_way(way, carry):
                index = jnp.where(way == 0, indices[0], indices[1])
                self.terms[which][way] = self.term(which, way, index)
                return carry

            lax.fori_loop(0, 2, one_way, 0)

    def copy_of(self, which, way, step, source, target):
        return pltpu.make_async_remote_copy(
            src_ref=source,
            dst_ref=self.slots[which].at[way, target],
            send_sem=self.sems.at[0, which, way, step],
            recv_sem=self.sems.at[1, which, way, step],
            device_id=(jnp.where(way == 0, self.after, self.before), self.targets[0][1]),
            device_id_type=pl.DeviceIdType.MESH,
        )

    def blocks_at(self, step):
        size = self.size
        return (
            entry_of(self.order, lax.rem(self.place + 2 * size - 2 - step, size)),
            entry_of(self.order, lax.rem(self.place + 2 + step, size)),
        )

    def arrive(self, which, way, step):
        slot = self.slots[which].at[way, step]
        self.copy_of(which, way, step, slot, step).wait_recv()

    def begin(self, which):
        width = 256

        def turn(index, carry):
            span = pl.ds(pl.multiple_of(index * width, width), width)
            self.turned[which][span, :] = self.lefts[which][:, span].T
            return carry

        lax.fori_loop(0, self.turned[which].shape[0] // width, turn, 0)

        def one_way(way, carry):
            index = jnp.where(way == 0, self.before, self.after)
            self.slots[which][way, self.size - 1] = self.term(which, way, index)
            return carry

        lax.fori_loop(0, 2, one_way, 0)
        for way in range(2):
            self.copy_of(which, way, 0, self.slots[which].at[way, self.size - 1], 0).start()

    def rounds(self, first, last):
        def round_of(step, carry):
            self.work_out(self.blocks_at(step))
            for which in range(len(self.lefts)):

                def one_way(way, inner):
                    self.arrive(which, way, step)
                    slot = self.slots[which].at[way, step]
                    slot[...] = slot[...] + self.terms[which][way]
                    self.copy_of(which, way, step + 1, slot, step + 1).start()
                    return inner

                lax.fori_loop(0, 2, one_way, 0)
            return carry

        lax.fori_loop(first, last, round_of, 0)

    def finish(self, put_later, put_total):
        def settle(turn, carry):
            step = jnp.where(turn < self.rest, self.last + 1 + turn, self.last)
            self.work_out(self.blocks_at(step))
            for later in range(self.rest):

                @pl.when(turn == later)
                def _():
                    for which, way in self.chains:
                        put_later(later, which, way, self.terms[which][way])

            return carry

        lax.fori_loop(0, self.rest + 1, settle, 0)
        for which, way in self.chains:
            self.arrive(which, way, self.last)
            put_total(which, way, self.slots[which][way, self.last] + self.terms[which][way])

        def sent(step, carry):
            for which, way in self.chains:
                slot = self.slots[which].at[way, self.size - 1]
                self.copy_of(which, way, step, slot, step).wait_send()
            return carry

        lax.fori_loop(0, self.last + 1, sent, 0)


def taker(refs):
    refs = list(refs)

    def take(number):
        taken = refs[:number]
        del refs[:number]
        return taken

    return take


def ring_scratch(size, halves, lefts, count_kind=jnp.bfloat16):
    return (
        [pltpu.VMEM((2, size) + half, jnp.float32) for half in halves]
        + [pltpu.VMEM((2,) + half, jnp.float32) for half in halves]
        + [pltpu.VMEM(shape[::-1], count_kind) for shape in lefts]
        + [pltpu.SemaphoreType.DMA((2, len(halves), 2, size - 1))]
    )


def front_kernel(seqs, real, block, by_seqs, *refs):
    take = taker(refs)
    mod_ref, gain_ref, bias_ref = take(3)
    input_hbm = take(2)
    weight_hbm, proj_hbm = take(2)
    hidden_hbm, raw_hbm, attn_hbm, sum_hbm = take(2), (take(3), take(3)), take(2), take(2)
    (got_hbm,) = take(1)
    inputs, hidden, raw, attn = take(2), take(2), (take(3), take(3)), take(2)
    weight_ref, proj_ref = take(2)
    outgoing, incoming, own = take(2), take(2), take(2)
    load_sems, core_sems, swap_sems, out_sems = take(4)
    feat = hidden[0].shape[1]
    lengths = [ref.shape[2] for ref in attn]
    partner = (lax.axis_index("dp"), xor_index(lax.axis_index("tensor"), 1))
    facing = (lax.axis_index("dp"), xor_index(lax.axis_index("tensor"), 2))
    started = []

    def load(source, target):
        copy = pltpu.make_async_copy(source, target, load_sems.at[len(started)])
        copy.start()
        started.append(copy)
        return copy

    input_loads = [
        move_halves(load, input_hbm[stream], inputs[stream], seqs, by_seqs[stream]) for stream in range(2)
    ]
    weight_loads = [load(weight_hbm, weight_ref), load(proj_hbm, proj_ref)]
    greet((partner, facing))
    for copies in input_loads:
        wait_all(copies)

    def core_copy(stream, seq):
        span = pl.ds(pl.multiple_of(seq * lengths[stream], ROW_TILE), lengths[stream])
        return pltpu.make_async_remote_copy(
            src_ref=outgoing[stream].at[span],
            dst_ref=incoming[stream].at[span],
            send_sem=core_sems.at[0, stream, seq],
            recv_sem=core_sems.at[1, stream, seq],
            device_id=partner,
            device_id_type=pl.DeviceIdType.MESH,
        )

    def chip_copy(seq):
        span = pl.ds(pl.multiple_of(seq * lengths[1], ROW_TILE), lengths[1])
        return pltpu.make_async_remote_copy(
            src_ref=own[1].at[span],
            dst_ref=got_hbm.at[span],
            send_sem=swap_sems.at[0, seq],
            recv_sem=swap_sems.at[1, seq],
            device_id=facing,
            device_id_type=pl.DeviceIdType.MESH,
        )

    def normalize(seq):
        for stream in range(2):
            shift = mod_ref[stream * 6, pl.ds(seq, 1), :]
            scale = 1.0 + mod_ref[stream * 6 + 1, pl.ds(seq, 1), :]

            def first_norm(at):
                normed, _ = norm_of(inputs[stream][at].astype(jnp.float32))
                hidden[stream][at] = (normed * scale + shift).astype(jnp.bfloat16)
                return ()

            def one_half(half, carry):
                over_rows((half * seqs + seq) * lengths[stream], lengths[stream], feat, 0, first_norm)
                return carry

            lax.fori_loop(0, 2, one_half, 0)

    def attend(seq):
        for stream in range(2):
            length = lengths[stream]
            left = jnp.concatenate(
                [
                    hidden[stream][pl.ds(pl.multiple_of((half * seqs + seq) * length, ROW_TILE), length), :]
                    for half in range(2)
                ],
                axis=0,
            )
            for part in range(3):
                values = dot_plain(left, weight_ref[stream, part]) + bias_ref[part, stream : stream + 1].astype(
                    jnp.float32
                )
                raw[stream][part][0, seq] = values[:length]
                raw[stream][part][1, seq] = values[length:]
        one = pl.ds(seq, 1)
        attn_forward(
            real,
            gain_ref,
            [[ref.at[:, one] for ref in raw[stream]] for stream in range(2)],
            attn[0].at[:, one],
            attn[1].at[:, one],
        )
        for stream in (1, 0):
            length = lengths[stream]
            span = pl.ds(pl.multiple_of(seq * length, ROW_TILE), length)
            left = jnp.concatenate([attn[stream][0, seq], attn[stream][1, seq]], axis=0)
            for start in range(0, feat, block):
                cols = slice(start, start + block)
                both = dot_plain(left, proj_ref[stream, :, cols])
                own[stream][span, cols] = both[:length]
                outgoing[stream][span, cols] = both[length:]
            core_copy(stream, seq).start()

    def pass_on(seq):
        for stream in (1, 0):
            core_copy(stream, seq).wait()

            def add(at):
                own[stream][at] = own[stream][at] + incoming[stream][at]
                return ()

            over_rows(seq * lengths[stream], lengths[stream], feat, 0, add, LIGHT)
            if stream == 1:
                chip_copy(seq).start()

    def one_sequence(seq, carry):
        normalize(seq)

        @pl.when(seq == 0)
        def _():
            wait_all(weight_loads)

        @pl.when(seq > 0)
        def _():
            pass_on(seq - 1)

        attend(seq)
        return carry

    lax.fori_loop(0, seqs, one_sequence, 0)
    stores = []
    for source, target in zip(
        list(hidden) + list(raw[0]) + list(raw[1]) + list(attn),
        list(hidden_hbm) + list(raw_hbm[0]) + list(raw_hbm[1]) + list(attn_hbm),
    ):
        stores.append(pltpu.make_async_copy(source, target, out_sems.at[len(stores)]))
        stores[-1].start()
    pass_on(seqs - 1)
    for source, target in zip(own, sum_hbm):
        stores.append(pltpu.make_async_copy(source, target, out_sems.at[len(stores)]))
        stores[-1].start()
    for copy in stores:
        copy.wait()

    def arrive(seq, carry):
        chip_copy(seq).wait()
        return carry

    lax.fori_loop(0, seqs, arrive, 0)


def front(modulate, gain_pair, inputs, by_seqs, weight, bias, proj_weight, real, collective_id):
    seqs, feat = modulate.shape[1:]
    local = weight.shape[3]
    lengths = [array.shape[2] for array in inputs]
    rows = [seqs * length for length in lengths]
    vmem = pl.BlockSpec(memory_space=pltpu.VMEM)
    anywhere = pl.BlockSpec(memory_space=pl.ANY)
    shapes = [((2 * count, feat), jnp.bfloat16) for count in rows]
    shapes += [((2, seqs, length, local), jnp.float32) for length in lengths for _ in range(3)]
    shapes += [((2, seqs, length, local), jnp.bfloat16) for length in lengths]
    sums = [((count, feat), jnp.float32) for count in rows]
    outs = shapes + sums + sums[1:]
    results = pl.pallas_call(
        functools.partial(front_kernel, seqs, real, 512, by_seqs),
        out_shape=[jax.ShapeDtypeStruct(*out) for out in outs],
        in_specs=[vmem] * 3 + [anywhere] * 4,
        out_specs=[anywhere] * len(outs),
        scratch_shapes=[pltpu.VMEM((2 * count, feat), jnp.bfloat16) for count in rows]
        + [pltpu.VMEM(*shape) for shape in shapes]
        + [pltpu.VMEM(weight.shape, jnp.bfloat16), pltpu.VMEM(proj_weight.shape, jnp.bfloat16)]
        + [pltpu.VMEM(*each) for each in sums] * 3
        + [
            pltpu.SemaphoreType.DMA((2 + 4 * seqs,)),
            pltpu.SemaphoreType.DMA((2, 2, seqs)),
            pltpu.SemaphoreType.DMA((2, seqs)),
            pltpu.SemaphoreType.DMA((len(shapes) + 2,)),
        ],
        compiler_params=pltpu.CompilerParams(
            collective_id=collective_id, has_side_effects=True, vmem_limit_bytes=60 << 20
        ),
        name="front",
    )(
        modulate,
        gain_pair,
        bias,
        *inputs,
        weight,
        proj_weight,
    )
    return results[:2], (results[2:5], results[5:8]), results[8:10], results[10:12], results[12]


def mlp_ring_kernel(order, stream, seqs, block, swaps, rest, direct, *refs):
    take = taker(refs)
    mod_ref, proj_bias_ref, up_bias_ref, down_bias_ref = take(4)
    mine_hbm, got_hbm, input_hbm, cot_hbm, up_hbm, down_hbm, proj_hbm = take(7)
    gives = take(swaps)
    outs = take(2 * (rest + 1)) if rest else take(2)
    gets = take(swaps)
    up_sum_ref, down_sum_ref, proj_sum_ref, mod_sum_ref = take(4)
    branch_hbm, normed_hbm, hidden_got_hbm, mlp_got_hbm, through_hbm = take(5)
    grad_branch_hbm, grad_attn_hbm, out_hbm = take(3)
    slots, terms, turned = take(2), take(2), take(2)
    (ring_sems,) = take(1)
    up_ref, down_ref, input_ref, hidden_ref, active_ref, grad_up_ref, grad_mlp_ref = take(7)
    proj_ref, grad_attn_ref, inverse_ref = take(3)
    mine_ref, got_ref, branch_ref, normed_ref, normed_in, spare = take(6)
    load_sems, core_sems, swap_sems, out_sems, ready_sem = take(5)
    rows, feat = mine_ref.shape
    units = active_ref.shape[1]
    length = rows // seqs
    ring = Ring(
        order, rest, (grad_mlp_ref, hidden_ref), (active_ref, grad_up_ref), slots, terms, turned, ring_sems
    )
    partner = (lax.axis_index("dp"), xor_index(lax.axis_index("tensor"), 1))
    facing = (lax.axis_index("dp"), xor_index(lax.axis_index("tensor"), 2))

    started = []

    def load(source, target):
        copy = pltpu.make_async_copy(source, target, load_sems.at[len(started)])
        copy.start()
        started.append(copy)
        return copy

    first_loads = [load(mine_hbm, mine_ref), load(got_hbm, got_ref)]
    first_loads += move_halves(load, input_hbm, input_ref, seqs, direct)
    cot_loads = move_halves(load, cot_hbm, grad_mlp_ref, seqs, direct)
    weight_loads = [
        load(up_hbm.at[stream], up_ref),
        load(down_hbm.at[stream], down_ref),
        load(proj_hbm.at[stream], proj_ref),
    ]
    greet(ring.targets + (facing, partner))
    swapped = [
        remote(gives[index], gets[index], swap_sems, index, facing) for index in range(swaps)
    ]

    def mod(index, seq):
        return mod_ref[stream * 6 + index, pl.ds(seq, 1), :]

    count = feat // block
    ways = ((normed_ref, normed_in, 0), (branch_ref, got_ref, seqs + 2 * count), (normed_ref, got_ref, 2 * seqs + 2 * count))

    def row_copy(kind, seq):
        source, target, first = ways[kind]
        span = pl.ds(pl.multiple_of(seq * length, ROW_TILE), length)
        return pltpu.make_async_remote_copy(
            src_ref=source.at[span],
            dst_ref=target.at[span],
            send_sem=core_sems.at[0, first + seq],
            recv_sem=core_sems.at[1, first + seq],
            device_id=partner,
            device_id_type=pl.DeviceIdType.MESH,
        )

    stored = []

    def store(source, target):
        copy = pltpu.make_async_copy(source, target, out_sems.at[len(stored)])
        copy.start()
        stored.append(copy)
        return copy

    def row_sum(values):
        return jnp.sum(values, axis=0, keepdims=True)

    wait_all(first_loads)
    proj_bias = proj_bias_ref[stream : stream + 1].astype(jnp.float32)

    def second_norms(seq, carry):
        gate, shift, scale = mod(2, seq), mod(3, seq), 1.0 + mod(4, seq)

        def second_norm(at):
            branch = mine_ref[at] + got_ref[at] + proj_bias
            branch_ref[at] = branch
            normed, inverse = norm_of(input_ref[at].astype(jnp.float32) + gate * branch)
            normed_ref[at] = normed
            inverse_ref[at] = inverse
            hidden_ref[at] = (normed * scale + shift).astype(jnp.bfloat16)
            return ()

        over_rows(seq * length, length, feat, 0, second_norm)
        row_copy(0, seq).start()
        return carry

    lax.fori_loop(0, seqs, second_norms, 0)
    kept = [store(branch_ref, branch_hbm), store(normed_ref, normed_hbm)]
    wait_all(cot_loads)

    def gate_rows(turn, own_total):
        gate = mod(5, lax.rem(turn, seqs))

        def gated(at):
            grad_mlp = grad_mlp_ref[at].astype(jnp.float32) * gate
            grad_mlp_ref[at] = grad_mlp.astype(jnp.bfloat16)
            return (grad_mlp,)

        (total,) = over_rows(turn * length, length, feat, 1, gated, LIGHT)
        return own_total + jnp.where(turn < seqs, total, 0.0)

    down_sum_ref[...] = lax.fori_loop(0, 2 * seqs, gate_rows, jnp.zeros((1, feat), jnp.float32))

    def other_hiddens(seq, carry):
        row_copy(0, seq).wait()
        shift, scale = mod(3, seq), 1.0 + mod(4, seq)

        def other_hidden(at):
            hidden_ref[shifted(at, rows)] = (normed_in[at] * scale + shift).astype(jnp.bfloat16)
            return ()

        over_rows(seq * length, length, feat, 0, other_hidden, LIGHT)
        return carry

    lax.fori_loop(0, seqs, other_hiddens, 0)
    wait_all(weight_loads)

    def unit_block(index, carry):
        cols = pl.ds(pl.multiple_of(index * block, block), block)
        upward = dot_plain(hidden_ref[...], up_ref[:, cols]) + up_bias_ref[
            stream : stream + 1, cols
        ].astype(jnp.float32)
        active, slope = gelu_both(upward)
        active_ref[:, cols] = active.astype(jnp.bfloat16)
        grad_up = dot_right_t(grad_mlp_ref[...], down_ref[cols, :]) * slope
        up_sum_ref[:, cols] = row_sum(grad_up)
        grad_up_ref[:, cols] = grad_up.astype(jnp.bfloat16)
        return carry

    lax.fori_loop(0, units // block, unit_block, 0)
    for which in range(2):
        ring.begin(which)

    wait_all(kept)
    sums = ((branch_ref, mine_ref, normed_in), (normed_ref, got_ref, spare))

    def columns(index):
        return pl.ds(pl.multiple_of(index * block, block), block)

    def part_copy(kind, index):
        return pltpu.make_async_remote_copy(
            src_ref=sums[kind][0].at[:, columns(index)],
            dst_ref=sums[kind][1].at[:, columns(index)],
            send_sem=core_sems.at[0, seqs + kind * count + index],
            recv_sem=core_sems.at[1, seqs + kind * count + index],
            device_id=partner,
            device_id_type=pl.DeviceIdType.MESH,
        )

    for kind, (outgoing, _, own) in enumerate(sums):

        def send_part(index, carry):
            cols = columns(index)
            if kind == 0:
                both = dot_right_t(grad_up_ref[...], up_ref[cols, :])
            else:
                both = dot_plain(active_ref[...], down_ref[:, cols])
            own[:, cols] = both[:rows]
            outgoing[:, cols] = both[rows:]
            part_copy(kind, index).start()
            return carry

        lax.fori_loop(0, count, send_part, 0)
    exchanges = []
    for kind, got in enumerate((hidden_got_hbm, mlp_got_hbm)):
        _, incoming, own = sums[kind]

        def add_part(index, carry):
            part_copy(kind, index).wait()
            cols = columns(index)
            own[:, cols] = own[:, cols] + incoming[:, cols]
            return carry

        lax.fori_loop(0, count, add_part, 0)
        exchanges.append(remote(own, got, swap_sems, swaps + kind, facing))
    pl.semaphore_signal(ready_sem, inc=1, device_id=partner, device_id_type=pl.DeviceIdType.MESH)
    again = [load(branch_hbm, branch_ref), load(normed_hbm, normed_ref)]
    again += move_halves(load, cot_hbm, hidden_ref.at[:rows], seqs, direct, halves=1)
    middle = min(3, ring.last)
    ring.rounds(0, middle)

    exchanges[0].wait()
    again.append(load(hidden_got_hbm, mine_ref))
    wait_all(again)
    pl.semaphore_wait(ready_sem, 1)

    def back_rows(seq, proj_total):
        gate, scale = mod(2, seq), 1.0 + mod(4, seq)

        def back(at):
            grad_hidden = normed_in[at] + mine_ref[at]
            normed = normed_ref[at]
            through = norm_back(grad_hidden * scale, normed, inverse_ref[at])
            grad_resid = hidden_ref[at].astype(jnp.float32) + through
            branch = branch_ref[at]
            normed_in[at] = through
            branch_ref[at] = grad_resid
            grad_mlp_ref[at] = (grad_resid * gate).astype(jnp.bfloat16)
            return grad_resid * branch, grad_hidden, grad_hidden * normed, grad_resid

        totals = over_rows(seq * length, length, feat, 4, back)
        for index in range(3):
            mod_sum_ref[index, pl.ds(seq, 1)] = totals[index]
        row_copy(1, seq).start()
        return proj_total + totals[3] * gate

    proj_sum_ref[...] = lax.fori_loop(0, seqs, back_rows, jnp.zeros((1, feat), jnp.float32))
    store(normed_in, through_hbm)

    def other_backs(seq, carry):
        row_copy(1, seq).wait()
        gate = mod(2, seq)

        def other_back(at):
            grad_mlp_ref[shifted(at, rows)] = (got_ref[at] * gate).astype(jnp.bfloat16)
            return ()

        over_rows(seq * length, length, feat, 0, other_back, LIGHT)
        return carry

    lax.fori_loop(0, seqs, other_backs, 0)
    grad_attn_ref[...] = dot_right_t(grad_mlp_ref[...], proj_ref[...]).astype(jnp.bfloat16)
    store(grad_mlp_ref, grad_branch_hbm)
    store(grad_attn_ref, grad_attn_hbm)
    pl.semaphore_signal(ready_sem, inc=1, device_id=partner, device_id_type=pl.DeviceIdType.MESH)
    again = [load(branch_hbm, branch_ref)]
    ring.rounds(middle, ring.last)

    exchanges[1].wait()
    again.append(load(mlp_got_hbm, mine_ref))
    wait_all(again)
    pl.semaphore_wait(ready_sem, 1)
    down_bias = down_bias_ref[stream : stream + 1].astype(jnp.float32)

    def finish_sequences(seq, carry):
        first_gate, second_gate = mod(2, seq), mod(5, seq)

        def finish_rows(at):
            mlp_out = spare[at] + mine_ref[at] + down_bias
            added = first_gate * branch_ref[at] + second_gate * mlp_out
            normed_ref[at] = added
            input_ref[at] = (input_ref[at].astype(jnp.float32) + added).astype(jnp.bfloat16)
            return (hidden_ref[at].astype(jnp.float32) * mlp_out,)

        (mod_sum_ref[3, pl.ds(seq, 1)],) = over_rows(seq * length, length, feat, 1, finish_rows)
        row_copy(2, seq).start()
        return carry

    lax.fori_loop(0, seqs, finish_sequences, 0)

    def other_outs(seq, carry):
        row_copy(2, seq).wait()

        def other_rows(at):
            there = shifted(at, rows)
            input_ref[there] = (input_ref[there].astype(jnp.float32) + got_ref[at]).astype(jnp.bfloat16)
            return ()

        over_rows(seq * length, length, feat, 0, other_rows, LIGHT)
        return carry

    lax.fori_loop(0, seqs, other_outs, 0)
    move_halves(store, out_hbm, input_ref, seqs, direct, to_array=True)

    buffers = (mine_ref, got_ref, branch_ref, normed_ref)
    each = rows // (2 * ring.half)

    def piece_of(index):
        start = index % each * 2 * ring.half
        return buffers[index // each].at[start : start + 2 * ring.half]

    def put_later(later, which, way, values):
        piece_of(2 * (later + 1) + way)[which * ring.half : (which + 1) * ring.half] = values

    def put_total(which, way, values):
        if rest:
            piece_of(way)[which * ring.half : (which + 1) * ring.half] = values
        else:
            outs[which][0, way * ring.half : (way + 1) * ring.half] = values

    ring.finish(put_later, put_total)
    if rest:
        for index, out in enumerate(outs):
            store(piece_of(index), out)
    for copy in swapped:
        copy.wait()
    for copy in stored[len(kept) :]:
        copy.wait()


def mlp_ring(
    stream, mine, got, inputs, cots, modulate, proj_bias, up_bias, down_bias, up_weight, down_weight,
    proj_weight, gives, order, rest, direct, collective_id,
):
    seqs, feat = modulate.shape[1:]
    length = inputs.shape[2]
    rows, units, size, swaps = seqs * length, up_weight.shape[2], len(order), len(gives)
    local = proj_weight.shape[1]
    block = 256
    half = feat // (2 * size)
    vmem = pl.BlockSpec(memory_space=pltpu.VMEM)
    anywhere = pl.BlockSpec(memory_space=pl.ANY)

    def wide(*dims):
        return jax.ShapeDtypeStruct(dims, jnp.float32)

    def narrow(*dims):
        return jax.ShapeDtypeStruct(dims, jnp.bfloat16)

    def low(*dims):
        return pltpu.VMEM(dims, jnp.bfloat16)

    ring_outs = [wide(2 * half, units)] * (2 * (rest + 1)) if rest else [wide(1, 2 * half, units)] * 2
    gets = [jax.ShapeDtypeStruct(give.shape, give.dtype) for give in gives]
    small = {
        "up_bias": wide(1, units),
        "down_bias": wide(1, feat),
        "proj_bias": wide(1, feat),
        "mod_sums": wide(4, seqs, feat),
    }
    large = {name: wide(rows, feat) for name in ("branch", "normed", "hidden_got", "mlp_got", "through")}
    large |= {
        "grad_branch": narrow(2 * rows, feat),
        "grad_attn": narrow(2 * rows, local),
        "out": narrow(*inputs.shape),
    }
    moved = 4 * 2 * 2 * (size - 1) * half * units
    blocks = 2 * feat // block
    results = pl.pallas_call(
        functools.partial(mlp_ring_kernel, order, stream, seqs, block, swaps, rest, direct),
        out_shape=ring_outs + gets + list(small.values()) + list(large.values()),
        in_specs=[vmem] * 4 + [anywhere] * (7 + swaps),
        out_specs=[anywhere if rest else vmem] * len(ring_outs)
        + [anywhere] * swaps
        + [vmem] * len(small)
        + [anywhere] * len(large),
        scratch_shapes=ring_scratch(size, [(half, units)] * 2, [(2 * rows, feat)] * 2)
        + [
            low(feat, units),
            low(units, feat),
            low(2 * rows, feat),
            low(2 * rows, feat),
            low(2 * rows, units),
            low(2 * rows, units),
            low(2 * rows, feat),
            low(local, feat),
            low(2 * rows, local),
            pltpu.VMEM((rows, 1), jnp.float32),
        ]
        + [pltpu.VMEM((rows, feat), jnp.float32)] * 6
        + [
            pltpu.SemaphoreType.DMA((10 + 5 * seqs,)),
            pltpu.SemaphoreType.DMA((2, 3 * seqs + blocks)),
            pltpu.SemaphoreType.DMA((2, swaps + 2)),
            pltpu.SemaphoreType.DMA((6 + 2 * seqs + len(ring_outs),)),
            pltpu.SemaphoreType.REGULAR,
        ],
        compiler_params=pltpu.CompilerParams(
            collective_id=collective_id, has_side_effects=True, vmem_limit_bytes=67043328
        ),
        cost_estimate=pl.CostEstimate(flops=moved * 10000, bytes_accessed=moved, transcendentals=0),
        name="mlp_ring",
    )(
        modulate,
        proj_bias,
        up_bias,
        down_bias,
        mine,
        got,
        inputs,
        cots,
        up_weight,
        down_weight,
        proj_weight,
        *gives,
    )
    ring_parts, results = results[: len(ring_outs)], results[len(ring_outs) :]
    made = dict(zip(list(small) + list(large), results[swaps:]))
    made["ring"], made["gets"] = ring_parts, results[:swaps]
    return made


def attn_ring_kernel(order, tensor_size, seqs, block, row_share, directs, *refs):
    take = taker(refs)
    mod_ref, cond_ref, gain_sum_ref, bias_sum_ref = take(4)
    small_sums = (take(4), take(4))
    packed_hbm, attn_hbm, hidden_hbm, branch_hbm = take(2), take(2), take(2), take(2)
    through_hbm, input_hbm, cot_hbm = take(2), take(2), take(2)
    weight_hbm, ada_hbm = take(2)
    arrived = (take(4), take(4))
    out_hbm, got_hbm = take(2), take(2)
    qkv_out, proj_out, ada_out = take(3)
    mlp_outs = take(2)
    cond_out, ada_bias_out, qkv_bias_out, up_bias_out, gain_out, proj_bias_out, down_bias_out = take(7)
    slots, terms, turned = take(4), take(4), take(4)
    (ring_sems,) = take(1)
    packed, attn, left, inputs = take(2), take(2), take(2), take(2)
    (weight_ref,) = take(1)
    outgoing, incoming, own = take(2), take(2), take(2)
    (edge_sums,) = take(1)
    load_sems, core_sems, swap_sems, out_sems, ready_sem = take(5)
    scratch = take(14)
    (mod_sems,) = take(1)
    size = len(order)
    feat = mod_ref.shape[2]
    local = attn[0].shape[1]
    cols = ada_hbm.shape[1]
    rows = [ref.shape[0] for ref in own]
    lengths = [count // seqs for count in rows]
    row, _, around, across = peers_of(size, tensor_size)
    partner, facing = across[0], across[1]
    ring = Ring(
        order, 0, (left[0], left[1], left[0], left[1]), packed + attn, slots, terms, turned, ring_sems
    )
    started = []

    def load(source, target):
        copy = pltpu.make_async_copy(source, target, load_sems.at[len(started)])
        copy.start()
        started.append(copy)
        return copy

    stored = []

    def store(source, target):
        copy = pltpu.make_async_copy(source, target, out_sems.at[len(stored)])
        copy.start()
        stored.append(copy)
        return copy

    first = [
        (load(hidden_hbm[stream], left[stream]), load(packed_hbm[stream], packed[stream]))
        for stream in range(2)
    ]
    second = [load(attn_hbm[stream], attn[stream]) for stream in range(2)]
    weight_load = load(weight_hbm, weight_ref)
    input_loads = [
        move_halves(load, input_hbm[stream], inputs[stream], seqs, directs[stream], halves=1)
        for stream in range(2)
    ]
    greet(around + across)
    again = []
    for stream in range(2):
        for copy in first[stream]:
            copy.wait()
        ring.begin(stream)
        again.append(load(branch_hbm[stream], left[stream]))
    for stream in range(2):
        again[stream].wait()
        second[stream].wait()
        ring.begin(2 + stream)
    cot_loads = [
        move_halves(load, cot_hbm[stream], left[stream], seqs, directs[stream]) for stream in range(2)
    ]

    weight_load.wait()
    count = feat // block
    exchanges = []

    def columns(index):
        return pl.ds(pl.multiple_of(index * block, block), block)

    def part_copy(stream, index):
        return pltpu.make_async_remote_copy(
            src_ref=outgoing[stream].at[:, columns(index)],
            dst_ref=incoming[stream].at[:, columns(index)],
            send_sem=core_sems.at[0, stream * count + index],
            recv_sem=core_sems.at[1, stream * count + index],
            device_id=partner,
            device_id_type=pl.DeviceIdType.MESH,
        )

    for stream in (1, 0):

        def send_part(index, carry):
            cols = columns(index)
            both = sum(
                dot_right_t(
                    packed[stream][:, part * local : (part + 1) * local], weight_ref[stream, part, cols, :]
                )
                for part in range(3)
            )
            own[stream][:, cols] = both[: rows[stream]]
            outgoing[stream][:, cols] = both[rows[stream] :]
            part_copy(stream, index).start()
            return carry

        lax.fori_loop(0, count, send_part, 0)
    for stream in (1, 0):

        def add_part(index, carry):
            part_copy(stream, index).wait()
            cols = columns(index)
            own[stream][:, cols] = own[stream][:, cols] + incoming[stream][:, cols]
            return carry

        lax.fori_loop(0, count, add_part, 0)
        exchanges.append(remote(own[stream], got_hbm[stream], swap_sems, stream, facing))
    through_loads = [load(through_hbm[stream], incoming[stream]) for stream in range(2)]
    middle = max(ring.last - 2, 0)
    ring.rounds(0, middle)

    for copy in exchanges:
        copy.wait()
    got_loads = [load(got_hbm[stream], outgoing[stream]) for stream in range(2)]
    for stream in range(2):
        wait_all(input_loads[stream] + cot_loads[stream] + [through_loads[stream]])
    for stream in (1, 0):
        got_loads[stream].wait()

        def back_rows(seq, carry):
            scale = 1.0 + mod_ref[stream * 6 + 1, pl.ds(seq, 1), :]

            def back(at):
                normed, inverse = norm_of(inputs[stream][at].astype(jnp.float32))
                grad_hidden = own[stream][at] + outgoing[stream][at]
                added = incoming[stream][at] + norm_back(grad_hidden * scale, normed, inverse)
                own[stream][at] = added
                left[stream][at] = (left[stream][at].astype(jnp.float32) + added).astype(jnp.bfloat16)
                return grad_hidden, grad_hidden * normed

            totals = over_rows(seq * lengths[stream], lengths[stream], feat, 2, back)
            for index in range(2):
                edge_sums[2 * stream + index, pl.ds(seq, 1)] = totals[index]
            return carry

        lax.fori_loop(0, seqs, back_rows, 0)
    pl.semaphore_signal(ready_sem, inc=1, device_id=partner, device_id_type=pl.DeviceIdType.MESH)

    def mod_rows(stream):
        inner = small_sums[stream][3]
        return jnp.concatenate(
            [edge_sums[2 * stream], edge_sums[2 * stream + 1]] + [inner[index] for index in range(4)],
            axis=1,
        )

    def lines_of():
        def wide(values):
            return jnp.pad(values, ((0, 0), (0, feat - values.shape[1])))

        bias = functools.reduce(jnp.add, [bias_sum_ref[seq] for seq in range(seqs)])
        gain = functools.reduce(jnp.add, [gain_sum_ref[seq] for seq in range(seqs)])
        gain = gain[:, : gain.shape[1] // 2] + gain[:, gain.shape[1] // 2 :]
        group = [wide(bias)] + [wide(small_sums[stream][0][...]) for stream in range(2)]
        every = [wide(gain)]
        every += [small_sums[stream][1][...] * row_share for stream in range(2)]
        every += [small_sums[stream][2][...] * row_share for stream in range(2)]
        return jnp.concatenate(group + [jnp.zeros((4, feat), jnp.float32)] + every, axis=0)

    def put(name, values):
        if name == "group":
            for part in range(3):
                qkv_bias_out[part] = values[0:2, part * local : (part + 1) * local]
            up_bias_out[...] = values[2:4, : up_bias_out.shape[1]]
        elif name == "every":
            for stream in range(2):
                gain_out[stream] = values[2 * stream : 2 * stream + 2, : gain_out.shape[2]]
            proj_bias_out[...] = values[4:6]
            down_bias_out[...] = values[6:8]
        elif name == "silu":
            cond = cond_ref[0:seqs].astype(jnp.float32)
            for index in range(1, size):
                rows_here = cond_ref[index * seqs : (index + 1) * seqs].astype(jnp.float32)
                cond = jnp.where(row == index, rows_here, cond)
            sig = 1.0 / (1.0 + jnp.exp(-cond))
            cond_out[...] = values * sig * (1.0 + cond * (1.0 - sig))
        elif name[0] == "ada_bias":
            ada_bias_out[name[1] : name[1] + 1] = values
        else:
            target = own[0] if name[1] == 0 else incoming[0]
            for start in range(0, feat, block):
                target[:cols, start : start + block] = values(slice(start, start + block))
            store(target.at[:cols], ada_out.at[name[1]])

    def weight_of(stream):
        return left[0][stream * cols : (stream + 1) * cols]

    steps = mod_backward_steps(
        size, tensor_size, mod_rows, cond_ref, weight_of, lines_of, put, scratch, mod_sems
    )
    next(steps)
    pl.semaphore_wait(ready_sem, 1)
    shares = [
        remote(own[stream], outgoing[stream], core_sems, 2 * count + stream, partner)
        for stream in range(2)
    ]
    next(steps)
    for copy in shares:
        copy.wait()
    results = []
    for stream in (1, 0):
        def other_rows(at):
            there = shifted(at, rows[stream])
            left[stream][there] = (
                left[stream][there].astype(jnp.float32) + outgoing[stream][at]
            ).astype(jnp.bfloat16)
            return ()

        over_rows(0, rows[stream], feat, 0, other_rows, LIGHT)
        results.append(
            move_halves(store, out_hbm[stream], left[stream], seqs, directs[stream], to_array=True)
        )

    height = arrived[0][0].shape[0]
    sides = (
        (outgoing[0].at[:height], outgoing[0].at[height : 2 * height]),
        (outgoing[1].at[:height], incoming[1].at[:height]),
    )

    def fetch(stream):
        return [
            load(arrived[stream][2 * way + side], sides[way][side]) for way in range(2) for side in range(2)
        ]

    def add_up(stream, copies):
        puts = []
        for copy in copies:
            copy.wait()
        for way, (first, second) in enumerate(sides):
            first[...] = first[...] + second[...]
            for which in range(2):
                puts.append(
                    store(
                        first.at[which * ring.half : (which + 1) * ring.half],
                        mlp_outs[which].at[stream, way * ring.half : (way + 1) * ring.half],
                    )
                )
        return puts

    fetched = fetch(1)
    ring.rounds(middle, ring.last - 1)
    puts = add_up(1, fetched)
    for copy in results[1]:
        copy.wait()
    ada_loads = [
        load(ada_hbm.at[stream], left[0].at[stream * cols : (stream + 1) * cols]) for stream in range(2)
    ]
    for copy in ada_loads:
        copy.wait()
    next(steps)
    for copy in puts:
        copy.wait()
    fetched = fetch(0)
    ring.rounds(ring.last - 1, ring.last)
    add_up(0, fetched)
    for _ in range(len(across)):
        next(steps)

    def put_total(which, way, values):
        slot = slots[which].at[way, ring.last]
        slot[...] = values
        place = slice(way * ring.half, (way + 1) * ring.half)
        if which < 2:
            for part in range(3):
                store(slot.at[:, part * local : (part + 1) * local], qkv_out.at[which, part, place])
        else:
            store(slot, proj_out.at[which - 2, place])

    ring.finish(None, put_total)
    for _ in steps:
        pass
    waited = {id(copy) for copy in puts + results[1]}
    for copy in stored:
        if id(copy) not in waited:
            copy.wait()


def attn_ring(
    modulate, conditioning, gain_sums, bias_sums, states, packed, attn, hidden, inputs, cots, weight,
    ada_weight, order, tensor_size, row_share, directs, collective_id,
):
    seqs, feat = modulate.shape[1:]
    size, local, cols = len(order), attn[0].shape[1], ada_weight.shape[1]
    rows = [seqs * array.shape[2] for array in inputs]
    units = states[0]["up_bias"].shape[1]
    block = 256
    half = feat // (2 * size)
    vmem = pl.BlockSpec(memory_space=pltpu.VMEM)
    anywhere = pl.BlockSpec(memory_space=pl.ANY)

    def wide(*dims):
        return jax.ShapeDtypeStruct(dims, jnp.float32)

    def low(*dims):
        return pltpu.VMEM(dims, jnp.bfloat16)

    large = [jax.ShapeDtypeStruct(array.shape, jnp.bfloat16) for array in inputs]
    large += [wide(count, feat) for count in rows]
    large += [wide(2, 3, 2 * half, local), wide(2, 2 * half, local), wide(2, cols, feat)]
    large += [wide(2, 2 * half, units)] * 2
    small = [
        wide(seqs, feat),
        wide(2, cols),
        wide(3, 2, local),
        wide(2, units),
        wide(2, 2, gain_sums.shape[2] // 2),
        wide(2, feat),
        wide(2, feat),
    ]
    halves = [(half, 3 * local)] * 2 + [(half, local)] * 2
    doubled = [(2 * count, feat) for count in rows]
    mod_refs, mod_sems = mod_scratch(size, tensor_size, seqs, feat, cols)
    moved = 4 * 2 * (size - 1) * half * 8 * local
    blocks = feat // block
    sums = [
        state[name] for state in states for name in ("up_bias", "proj_bias", "down_bias", "mod_sums")
    ]
    pairs = [
        packed,
        attn,
        hidden,
        [state["grad_branch"] for state in states],
        [state["through"] for state in states],
        inputs,
        cots,
    ]
    return pl.pallas_call(
        functools.partial(attn_ring_kernel, order, tensor_size, seqs, block, row_share, directs),
        out_shape=large + small,
        in_specs=[vmem] * (4 + len(sums)) + [anywhere] * (2 * len(pairs) + 10),
        out_specs=[anywhere] * len(large) + [vmem] * len(small),
        scratch_shapes=ring_scratch(size, halves, doubled + doubled)
        + [low(2 * count, 3 * local) for count in rows]
        + [low(2 * count, local) for count in rows]
        + [low(2 * count, feat) for count in rows]
        + [low(count, feat) for count in rows]
        + [low(2, 3, feat, local)]
        + [pltpu.VMEM((count, feat), jnp.float32) for count in rows] * 3
        + [
            pltpu.VMEM((4, seqs, feat), jnp.float32),
            pltpu.SemaphoreType.DMA((28 + 6 * seqs,)),
            pltpu.SemaphoreType.DMA((2, 2 * blocks + 2)),
            pltpu.SemaphoreType.DMA((2, 2)),
            pltpu.SemaphoreType.DMA((32 + 4 * seqs,)),
            pltpu.SemaphoreType.REGULAR,
        ]
        + mod_refs
        + [mod_sems],
        compiler_params=pltpu.CompilerParams(
            collective_id=collective_id, has_side_effects=True, vmem_limit_bytes=67043328
        ),
        cost_estimate=pl.CostEstimate(flops=moved * 10000, bytes_accessed=moved, transcendentals=0),
        name="attn_ring",
    )(
        modulate,
        conditioning,
        gain_sums,
        bias_sums,
        *sums,
        *[array for pair in pairs for array in pair],
        weight,
        ada_weight,
        *[array for state in states for pair in state["ring"] for array in pair],
    )


def ring_rest(parts, order, rest):
    size = len(order)
    ahead = [(order[index], order[(index + 1) % size]) for index in range(size)]
    ways = (ahead, [(second, first) for first, second in ahead])
    totals = list(parts[:2])
    for later in range(rest):
        for way in range(2):
            if later:
                totals[way] = totals[way] + parts[2 * later + way]
            totals[way] = lax.ppermute(totals[way], "dp", ways[way])
    return [(totals[way], parts[2 * rest + way]) for way in range(2)]


def on_device(
    order,
    tensor_size,
    input_img,
    input_txt,
    conditioning,
    ada_weight,
    ada_bias,
    qkv_weight,
    qkv_bias,
    norm_gain,
    proj_weight,
    proj_bias,
    up_weight,
    up_bias,
    down_weight,
    down_bias,
    cotangent_img,
    cotangent_txt,
):
    data_size = len(order)
    seqs, _, feat = input_img.shape
    reals = (input_img.shape[1] // 2, input_txt.shape[1] // 2)
    directs = [
        shape[1] == 2 * real and real % ROW_TILE == 0
        for shape, real in zip((input_img.shape, input_txt.shape), reals)
    ]

    def split_rows(array, stream):
        real = reals[stream]
        if directs[stream]:
            return array.reshape(seqs, 2, real, feat)
        pad = -real % ROW_TILE
        return jnp.stack(
            [
                jnp.pad(part, ((0, 0), (0, pad), (0, 0)))
                for part in (array[:, :real], array[:, real:])
            ]
        )

    def join_rows(halves, stream):
        real = reals[stream]
        if directs[stream]:
            return halves.reshape(seqs, 2 * real, feat)
        return jnp.concatenate([halves[0][:, :real], halves[1][:, :real]], axis=1)

    ada_weight = ada_weight.transpose(0, 2, 1)
    modulate = mod_forward(
        conditioning, ada_weight, ada_bias, seqs, feat, data_size, tensor_size
    )
    inputs = [split_rows(input_img, 0), split_rows(input_txt, 1)]
    cotangents = [split_rows(cotangent_img, 0), split_rows(cotangent_txt, 1)]
    gain_pair = jnp.concatenate([norm_gain, norm_gain], axis=2)

    qkv_weight = qkv_weight.transpose(0, 2, 1, 3)
    hidden1, raw, attn, branch_sums, got = front(
        modulate, gain_pair, inputs, directs, qkv_weight, qkv_bias.transpose(1, 0, 2), proj_weight, reals[1], 5
    )
    local = attn[0].shape[3]

    def mlp_stage(stream, got, gives, rest, collective_id):
        made = mlp_ring(
            stream,
            branch_sums[stream],
            got,
            inputs[stream],
            cotangents[stream],
            modulate,
            proj_bias,
            up_bias,
            down_bias,
            up_weight,
            down_weight,
            proj_weight,
            gives,
            order,
            rest,
            directs[stream],
            collective_id,
        )
        made["ring"] = ring_rest(made["ring"], order, rest)
        return made

    state = [None, None]
    state[1] = mlp_stage(1, got, [branch_sums[0]], RESTS[0], 2)
    state[0] = mlp_stage(0, state[1]["gets"][0], [], RESTS[1], 3)

    grad_attn = [state[stream]["grad_attn"].reshape(attn[stream].shape) for stream in range(2)]
    grad_packed = attn_backward(gain_pair, list(raw[0]), list(raw[1]), grad_attn[0], grad_attn[1], reals[1])
    made = attn_ring(
        modulate,
        conditioning,
        grad_packed[3],
        grad_packed[2],
        state,
        [grad_packed[stream].reshape(-1, 3 * local) for stream in range(2)],
        [attn[stream].reshape(-1, local) for stream in range(2)],
        hidden1,
        inputs,
        cotangents,
        qkv_weight,
        ada_weight,
        order,
        tensor_size,
        2.0 / tensor_size,
        directs,
        4,
    )
    grad_qkv, grad_proj, grad_ada_weight, grad_down, grad_up, grad_conditioning, grad_ada_bias = made[4:11]
    qkv_bias_sums, up_bias_sums, gain_sums, proj_sums, down_sums = made[11:]

    outputs = [join_rows(state[stream]["out"], stream) for stream in range(2)]
    grad_inputs = [join_rows(made[stream], stream) for stream in range(2)]
    return (
        outputs[0],
        outputs[1],
        grad_inputs[0],
        grad_inputs[1],
        grad_conditioning,
        grad_ada_weight.transpose(0, 2, 1),
        grad_ada_bias,
        grad_qkv.transpose(0, 2, 1, 3),
        qkv_bias_sums.transpose(1, 0, 2),
        gain_sums,
        grad_proj.transpose(0, 2, 1),
        proj_sums,
        grad_up,
        up_bias_sums,
        grad_down.transpose(0, 2, 1),
        down_sums,
    )


def solution(mesh):
    in_specs = (
        P("dp", None, None),
        P("dp", None, None),
        P(),
        P(None, None, ("dp", "tensor")),
        P(None, ("dp", "tensor")),
        P(None, None, None, "tensor"),
        P(None, None, "tensor"),
        P(),
        P(None, "tensor", None),
        P(),
        P(None, None, "tensor"),
        P(None, "tensor"),
        P(None, "tensor", None),
        P(),
        P("dp", None, None),
        P("dp", None, None),
    )
    out_specs = (
        P("dp", None, None),
        P("dp", None, None),
        P("dp", None, None),
        P("dp", None, None),
        P("dp", None),
        P(None, None, ("dp", "tensor")),
        P(None, ("dp", "tensor")),
        P(None, "dp", None, "tensor"),
        P(None, None, "tensor"),
        P(),
        P(None, "tensor", "dp"),
        P(),
        P(None, "dp", "tensor"),
        P(None, "tensor"),
        P(None, "tensor", "dp"),
        P(),
    )

    def step(*arrays):
        return on_device(ring_order(mesh), mesh.shape["tensor"], *arrays)

    return jax.shard_map(
        step, mesh=mesh, in_specs=in_specs, out_specs=out_specs, check_vma=False
    )
```
